128 devices in a mesh: grid: 32 (over x_hi, z, y), band: 4 (over x_lo, core).
Axes of the slice: x: 4 (x_hi: 2, x_lo: 2; x = x_hi * 2 + x_lo), y: 4, z: 4, core: 2. Of those that a mesh axis runs over, the one named last changes fastest.
Arguments:
- orbitals: float32 [128, 16, 16, 512], P('grid', None, None, 'band'), may hold values from -80 to 80
- projectors: float32 [128, 16, 16, 512], P('grid', None, None, 'band'), may hold values from -0.046875 to 0.046875
- potential: float32 [128, 16, 16], P('grid'), may hold values from 0.3 to 3
Outputs:
- updated_orbitals: float32 [128, 16, 16, 512], P('grid', None, None, 'band')
- rayleigh_quotients: float32 [3, 512], P(None, 'band')
- residual_norms: float32 [3, 512], P(None, 'band')
The draws below stay inside these ranges and needn't reach their ends.
All inputs are finite; a program needn't handle non-finite values.
Results may differ from the reference program's by a relative error of at most 0.00012.
Values sent between devices are 32-bit elements; how exact they have to be, the bound alone decides.
No kernel may reach another device: no remote copies, remote signals or barrier semaphores. Data moves between devices by JAX's collectives and lax.ppermute only.
A program may use at most 128 MiB of HBM per device.

```python
import math
import jax
import jax.numpy as jnp
from jax import lax

NX = 16
NY = 16
BANDS = 512
NXI = 512
ITERS = 3
NZ = 128


def draw_orbitals(key, part):
    jitter_key = jax.random.fold_in(key, 11)
    scale_key = jax.random.fold_in(key, 12)
    height = jnp.arange(NZ, dtype=jnp.float32) / max(NZ - 1, 1)
    scales = jnp.exp(jax.random.uniform(scale_key, (BANDS,), jnp.float32, 0.0, math.log(10.0)))
    profile = 0.6 + 1.2 * height
    jitter = jnp.clip(jax.random.normal(jitter_key, (NZ, NX, NY, BANDS), jnp.float32), -4.0, 4.0)
    values = jitter * profile[:, None, None, None] * scales
    return values.astype(jnp.float32)


def steps_of(key, extent, shards, smallest, top_value):
    def one(axis_at, shards_of):
        draws = jax.random.uniform(jax.random.fold_in(jax.random.fold_in(key, 6), axis_at), (shards_of,), jnp.float32, smallest / len(shards), top_value / len(shards))
        return jnp.repeat(jnp.exp(draws), extent[axis_at] // shards_of).reshape((-1,) + (1,) * (len(extent) - axis_at - 1))

    gain = one(*shards[0])
    for cut in shards[1:]:
        gain = gain * one(*cut)
    return gain


def scatter_about(key, shape, spread, bound, split=(), held_as=jnp.bfloat16):
    factor_of = steps_of(key, shape, split, -0.22, 0.18) if split else 1.0
    values = jax.random.normal(key, shape, jnp.float32) * spread * factor_of
    return jnp.minimum(jnp.maximum(values, -bound), bound).astype(held_as)


def setup_inputs(seed: int = 0) -> dict:
    splits = jax.random.split(jax.random.key(seed), 4)
    return {
        "orbitals": draw_orbitals(jax.random.fold_in(splits[3], 71), 0),
        "projectors": scatter_about(splits[1], (NZ, NX, NY, NXI), ((2.0 / (NZ * NX * NY)) ** 0.5), 0.046875, ((0, 32), (3, 4)), jnp.float32),
        "potential": jnp.clip(jnp.exp(math.log(3.0) - 2.3025851 * jax.random.uniform(splits[2], (NZ, NX, NY), jnp.float32) ** steps_of(splits[2], (NZ, NX, NY), ((0, 32),), -0.2, 0.2)), 0.3, 3.0),
    }


STENCIL = (-205.0 / 72.0, 8.0 / 5.0, -1.0 / 5.0, 8.0 / 315.0, -1.0 / 560.0)
STEP_LENGTH = 0.25
NORM_EPS = 1e-06
HIGHEST = lax.Precision.HIGHEST

def laplacian(grid_field):
    result = 3.0 * STENCIL[0] * grid_field
    for dimension in (0, 1, 2):
        for distance in range(1, 5):
            result = result + STENCIL[distance] * (jnp.roll(grid_field, distance, dimension) + jnp.roll(grid_field, -distance, dimension))
    return result

def matmul(left, right):
    return jnp.dot(left.astype(jnp.float32), right.astype(jnp.float32), precision=HIGHEST, preferred_element_type=jnp.float32)

def reference(orbitals, projectors, potential):
    grid_shape = orbitals.shape
    vectors = orbitals.reshape(-1, BANDS)
    projector_rows = projectors.reshape(-1, NXI)
    identity_matrix = jnp.eye(BANDS, dtype=jnp.float32)
    quotient_list = []
    norm_list = []
    for iteration in range(ITERS):
        margin = matmul(vectors.T, vectors)
        factor = jnp.linalg.cholesky(margin)
        inverse = jax.scipy.linalg.solve_triangular(factor, identity_matrix, lower=True)
        vectors = matmul(vectors, inverse.T)
        coupling = matmul(projector_rows.T, vectors)
        exchange_part = matmul(projector_rows, coupling)
        grid_field = vectors.reshape(grid_shape)
        applied = (-0.5 * laplacian(grid_field) + potential[..., None] * grid_field).reshape(-1, BANDS) - exchange_part
        rayleigh = lax.optimization_barrier(jnp.sum(vectors * applied, axis=0))
        residual = applied - rayleigh[None, :] * vectors
        squared = lax.optimization_barrier(jnp.sum(residual * residual, axis=0))
        vectors = vectors - STEP_LENGTH * residual / jnp.sqrt(squared + NORM_EPS)[None, :]
        quotient_list.append(rayleigh)
        norm_list.append(jnp.sqrt(squared))
    return (vectors.reshape(grid_shape), jnp.stack(quotient_list), jnp.stack(norm_list))
```

```python
import jax
import jax.numpy as jnp
from jax import lax
from jax.experimental import pallas as pl
from jax.experimental.pallas import tpu as pltpu
from jax.sharding import Mesh
from jax.sharding import PartitionSpec as P

ITERS = 3
BAND = ("band_0", "band_1")


STENCIL = (-205.0 / 72.0, 8.0 / 5.0, -1.0 / 5.0, 8.0 / 315.0, -1.0 / 560.0)
STEP_LENGTH = 0.25
NORM_EPS = 1e-06
HIGHEST = lax.Precision.HIGHEST

BLOCK = 128
TILE = 8

def dot_t(left, right):
    return lax.dot_general(left, right, (((0,), (0,)), ((), ())), precision=HIGHEST,
                           preferred_element_type=jnp.float32)

def row_of(tile, j):
    return jnp.broadcast_to(tile[j:j + 1, :], tile.shape)

def lane_of(tile, j):
    return jnp.broadcast_to(tile[:, j:j + 1], tile.shape)

def inverse_factor(tiles):
    count = len(tiles)
    lane = lax.broadcasted_iota(jnp.int32, tiles[0].shape, 1)
    sub = lax.broadcasted_iota(jnp.int32, tiles[0].shape, 0)
    tiles = list(tiles)
    for p in range(count):
        base = TILE * p
        inside = (lane >= base) & (lane < base + TILE)
        head = [lane_of(tiles[p], base + j) for j in range(TILE)]
        own = jnp.where(inside, (lane == base + sub).astype(jnp.float32), tiles[p])
        rows, scales, crosses = [], [], []
        for j in range(TILE):
            scale = lax.rsqrt(row_of(head[j], j))
            row = row_of(own, j) * scale
            column = jnp.where(sub > j, head[j] * scale, 0.0)
            own = jnp.where(sub == j, row, own - column * row)
            cross = [None] * TILE
            for k in range(j + 1, TILE):
                cross[k] = row_of(head[k], j) * scale
                head[k] = head[k] - column * cross[k]
            rows.append(row)
            scales.append(scale)
            crosses.append(cross)
        tiles[p] = jnp.where(lane < base + TILE, own, 0.0)
        for t in range(p + 1, count):
            parts = [lane_of(tiles[t], base + j) for j in range(TILE)]
            tile = jnp.where(inside, 0.0, tiles[t])
            for j in range(TILE):
                column = parts[j] * scales[j]
                tile = tile - column * rows[j]
                for k in range(j + 1, TILE):
                    parts[k] = parts[k] - column * crosses[j][k]
            tiles[t] = tile
    return tiles

def factor_kernel(s_ref, x_ref):
    size = s_ref.shape[0]
    blocks = size // BLOCK
    x_ref[...] = s_ref[...]
    def step(k, carry):
        here = pl.ds(pl.multiple_of(k * BLOCK, BLOCK), BLOCK)
        tiles = [x_ref[pl.ds(pl.multiple_of(k * BLOCK + TILE * t, TILE), TILE), here] for t in range(BLOCK // TILE)]
        own = jnp.concatenate(inverse_factor(tiles), axis=0)
        x_ref[here, here] = jnp.eye(BLOCK, dtype=jnp.float32)
        panel = jnp.dot(own, x_ref[here, :], precision=HIGHEST, preferred_element_type=jnp.float32)
        x_ref[here, :] = panel
        def update(i, carry):
            there = pl.ds(pl.multiple_of(i * BLOCK, BLOCK), BLOCK)
            x_ref[there, here] = jnp.zeros((BLOCK, BLOCK), jnp.float32)
            x_ref[there, :] = x_ref[there, :] - dot_t(x_ref[here, there], x_ref[here, :])
            return carry
        return lax.fori_loop(k + 1, blocks, update, carry)
    lax.fori_loop(0, blocks, step, 0)
    row = lax.broadcasted_iota(jnp.int32, (size, size), 0)
    column = lax.broadcasted_iota(jnp.int32, (size, size), 1)
    x_ref[...] = jnp.where(row >= column, x_ref[...], 0.0)

def inverse_cholesky(s):
    return pl.pallas_call(
        factor_kernel,
        out_shape=jax.ShapeDtypeStruct(s.shape, jnp.float32),
        in_specs=[pl.BlockSpec(memory_space=pltpu.VMEM)],
        out_specs=pl.BlockSpec(memory_space=pltpu.VMEM),
        name="inverse_factor",
        cost_estimate=pl.CostEstimate(flops=20_000_000_000, bytes_accessed=2 * s.size * 4, transcendentals=s.shape[0]),
    )(s)


def with_halo(block, sides, width):
    for axis, dim in sides:
        count = lax.axis_size(axis)
        forward = [(i, i + 1) for i in range(count - 1)]
        forward.append((count - 1, 0))
        backward = [(target, source) for source, target in forward]
        low = lax.ppermute(
            lax.slice_in_dim(block, block.shape[dim] - width, None, axis=dim), axis, forward
        )
        high = lax.ppermute(lax.slice_in_dim(block, 0, width, axis=dim), axis, backward)
        block = jnp.concatenate([low, block, high], axis=dim)
    return block


def from_everyone(x, axis):
    copies = jnp.broadcast_to(x, (lax.axis_size(axis), *x.shape))
    return lax.all_to_all(copies, axis, split_axis=0, concat_axis=0, tiled=True)


def joined_along(pieces, dim):
    dims = list(pieces.shape[1:])
    dims[dim] *= pieces.shape[0]
    return jnp.moveaxis(pieces, 0, dim).reshape(dims)


def gathered_by_axis(x, axes, dim):
    far, near = axes
    initial = from_everyone(x, far)
    pieces = jnp.swapaxes(from_everyone(initial, near), 0, 1)
    return joined_along(pieces.reshape(-1, *x.shape), dim)


def rows_for(lines, count):
    spare = -len(lines) % count
    return jnp.pad(lines, [(0, spare)] + [(0, 0)] * (lines.ndim - 1))


def collect(x, axis, dim):
    pieces = from_everyone(x, axis)
    return joined_along(pieces, dim)


def cut_along(x, dim, count):
    before, after = (x.shape[:dim], x.shape[dim + 1 :])
    return jnp.moveaxis(x.reshape(*before, count, -1, *after), dim, 0)


def sum_at_owner(x, axis, dim):
    pieces = cut_along(x, dim, lax.axis_size(axis))
    arrived = lax.all_to_all(pieces, axis, split_axis=0, concat_axis=0, tiled=True)
    return arrived.sum(axis=0)


def nested_sum(x, axes):
    lines = x.reshape(-1, x.shape[-1])
    padded = rows_for(lines, lax.axis_size(axes))
    whole = collect(sum_at_owner(padded, axes, 0), axes, 0)
    return lax.slice_in_dim(whole, 0, len(lines)).reshape(x.shape)


def over_copies(x, axis):
    return from_everyone(x, axis).sum(axis=0)


def together(arrays, axis):
    ends = [0]
    for a in arrays:
        ends.append(ends[-1] + a.size)
    subtotal = over_copies(jnp.concatenate([a.ravel() for a in arrays]), axis)
    return tuple((subtotal[b:e].reshape(a.shape) for a, b, e in zip(arrays, ends, ends[1:])))


def matmul(left, right):
    return jnp.dot(left, right, precision=HIGHEST, preferred_element_type=jnp.float32)


def laplacian(grid_field):
    padded = with_halo(grid_field, (("grid", 0),), 4)
    planes_here = grid_field.shape[0]
    result = 3.0 * STENCIL[0] * grid_field
    for distance in range(1, 5):
        result = result + STENCIL[distance] * (
            padded[4 + distance : 4 + distance + planes_here]
            + padded[4 - distance : 4 - distance + planes_here]
        )
    for dimension in (1, 2):
        for distance in range(1, 5):
            result = result + STENCIL[distance] * (
                jnp.roll(grid_field, distance, dimension)
                + jnp.roll(grid_field, -distance, dimension)
            )
    return result


def local(orbitals, projectors, potential):
    grid_shape = orbitals.shape
    local_bands = orbitals.shape[3]
    total_bands = local_bands * lax.axis_size(BAND)
    first_band = lax.axis_index(BAND) * local_bands
    vectors = orbitals.reshape(-1, local_bands)
    every_projector = gathered_by_axis(projectors, ("band_0", "band_1"), 3).reshape(
        -1, projectors.shape[3] * lax.axis_size(BAND)
    )
    quotient_list = []
    norm_list = []
    for iteration in range(ITERS):
        gathered = gathered_by_axis(vectors.reshape(grid_shape), ("band_0", "band_1"), 3).reshape(
            -1, total_bands
        )
        own_rows = nested_sum(matmul(vectors.T, gathered), "grid")
        margin = collect(own_rows, BAND, 0)
        inverse = inverse_cholesky(margin)
        transform = inverse.T
        vectors = matmul(gathered, lax.dynamic_slice_in_dim(transform, first_band, local_bands, 1))
        coupling = nested_sum(matmul(every_projector.T, vectors), "grid")
        exchange_part = matmul(every_projector, coupling)
        grid_field = vectors.reshape(grid_shape)
        applied = (-0.5 * laplacian(grid_field) + potential[..., None] * grid_field).reshape(
            -1, local_bands
        ) - exchange_part
        rayleigh, energy, weight = together(
            (
                jnp.sum(vectors * applied, axis=0),
                jnp.sum(applied * applied, axis=0),
                jnp.sum(vectors * vectors, axis=0),
            ),
            "grid",
        )
        residual = applied - rayleigh[None, :] * vectors
        squared = energy - 2.0 * rayleigh * rayleigh + rayleigh * rayleigh * weight
        vectors = vectors - STEP_LENGTH * residual / jnp.sqrt(squared + NORM_EPS)[None, :]
        quotient_list.append(rayleigh)
        norm_list.append(jnp.sqrt(squared))
    return (vectors.reshape(grid_shape), jnp.stack(quotient_list), jnp.stack(norm_list))


def solution(mesh):
    finer = Mesh(mesh.devices.reshape(mesh.shape["grid"], 2, 2), ("grid", "band_0", "band_1"))
    placed = (P("grid", None, None, BAND), P("grid", None, None, BAND), P("grid", None, None))
    return jax.shard_map(
        local,
        mesh=finer,
        in_specs=placed,
        out_specs=(P("grid", None, None, BAND), P(None, BAND), P(None, BAND)),
        check_vma=False,
    )
```

```python
import jax
import jax.numpy as jnp
from jax import lax
from jax.experimental import pallas as pl
from jax.experimental.pallas import tpu as pltpu
from jax.sharding import Mesh
from jax.sharding import PartitionSpec as P

ITERS = 3
BAND = ("band_0", "band_1")
EVERY = ("grid", "band_0", "band_1")
BLOCK = 128
TILE = 8

STENCIL = (-205.0 / 72.0, 8.0 / 5.0, -1.0 / 5.0, 8.0 / 315.0, -1.0 / 560.0)
STEP_LENGTH = 0.25
NORM_EPS = 1e-06
HIGHEST = lax.Precision.HIGHEST
WHOLE = pl.BlockSpec(memory_space=pltpu.VMEM)


def dot(left, right, sides):
    return lax.dot_general(
        left, right, ((sides[:1], sides[1:]), ((), ())), precision=HIGHEST,
        preferred_element_type=jnp.float32,
    )


def row_of(tile, j):
    return jnp.broadcast_to(tile[j:j + 1, :], tile.shape)

def lane_of(tile, j):
    return jnp.broadcast_to(tile[:, j:j + 1], tile.shape)

def inverse_factor(tiles):
    count = len(tiles)
    lane = lax.broadcasted_iota(jnp.int32, tiles[0].shape, 1)
    sub = lax.broadcasted_iota(jnp.int32, tiles[0].shape, 0)
    tiles = list(tiles)
    for p in range(count):
        base = TILE * p
        inside = (lane >= base) & (lane < base + TILE)
        head = [lane_of(tiles[p], base + j) for j in range(TILE)]
        own = jnp.where(inside, (lane == base + sub).astype(jnp.float32), tiles[p])
        rows, scales, crosses = [], [], []
        for j in range(TILE):
            scale = lax.rsqrt(row_of(head[j], j))
            row = row_of(own, j) * scale
            column = jnp.where(sub > j, head[j] * scale, 0.0)
            own = jnp.where(sub == j, row, own - column * row)
            cross = [None] * TILE
            for k in range(j + 1, TILE):
                cross[k] = row_of(head[k], j) * scale
                head[k] = head[k] - column * cross[k]
            rows.append(row)
            scales.append(scale)
            crosses.append(cross)
        tiles[p] = jnp.where(lane < base + TILE, own, 0.0)
        for t in range(p + 1, count):
            parts = [lane_of(tiles[t], base + j) for j in range(TILE)]
            tile = jnp.where(inside, 0.0, tiles[t])
            for j in range(TILE):
                column = parts[j] * scales[j]
                tile = tile - column * rows[j]
                for k in range(j + 1, TILE):
                    parts[k] = parts[k] - column * crosses[j][k]
            tiles[t] = tile
    return tiles


def pairs_of(blocks):
    return [(i, j) for i in range(blocks) for j in range(i, blocks)]


def factor_kernel(s_ref, x_ref):
    blocks = x_ref.shape[0] // BLOCK
    for at, (i, j) in enumerate(pairs_of(blocks)):
        x_ref[BLOCK * i : BLOCK * (i + 1), BLOCK * j : BLOCK * (j + 1)] = s_ref[
            BLOCK * at : BLOCK * (at + 1), :
        ]

    def step(k, carry):
        here = pl.ds(pl.multiple_of(k * BLOCK, BLOCK), BLOCK)
        tiles = [
            x_ref[pl.ds(pl.multiple_of(k * BLOCK + TILE * t, TILE), TILE), here]
            for t in range(BLOCK // TILE)
        ]
        own = jnp.concatenate(inverse_factor(tiles), axis=0)
        x_ref[here, here] = jnp.eye(BLOCK, dtype=jnp.float32)
        x_ref[here, :] = dot(own, x_ref[here, :], (1, 0))

        def update(i, carry):
            there = pl.ds(pl.multiple_of(i * BLOCK, BLOCK), BLOCK)
            x_ref[there, here] = jnp.zeros((BLOCK, BLOCK), jnp.float32)
            x_ref[there, :] = x_ref[there, :] - dot(x_ref[here, there], x_ref[here, :], (0, 0))
            return carry

        return lax.fori_loop(k + 1, blocks, update, carry)

    for i in range(1, blocks):
        x_ref[BLOCK * i : BLOCK * (i + 1), : BLOCK * i] = jnp.zeros((BLOCK, BLOCK * i), jnp.float32)
    lax.fori_loop(0, blocks, step, 0)
    for i in range(blocks - 1):
        x_ref[BLOCK * i : BLOCK * (i + 1), BLOCK * (i + 1) :] = jnp.zeros(
            (BLOCK, BLOCK * (blocks - 1 - i)), jnp.float32
        )


def inverse_cholesky(s, size):
    return pl.pallas_call(
        factor_kernel,
        out_shape=jax.ShapeDtypeStruct((size, size), jnp.float32),
        in_specs=[WHOLE],
        out_specs=WHOLE,
        name="inverse_factor",
        cost_estimate=pl.CostEstimate(
            flops=20_000_000_000, bytes_accessed=2 * size * size * 4, transcendentals=size
        ),
    )(s)


def joined(ref):
    return jnp.concatenate([ref[b] for b in range(ref.shape[0])], axis=1)


def write_gram(v, xi, s_ref, c_ref):
    blocks = v.shape[1] // BLOCK
    at = 0
    for i in range(blocks):
        row = dot(v[:, BLOCK * i : BLOCK * (i + 1)], v[:, BLOCK * i :], (0, 0))
        for j in range(blocks - i):
            s_ref[BLOCK * at : BLOCK * (at + 1), :] = row[:, BLOCK * j : BLOCK * (j + 1)]
            at += 1
    c = dot(xi, v, (0, 0))
    for j in range(blocks):
        c_ref[j] = c[:, BLOCK * j : BLOCK * (j + 1)]


def gram_kernel(v_ref, xi_ref, s_ref, c_ref):
    write_gram(joined(v_ref), joined(xi_ref), s_ref, c_ref)


def stepped(vp, w, totals, blocks):
    rayleigh, energy, weight = (
        jnp.concatenate([totals[blocks * k + b : blocks * k + b + 1] for b in range(blocks)], axis=1)
        for k in range(3)
    )
    squared = energy - 2.0 * rayleigh * rayleigh + rayleigh * rayleigh * weight
    squared = jnp.maximum(squared, 0.0)
    factor = STEP_LENGTH / jnp.sqrt(squared + NORM_EPS)
    return vp - (w - rayleigh * vp) * factor, squared


def step_kernel(vp_ref, w_ref, sums_ref, xi_ref, v_ref, totals_ref, s_ref, c_ref):
    blocks = vp_ref.shape[0]
    totals = jnp.sum(sums_ref[...], axis=0)
    v, squared = stepped(joined(vp_ref), joined(w_ref), totals, blocks)
    for b in range(blocks):
        v_ref[b] = v[:, BLOCK * b : BLOCK * (b + 1)]
    totals_ref[...] = totals
    write_gram(v, joined(xi_ref), s_ref, c_ref)


def last_kernel(vp_ref, w_ref, sums_ref, v_ref, totals_ref):
    blocks = vp_ref.shape[0]
    totals = jnp.sum(sums_ref[...], axis=0)
    v, squared = stepped(joined(vp_ref), joined(w_ref), totals, blocks)
    for b in range(blocks):
        v_ref[b] = v[:, BLOCK * b : BLOCK * (b + 1)]
    totals_ref[...] = totals


def transform_kernel(x_ref, c_ref, v_ref, u_ref, xi_ref, vp_ref, w_ref, sums_ref):
    blocks = v_ref.shape[0]
    x = x_ref[...]
    vp = dot(joined(v_ref), x, (1, 1))
    z = joined(u_ref) - dot(joined(xi_ref), joined(c_ref), (1, 0))
    w = dot(z, x, (1, 1))
    for b in range(blocks):
        vp_ref[b] = vp[:, BLOCK * b : BLOCK * (b + 1)]
        w_ref[b] = w[:, BLOCK * b : BLOCK * (b + 1)]
    for k, product in enumerate((vp * w, w * w, vp * vp)):
        total = jnp.sum(product, axis=0, keepdims=True)
        for b in range(blocks):
            sums_ref[blocks * k + b : blocks * k + b + 1, :] = total[:, BLOCK * b : BLOCK * (b + 1)]


def stencil_kernel(v_ref, below_ref, above_ref, left_ref, right_ref, p_ref, u_ref):
    planes, rows = v_ref.shape[1:3]
    along_z = [(below_ref, z) for z in range(planes)] + [(v_ref, z) for z in range(planes)]
    along_z += [(above_ref, z) for z in range(planes)]
    along_x = [(left_ref, x) for x in range(rows)] + [(v_ref, x) for x in range(rows)]
    along_x += [(right_ref, x) for x in range(rows)]
    for z in range(planes):
        for x in range(rows):
            centre = v_ref[0, z, x]
            count = centre.shape[0]
            total = 3.0 * STENCIL[0] * centre
            for d in range(1, 5):
                group = pltpu.roll(centre, d, 0) + pltpu.roll(centre, count - d, 0)
                for way in (d, -d):
                    ref, at = along_z[planes + z + way]
                    group = group + ref[0, at, x]
                    ref, at = along_x[rows + x + way]
                    group = group + ref[0, z, at]
                total = total + STENCIL[d] * group
            u_ref[0, z, x] = p_ref[z, x] * centre - 0.5 * total


def ring(count, by):
    return [(i, (i + by) % count) for i in range(count)]


def applied(v, potential):
    below = lax.ppermute(v, "grid", ring(lax.axis_size("grid"), 1))
    above = lax.ppermute(v, "grid", ring(lax.axis_size("grid"), -1))
    left = lax.ppermute(v, BAND, ring(lax.axis_size(BAND), 1))
    right = lax.ppermute(v, BAND, ring(lax.axis_size(BAND), -1))
    block = pl.BlockSpec((1, *v.shape[1:]), lambda b: (b, 0, 0, 0, 0))
    return pl.pallas_call(
        stencil_kernel,
        grid=(v.shape[0],),
        out_shape=jax.ShapeDtypeStruct(v.shape, jnp.float32),
        in_specs=[block] * 5 + [pl.BlockSpec(potential.shape, lambda b: (0, 0, 0, 0))],
        out_specs=block,
        name="stencil",
        cost_estimate=pl.CostEstimate(
            flops=30 * v.size, bytes_accessed=24 * v.size, transcendentals=0
        ),
    )(v, below, above, left, right, potential)


def total_everywhere(parts):
    rows, lanes = parts.shape
    count = lax.axis_size(EVERY)
    pieces = parts.reshape(count, rows // count, lanes)
    arrived = lax.all_to_all(pieces, EVERY, split_axis=0, concat_axis=0, tiled=True)
    return from_everyone(arrived.sum(axis=0)).reshape(rows, lanes)


def from_everyone(x):
    copies = jnp.broadcast_to(x, (lax.axis_size(EVERY), *x.shape))
    return lax.all_to_all(copies, EVERY, split_axis=0, concat_axis=0, tiled=True)


def to_cells(field):
    z, x, y, lanes = field.shape
    count = lax.axis_size(BAND)
    pieces = jnp.moveaxis(field.reshape(z, count, x // count, y, lanes), 1, 0)
    return lax.all_to_all(pieces, BAND, split_axis=0, concat_axis=0, tiled=True)


def to_bands(field):
    count, z, x, y, lanes = field.shape
    pieces = lax.all_to_all(field, BAND, split_axis=0, concat_axis=0, tiled=True)
    return jnp.moveaxis(pieces, 0, 1).reshape(z, count * x, y, lanes)


def call(kernel, shapes, *args):
    return pl.pallas_call(
        kernel,
        out_shape=[jax.ShapeDtypeStruct(s, jnp.float32) for s in shapes],
        in_specs=[WHOLE] * len(args),
        out_specs=[WHOLE] * len(shapes),
        name=kernel.__name__,
        cost_estimate=pl.CostEstimate(
            flops=2_000_000_000, bytes_accessed=4 * sum(a.size for a in args), transcendentals=0
        ),
    )(*args)


def local(orbitals, projectors, potential):
    v5 = to_cells(orbitals)
    xi = to_cells(projectors)
    blocks, planes, rows, columns, lanes = v5.shape
    cells = planes * rows * columns
    flat = (blocks, cells, lanes)
    total = blocks * lanes
    xi = xi.reshape(flat)
    band = lax.axis_index(BAND)
    own = lax.dynamic_slice_in_dim(potential, band * rows, rows, 1)
    own = jnp.broadcast_to(own[..., None], (planes, rows, columns, lanes))
    s_shape = (len(pairs_of(blocks)) * BLOCK, BLOCK)
    c_shape = (blocks, total, BLOCK)
    v = v5.reshape(flat)
    s, c = call(gram_kernel, [s_shape, c_shape], v, xi)
    quotient_list = []
    norm_list = []
    for iteration in range(ITERS):
        u = applied(v.reshape(v5.shape), own).reshape(flat)
        s = total_everywhere(s)
        c = total_everywhere(c.reshape(-1, BLOCK)).reshape(c_shape)
        x = inverse_cholesky(s, total)
        vp, w, sums = call(transform_kernel, [flat, flat, (3 * blocks, BLOCK)], x, c, v, u, xi)
        everyone = from_everyone(sums)
        if iteration < ITERS - 1:
            v, totals, s, c = call(
                step_kernel, [flat, sums.shape, s_shape, c_shape], vp, w, everyone, xi
            )
        else:
            v, totals = call(last_kernel, [flat, sums.shape], vp, w, everyone)
        mine = lax.dynamic_slice_in_dim(totals.reshape(3, blocks, lanes), band, 1, 1)[:, 0]
        rayleigh, energy, weight = mine
        squared = energy - 2.0 * rayleigh * rayleigh + rayleigh * rayleigh * weight
        quotient_list.append(rayleigh)
        norm_list.append(jnp.sqrt(jnp.maximum(squared, 0.0)))
    return (to_bands(v.reshape(v5.shape)), jnp.stack(quotient_list), jnp.stack(norm_list))


def solution(mesh):
    finer = Mesh(mesh.devices.reshape(mesh.shape["grid"], 2, 2), ("grid", "band_0", "band_1"))
    placed = (P("grid", None, None, BAND), P("grid", None, None, BAND), P("grid", None, None))
    return jax.shard_map(
        local,
        mesh=finer,
        in_specs=placed,
        out_specs=(P("grid", None, None, BAND), P(None, BAND), P(None, BAND)),
        check_vma=False,
    )
```

```python
import jax
import jax.numpy as jnp
from jax import lax
from jax.experimental import pallas as pl
from jax.experimental.pallas import tpu as pltpu
from jax.sharding import Mesh
from jax.sharding import PartitionSpec as P

ITERS = 3
BAND = ("band_0", "band_1")
CHIPS = ("grid", "band_0")
BLOCK = 128
TILE = 8

STENCIL = (-205.0 / 72.0, 8.0 / 5.0, -1.0 / 5.0, 8.0 / 315.0, -1.0 / 560.0)
STEP_LENGTH = 0.25
NORM_EPS = 1e-06
HIGHEST = lax.Precision.HIGHEST
WHOLE = pl.BlockSpec(memory_space=pltpu.VMEM)


def dot(left, right, sides):
    return lax.dot_general(
        left, right, ((sides[:1], sides[1:]), ((), ())), precision=HIGHEST,
        preferred_element_type=jnp.float32,
    )


def row_of(tile, j):
    return jnp.broadcast_to(tile[j:j + 1, :], tile.shape)

def lane_of(tile, j):
    return jnp.broadcast_to(tile[:, j:j + 1], tile.shape)

def inverse_factor(tiles):
    count = len(tiles)
    lane = lax.broadcasted_iota(jnp.int32, tiles[0].shape, 1)
    sub = lax.broadcasted_iota(jnp.int32, tiles[0].shape, 0)
    tiles = list(tiles)
    for p in range(count):
        base = TILE * p
        inside = (lane >= base) & (lane < base + TILE)
        head = [lane_of(tiles[p], base + j) for j in range(TILE)]
        own = jnp.where(inside, (lane == base + sub).astype(jnp.float32), tiles[p])
        rows, scales, crosses = [], [], []
        for j in range(TILE):
            scale = lax.rsqrt(row_of(head[j], j))
            row = row_of(own, j) * scale
            column = jnp.where(sub > j, head[j] * scale, 0.0)
            own = jnp.where(sub == j, row, own - column * row)
            cross = [None] * TILE
            for k in range(j + 1, TILE):
                cross[k] = row_of(head[k], j) * scale
                head[k] = head[k] - column * cross[k]
            rows.append(row)
            scales.append(scale)
            crosses.append(cross)
        tiles[p] = jnp.where(lane < base + TILE, own, 0.0)
        for t in range(p + 1, count):
            parts = [lane_of(tiles[t], base + j) for j in range(TILE)]
            tile = jnp.where(inside, 0.0, tiles[t])
            for j in range(TILE):
                column = parts[j] * scales[j]
                tile = tile - column * rows[j]
                for k in range(j + 1, TILE):
                    parts[k] = parts[k] - column * crosses[j][k]
            tiles[t] = tile
    return tiles


def pairs_of(blocks):
    return [(i, j) for i in range(blocks) for j in range(i, blocks)]


def fill_symmetric(x_ref, packed_ref):
    blocks = x_ref.shape[0] // BLOCK
    for at, (i, j) in enumerate(pairs_of(blocks)):
        x_ref[BLOCK * i : BLOCK * (i + 1), BLOCK * j : BLOCK * (j + 1)] = packed_ref[
            BLOCK * at : BLOCK * (at + 1), :
        ]
    for i in range(1, blocks):
        x_ref[BLOCK * i : BLOCK * (i + 1), : BLOCK * i] = jnp.zeros((BLOCK, BLOCK * i), jnp.float32)


def factor_kernel(core_ref, mine_ref, other_ref, x_ref):
    blocks = x_ref.shape[0] // BLOCK

    @pl.when(core_ref[0] == 0)
    def _():
        fill_symmetric(x_ref, mine_ref)

    @pl.when(core_ref[0] != 0)
    def _():
        fill_symmetric(x_ref, other_ref)

    def step(k, carry):
        here = pl.ds(pl.multiple_of(k * BLOCK, BLOCK), BLOCK)
        tiles = [
            x_ref[pl.ds(pl.multiple_of(k * BLOCK + TILE * t, TILE), TILE), here]
            for t in range(BLOCK // TILE)
        ]
        own = jnp.concatenate(inverse_factor(tiles), axis=0)
        x_ref[here, here] = jnp.eye(BLOCK, dtype=jnp.float32)
        x_ref[here, :] = dot(own, x_ref[here, :], (1, 0))

        def update(i, carry):
            there = pl.ds(pl.multiple_of(i * BLOCK, BLOCK), BLOCK)
            x_ref[there, here] = jnp.zeros((BLOCK, BLOCK), jnp.float32)
            x_ref[there, :] = x_ref[there, :] - dot(x_ref[here, there], x_ref[here, :], (0, 0))
            return carry

        return lax.fori_loop(k + 1, blocks, update, carry)

    lax.fori_loop(0, blocks, step, 0)
    for i in range(blocks - 1):
        x_ref[BLOCK * i : BLOCK * (i + 1), BLOCK * (i + 1) :] = jnp.zeros(
            (BLOCK, BLOCK * (blocks - 1 - i)), jnp.float32
        )


def joined(ref):
    return jnp.concatenate([ref[b] for b in range(ref.shape[0])], axis=1)


def write_gram(v, xi, core, packed_ref, mine_ref, other_ref):
    blocks = v.shape[1] // BLOCK
    at = 0
    for i in range(blocks):
        row = dot(v[:, BLOCK * i : BLOCK * (i + 1)], v[:, BLOCK * i :], (0, 0))
        for j in range(blocks - i):
            packed_ref[BLOCK * at : BLOCK * (at + 1), :] = row[:, BLOCK * j : BLOCK * (j + 1)]
            at += 1
    c = dot(xi, v, (0, 0))
    for j in range(blocks):
        packed_ref[BLOCK * at : BLOCK * (at + blocks), :] = c[:, BLOCK * j : BLOCK * (j + 1)]
        at += blocks
    half = mine_ref.shape[0]
    mine_ref[...] = packed_ref[pl.ds(pl.multiple_of(core * half, TILE), half), :]
    other_ref[...] = packed_ref[pl.ds(pl.multiple_of((1 - core) * half, TILE), half), :]


def gram_kernel(core_ref, v_ref, xi_ref, mine_ref, other_ref, packed_ref):
    write_gram(joined(v_ref), joined(xi_ref), core_ref[0], packed_ref, mine_ref, other_ref)


def totals_of(core, mine_ref, other_ref):
    mine = jnp.sum(mine_ref[...], axis=0)
    other = jnp.sum(other_ref[...], axis=0)
    first = jnp.full(mine.shape, core, jnp.int32) == 0
    return jnp.concatenate([jnp.where(first, mine, other), jnp.where(first, other, mine)], axis=0)


def stepped(vp, w, totals, blocks):
    rayleigh, energy, weight = (
        jnp.concatenate([totals[blocks * k + b : blocks * k + b + 1] for b in range(blocks)], axis=1)
        for k in range(3)
    )
    squared = energy - 2.0 * rayleigh * rayleigh + rayleigh * rayleigh * weight
    squared = jnp.maximum(squared, 0.0)
    factor = STEP_LENGTH / jnp.sqrt(squared + NORM_EPS)
    return vp - (w - rayleigh * vp) * factor


def step_kernel(
    core_ref, vp_ref, w_ref, here_ref, there_ref, xi_ref, v_ref, totals_ref, mine_ref, other_ref, packed_ref
):
    blocks = vp_ref.shape[0]
    totals = totals_of(core_ref[0], here_ref, there_ref)
    v = stepped(joined(vp_ref), joined(w_ref), totals, blocks)
    for b in range(blocks):
        v_ref[b] = v[:, BLOCK * b : BLOCK * (b + 1)]
    totals_ref[...] = totals
    write_gram(v, joined(xi_ref), core_ref[0], packed_ref, mine_ref, other_ref)


def last_kernel(core_ref, vp_ref, w_ref, here_ref, there_ref, v_ref, totals_ref):
    blocks = vp_ref.shape[0]
    totals = totals_of(core_ref[0], here_ref, there_ref)
    v = stepped(joined(vp_ref), joined(w_ref), totals, blocks)
    for b in range(blocks):
        v_ref[b] = v[:, BLOCK * b : BLOCK * (b + 1)]
    totals_ref[...] = totals


def fill_coupling(c_ref, first_ref, second_ref):
    blocks = c_ref.shape[1] // BLOCK
    at = len(pairs_of(blocks))
    half = first_ref.shape[0] // BLOCK
    for j in range(blocks):
        for i in range(blocks):
            ref, base = (first_ref, at) if at < half else (second_ref, at - half)
            c_ref[BLOCK * i : BLOCK * (i + 1), BLOCK * j : BLOCK * (j + 1)] = ref[
                BLOCK * base : BLOCK * (base + 1), :
            ]
            at += 1


def transform_kernel(
    core_ref, x_ref, mine_ref, other_ref, v_ref, below_ref, above_ref, left_ref, right_ref, p_ref,
    xi_ref, vp_ref, w_ref, first_ref, second_ref, c_ref, u_ref,
):
    blocks, planes, rows, columns, lanes = v_ref.shape

    @pl.when(core_ref[0] == 0)
    def _():
        fill_coupling(c_ref, mine_ref, other_ref)

    @pl.when(core_ref[0] != 0)
    def _():
        fill_coupling(c_ref, other_ref, mine_ref)

    along_z = [(below_ref, z) for z in range(planes)] + [(v_ref, z) for z in range(planes)]
    along_z += [(above_ref, z) for z in range(planes)]
    along_x = [(left_ref, x) for x in range(rows)] + [(v_ref, x) for x in range(rows)]
    along_x += [(right_ref, x) for x in range(rows)]

    def local_part(b, carry):
        for z in range(planes):
            for x in range(rows):
                centre = v_ref[b, z, x]
                total = 3.0 * STENCIL[0] * centre
                for d in range(1, 5):
                    group = pltpu.roll(centre, d, 0) + pltpu.roll(centre, columns - d, 0)
                    for way in (d, -d):
                        ref, at = along_z[planes + z + way]
                        group = group + ref[b, at, x]
                        ref, at = along_x[rows + x + way]
                        group = group + ref[b, z, at]
                    total = total + STENCIL[d] * group
                u_ref[b, z, x] = p_ref[z, x] * centre - 0.5 * total
        return carry

    lax.fori_loop(0, blocks, local_part, 0)
    x = x_ref[...]
    cells = planes * rows * columns
    v, u = (
        jnp.concatenate([ref[b].reshape(cells, lanes) for b in range(blocks)], axis=1)
        for ref in (v_ref, u_ref)
    )
    vp = dot(v, x, (1, 1))
    w = dot(u - dot(joined(xi_ref), c_ref[...], (1, 0)), x, (1, 1))
    for b in range(blocks):
        vp_ref[b] = vp[:, BLOCK * b : BLOCK * (b + 1)]
        w_ref[b] = w[:, BLOCK * b : BLOCK * (b + 1)]
    lines = []
    for product in (vp * w, w * w, vp * vp):
        total = jnp.sum(product, axis=0, keepdims=True)
        lines += [total[:, BLOCK * b : BLOCK * (b + 1)] for b in range(blocks)]
    half = len(lines) // 2
    first, second = (jnp.concatenate(lines[:half], axis=0), jnp.concatenate(lines[half:], axis=0))
    front = jnp.full(first.shape, core_ref[0], jnp.int32) == 0
    first_ref[...] = jnp.where(front, first, second)
    second_ref[...] = jnp.where(front, second, first)


def ring(count, by):
    return [(i, (i + by) % count) for i in range(count)]


def neighbours(v):
    near, far = lax.axis_size(BAND), lax.axis_size("grid")
    return (
        lax.ppermute(v, "grid", ring(far, 1)),
        lax.ppermute(v, "grid", ring(far, -1)),
        lax.ppermute(v, BAND, ring(near, 1)),
        lax.ppermute(v, BAND, ring(near, -1)),
    )


def swapped(x):
    return lax.ppermute(x, "band_1", ring(lax.axis_size("band_1"), 1))


def exchange(pieces):
    return lax.all_to_all(pieces, CHIPS, split_axis=0, concat_axis=0, tiled=True)


def from_every_chip(x):
    return exchange(jnp.broadcast_to(x, (lax.axis_size(CHIPS), *x.shape)))


def total_everywhere(mine, other):
    rows, lanes = mine.shape
    count = lax.axis_size(CHIPS)
    pieces = (mine + swapped(other)).reshape(count, rows // count, lanes)
    half = from_every_chip(exchange(pieces).sum(axis=0)).reshape(rows, lanes)
    return half, swapped(half)


def to_cells(*fields):
    count = lax.axis_size(BAND)
    z, x, y, lanes = fields[0].shape
    pieces = jnp.stack([f.reshape(z, count, x // count, y, lanes) for f in fields])
    pieces = lax.all_to_all(jnp.moveaxis(pieces, 2, 0), BAND, split_axis=0, concat_axis=0, tiled=True)
    return [pieces[:, at] for at in range(len(fields))]


def to_bands(field):
    count, z, x, y, lanes = field.shape
    pieces = lax.all_to_all(field, BAND, split_axis=0, concat_axis=0, tiled=True)
    return jnp.moveaxis(pieces, 0, 1).reshape(z, count * x, y, lanes)


def call(kernel, shapes, *args, scratch=(), flops=2_000_000_000):
    core = lax.axis_index("band_1").astype(jnp.int32).reshape(1)
    return pl.pallas_call(
        kernel,
        out_shape=[jax.ShapeDtypeStruct(s, jnp.float32) for s in shapes],
        in_specs=[pl.BlockSpec(memory_space=pltpu.SMEM)] + [WHOLE] * len(args),
        out_specs=[WHOLE] * len(shapes),
        scratch_shapes=[pltpu.VMEM(s, jnp.float32) for s in scratch],
        name=kernel.__name__,
        cost_estimate=pl.CostEstimate(
            flops=flops, bytes_accessed=4 * sum(a.size for a in args), transcendentals=0
        ),
    )(core, *args)


def local(orbitals, projectors, potential):
    v, xi = to_cells(orbitals, projectors)
    full = v.shape
    blocks, planes, rows, columns, lanes = full
    cells = planes * rows * columns
    flat = (blocks, cells, lanes)
    total = blocks * lanes
    v = v.reshape(flat)
    xi = xi.reshape(flat)
    band = lax.axis_index(BAND)
    own = lax.dynamic_slice_in_dim(potential, band * rows, rows, 1)
    own = jnp.broadcast_to(own[..., None], (planes, rows, columns, lanes))
    packed = (BLOCK * (len(pairs_of(blocks)) + blocks * blocks), BLOCK)
    half = (packed[0] // 2, BLOCK)
    sums = (3 * blocks // 2, BLOCK)
    totals_shape = (3 * blocks, BLOCK)
    mine, other = call(gram_kernel, [half, half], v, xi, scratch=[packed])
    quotient_list = []
    norm_list = []
    for iteration in range(ITERS):
        around = neighbours(v.reshape(full))
        mine, other = total_everywhere(mine, other)
        (x,) = call(factor_kernel, [(total, total)], mine, other, flops=20_000_000_000)
        vp, w, first, second = call(
            transform_kernel, [flat, flat, sums, sums], x, mine, other, v.reshape(full), *around,
            own, xi, scratch=[(total, total), full],
        )
        here = from_every_chip(first + swapped(second))
        there = swapped(here)
        if iteration < ITERS - 1:
            v, totals, mine, other = call(
                step_kernel, [flat, totals_shape, half, half], vp, w, here, there, xi, scratch=[packed]
            )
        else:
            v, totals = call(last_kernel, [flat, totals_shape], vp, w, here, there)
        own_bands = lax.dynamic_slice_in_dim(totals.reshape(3, blocks, lanes), band, 1, 1)[:, 0]
        rayleigh, energy, weight = own_bands
        squared = energy - 2.0 * rayleigh * rayleigh + rayleigh * rayleigh * weight
        quotient_list.append(rayleigh)
        norm_list.append(jnp.sqrt(jnp.maximum(squared, 0.0)))
    return (to_bands(v.reshape(full)), jnp.stack(quotient_list), jnp.stack(norm_list))


def solution(mesh):
    finer = Mesh(mesh.devices.reshape(mesh.shape["grid"], 2, 2), ("grid", "band_0", "band_1"))
    placed = (P("grid", None, None, BAND), P("grid", None, None, BAND), P("grid", None, None))
    return jax.shard_map(
        local,
        mesh=finer,
        in_specs=placed,
        out_specs=(P("grid", None, None, BAND), P(None, BAND), P(None, BAND)),
        check_vma=False,
    )
```

```python
import jax
import jax.numpy as jnp
from jax import lax
from jax.experimental import pallas as pl
from jax.experimental.pallas import tpu as pltpu
from jax.sharding import Mesh
from jax.sharding import PartitionSpec as P

ITERS = 3
BAND = ("band_0", "band_1")
CHIPS = ("grid", "band_0")
BLOCK = 128
TILE = 8

STENCIL = (-205.0 / 72.0, 8.0 / 5.0, -1.0 / 5.0, 8.0 / 315.0, -1.0 / 560.0)
STEP_LENGTH = 0.25
NORM_EPS = 1e-06
HIGHEST = lax.Precision.HIGHEST
WHOLE = pl.BlockSpec(memory_space=pltpu.VMEM)


def split(x):
    high = x.astype(jnp.bfloat16)
    return high, (x - high.astype(jnp.float32)).astype(jnp.bfloat16)


def dot(left, right, sides):
    (lh, ll), (rh, rl) = split(left), split(right)

    def once(a, b):
        return lax.dot_general(
            a, b, ((sides[:1], sides[1:]), ((), ())), preferred_element_type=jnp.float32
        )

    return once(lh, rl) + once(ll, rh) + once(lh, rh)


def full_dot(left, right, sides):
    return lax.dot_general(
        left, right, ((sides[:1], sides[1:]), ((), ())), precision=HIGHEST,
        preferred_element_type=jnp.float32,
    )


def row_of(tile, j):
    return jnp.broadcast_to(tile[j:j + 1, :], tile.shape)

def lane_of(tile, j):
    return jnp.broadcast_to(tile[:, j:j + 1], tile.shape)

def inverse_factor(tiles):
    count = len(tiles)
    lane = lax.broadcasted_iota(jnp.int32, tiles[0].shape, 1)
    sub = lax.broadcasted_iota(jnp.int32, tiles[0].shape, 0)
    tiles = list(tiles)
    for p in range(count):
        base = TILE * p
        inside = (lane >= base) & (lane < base + TILE)
        head = [lane_of(tiles[p], base + j) for j in range(TILE)]
        own = jnp.where(inside, (lane == base + sub).astype(jnp.float32), tiles[p])
        rows, scales, crosses = [], [], []
        for j in range(TILE):
            scale = lax.rsqrt(row_of(head[j], j))
            row = row_of(own, j) * scale
            column = jnp.where(sub > j, head[j] * scale, 0.0)
            own = jnp.where(sub == j, row, own - column * row)
            cross = [None] * TILE
            for k in range(j + 1, TILE):
                cross[k] = row_of(head[k], j) * scale
                head[k] = head[k] - column * cross[k]
            rows.append(row)
            scales.append(scale)
            crosses.append(cross)
        tiles[p] = jnp.where(lane < base + TILE, own, 0.0)
        for t in range(p + 1, count):
            parts = [lane_of(tiles[t], base + j) for j in range(TILE)]
            tile = jnp.where(inside, 0.0, tiles[t])
            for j in range(TILE):
                column = parts[j] * scales[j]
                tile = tile - column * rows[j]
                for k in range(j + 1, TILE):
                    parts[k] = parts[k] - column * crosses[j][k]
            tiles[t] = tile
    return tiles


def pairs_of(blocks):
    return [(i, j) for i in range(blocks) for j in range(i, blocks)]


def cut(x, b):
    return x[:, BLOCK * b : BLOCK * (b + 1)]


def rows_at(ref, at):
    return ref[BLOCK * at : BLOCK * (at + 1), :]


def factorize(x_ref):
    blocks = x_ref.shape[0] // BLOCK
    for i in range(1, blocks):
        x_ref[BLOCK * i : BLOCK * (i + 1), : BLOCK * i] = jnp.zeros((BLOCK, BLOCK * i), jnp.float32)

    def step(k, carry):
        here = pl.ds(pl.multiple_of(k * BLOCK, BLOCK), BLOCK)
        tiles = [
            x_ref[pl.ds(pl.multiple_of(k * BLOCK + TILE * t, TILE), TILE), here]
            for t in range(BLOCK // TILE)
        ]
        own = jnp.concatenate(inverse_factor(tiles), axis=0)
        x_ref[here, here] = jnp.eye(BLOCK, dtype=jnp.float32)
        x_ref[here, :] = full_dot(own, x_ref[here, :], (1, 0))

        def update(i, carry):
            there = pl.ds(pl.multiple_of(i * BLOCK, BLOCK), BLOCK)
            x_ref[there, here] = jnp.zeros((BLOCK, BLOCK), jnp.float32)
            x_ref[there, :] = x_ref[there, :] - full_dot(x_ref[here, there], x_ref[here, :], (0, 0))
            return carry

        return lax.fori_loop(k + 1, blocks, update, carry)

    lax.fori_loop(0, blocks, step, 0)
    for i in range(blocks - 1):
        x_ref[BLOCK * i : BLOCK * (i + 1), BLOCK * (i + 1) :] = jnp.zeros(
            (BLOCK, BLOCK * (blocks - 1 - i)), jnp.float32
        )


def by_core(core_ref, mine_ref, other_ref, do):
    @pl.when(core_ref[0] == 0)
    def _():
        do(mine_ref, other_ref)

    @pl.when(core_ref[0] != 0)
    def _():
        do(other_ref, mine_ref)


def first_factor_kernel(core_ref, mine_ref, other_ref, x_ref):
    blocks = x_ref.shape[0] // BLOCK

    def fill(first_ref, second_ref):
        for at, (i, j) in enumerate(pairs_of(blocks)):
            x_ref[BLOCK * i : BLOCK * (i + 1), BLOCK * j : BLOCK * (j + 1)] = rows_at(first_ref, at)

    by_core(core_ref, mine_ref, other_ref, fill)
    factorize(x_ref)


def squared_of(rayleigh, energy, weight):
    return jnp.maximum(energy - 2.0 * rayleigh * rayleigh + rayleigh * rayleigh * weight, 0.0)


def length_of(squared):
    return STEP_LENGTH / jnp.sqrt(squared + NORM_EPS)


def factor_kernel(core_ref, mine_ref, other_ref, x_ref, stats_ref):
    blocks = x_ref.shape[0] // BLOCK
    pairs = pairs_of(blocks)
    spot = lax.broadcasted_iota(jnp.int32, (BLOCK, BLOCK), 0) == lax.broadcasted_iota(
        jnp.int32, (BLOCK, BLOCK), 1
    )

    def fill(first_ref, second_ref):
        weight_at = blocks * blocks * BLOCK
        parts = {0: [], 1: []}
        for b in range(blocks):
            at = pairs.index((b, b))
            weight = second_ref[weight_at + b : weight_at + b + 1, :]
            for axis in (0, 1):
                rayleigh, energy, share = (
                    jnp.sum(jnp.where(spot, m, 0.0), axis=axis, keepdims=True)
                    for m in (
                        rows_at(first_ref, at),
                        rows_at(first_ref, len(pairs) + at),
                        jnp.broadcast_to(weight, (BLOCK, BLOCK)),
                    )
                )
                squared = squared_of(rayleigh, energy, share)
                length = length_of(squared)
                parts[axis].append((1.0 + rayleigh * length, length, share))
                if axis == 0:
                    stats_ref[b : b + 1, :] = rayleigh
                    stats_ref[blocks + b : blocks + b + 1, :] = squared
        for at, (i, j) in enumerate(pairs):
            a_i, d_i, _ = parts[1][i]
            a_j, d_j, share = parts[0][j]
            value = (d_i * d_j) * rows_at(first_ref, len(pairs) + at) - (
                a_i * d_j + d_i * a_j
            ) * rows_at(first_ref, at)
            if i == j:
                value = value + jnp.where(spot, a_j * a_j * share, 0.0)
            x_ref[BLOCK * i : BLOCK * (i + 1), BLOCK * j : BLOCK * (j + 1)] = value

    by_core(core_ref, mine_ref, other_ref, fill)
    factorize(x_ref)


def joined(ref):
    return jnp.concatenate([ref[b] for b in range(ref.shape[0])], axis=1)


def share_out(core, packed_ref, mine_ref, other_ref):
    half = mine_ref.shape[0]
    mine_ref[...] = packed_ref[pl.ds(pl.multiple_of(core * half, TILE), half), :]
    other_ref[...] = packed_ref[pl.ds(pl.multiple_of((1 - core) * half, TILE), half), :]


def write_pairs(left, right, at, packed_ref):
    blocks = left.shape[1] // BLOCK
    for i in range(blocks):
        row = dot(cut(left, i), right[:, BLOCK * i :], (0, 0))
        for j in range(blocks - i):
            packed_ref[BLOCK * at : BLOCK * (at + 1), :] = cut(row, j)
            at += 1
    return at


def write_coupling(xi, v, at, packed_ref):
    blocks = v.shape[1] // BLOCK
    c = dot(xi, v, (0, 0))
    for j in range(blocks):
        packed_ref[BLOCK * at : BLOCK * (at + blocks), :] = cut(c, j)
        at += blocks
    return at


def gram_kernel(core_ref, v_ref, xi_ref, mine_ref, other_ref, packed_ref):
    v = joined(v_ref)
    at = write_pairs(v, v, 0, packed_ref)
    write_coupling(joined(xi_ref), v, at, packed_ref)
    share_out(core_ref[0], packed_ref, mine_ref, other_ref)


def totals_of(core, mine_ref, other_ref):
    mine = jnp.sum(mine_ref[...], axis=0)
    other = jnp.sum(other_ref[...], axis=0)
    first = jnp.full(mine.shape, core, jnp.int32) == 0
    return jnp.concatenate([jnp.where(first, mine, other), jnp.where(first, other, mine)], axis=0)


def along_lanes(rows, at, blocks):
    return jnp.concatenate([rows[at + b : at + b + 1] for b in range(blocks)], axis=1)


def last_kernel(core_ref, vp_ref, w_ref, here_ref, there_ref, v_ref, stats_ref):
    blocks = vp_ref.shape[0]
    totals = totals_of(core_ref[0], here_ref, there_ref)
    rayleigh, energy, weight = (totals[blocks * k : blocks * (k + 1)] for k in range(3))
    squared = squared_of(rayleigh, energy, weight)
    length = length_of(squared)
    for b in range(blocks):
        vp = vp_ref[b]
        v_ref[b] = vp - (w_ref[b] - rayleigh[b : b + 1] * vp) * length[b : b + 1]
    stats_ref[:blocks, :] = rayleigh
    stats_ref[blocks:, :] = squared


def local_part(v_ref, around, p_ref, u_ref):
    below_ref, above_ref, left_ref, right_ref = around
    blocks, planes, rows, columns, lanes = v_ref.shape
    along_z = [(ref, z) for ref in (below_ref, v_ref, above_ref) for z in range(planes)]
    along_x = [(ref, x) for ref in (left_ref, v_ref, right_ref) for x in range(rows)]

    def one(b, carry):
        for z in range(planes):
            for x in range(rows):
                centre = v_ref[b, z, x]
                total = 3.0 * STENCIL[0] * centre
                for d in range(1, 5):
                    group = pltpu.roll(centre, d, 0) + pltpu.roll(centre, columns - d, 0)
                    for way in (d, -d):
                        ref, at = along_z[planes + z + way]
                        group = group + ref[b, at, x]
                        ref, at = along_x[rows + x + way]
                        group = group + ref[b, z, at]
                    total = total + STENCIL[d] * group
                u_ref[b, z, x] = p_ref[z, x] * centre - 0.5 * total
        return carry

    lax.fori_loop(0, blocks, one, 0)


def flat_lanes(ref):
    blocks, planes, rows, columns, lanes = ref.shape
    return jnp.concatenate(
        [ref[b].reshape(planes * rows * columns, lanes) for b in range(blocks)], axis=1
    )


def fill_coupling(c_ref, first_ref, second_ref, at):
    blocks = c_ref.shape[1] // BLOCK
    half = first_ref.shape[0] // BLOCK
    for j in range(blocks):
        for i in range(blocks):
            ref, base = (first_ref, at) if at < half else (second_ref, at - half)
            c_ref[BLOCK * i : BLOCK * (i + 1), BLOCK * j : BLOCK * (j + 1)] = rows_at(ref, base)
            at += 1


def transformed(v, x):
    middle = x.shape[0] // 2
    return jnp.concatenate(
        [dot(v[:, :middle], x[:middle, :middle], (1, 1)), dot(v, x[middle:, :], (1, 1))], axis=1
    )


def line_sums(product):
    total = jnp.sum(product, axis=0, keepdims=True)
    return [cut(total, b) for b in range(product.shape[1] // BLOCK)]


def finish(core, vp, w, xi, vp_ref, w_ref, packed_ref, mine_ref, other_ref):
    blocks = vp_ref.shape[0]
    for b in range(blocks):
        vp_ref[b] = cut(vp, b)
        w_ref[b] = cut(w, b).reshape(w_ref.shape[1:])
    if packed_ref is None:
        lines = line_sums(vp * w) + line_sums(w * w) + line_sums(vp * vp)
        half = len(lines) // 2
        first, second = (jnp.concatenate(part, axis=0) for part in (lines[:half], lines[half:]))
        front = jnp.full(first.shape, core, jnp.int32) == 0
        mine_ref[...] = jnp.where(front, first, second)
        other_ref[...] = jnp.where(front, second, first)
        return
    at = write_pairs(vp, w, 0, packed_ref)
    at = write_pairs(w, w, at, packed_ref)
    at = write_coupling(xi, w, at, packed_ref)
    packed_ref[BLOCK * at :, :] = jnp.zeros((packed_ref.shape[0] - BLOCK * at, BLOCK), jnp.float32)
    packed_ref[BLOCK * at : BLOCK * at + blocks, :] = jnp.concatenate(line_sums(vp * vp), axis=0)
    share_out(core, packed_ref, mine_ref, other_ref)


def first_transform_kernel(
    core_ref, x_ref, in_mine_ref, in_other_ref, v_ref, below_ref, above_ref, left_ref, right_ref, p_ref,
    xi_ref, vp_ref, w_ref, mine_ref, other_ref, c_ref, u_ref, packed_ref,
):
    blocks = v_ref.shape[0]
    at = len(pairs_of(blocks))
    by_core(core_ref, in_mine_ref, in_other_ref, lambda a, b: fill_coupling(c_ref, a, b, at))
    local_part(v_ref, (below_ref, above_ref, left_ref, right_ref), p_ref, u_ref)
    v = flat_lanes(v_ref)
    xi = joined(xi_ref)
    z = flat_lanes(u_ref) - dot(xi, c_ref[...], (1, 0))
    both = transformed(jnp.concatenate([v, z], axis=0), x_ref[...])
    finish(
        core_ref[0], both[: v.shape[0]], both[v.shape[0] :], xi, vp_ref, w_ref, packed_ref, mine_ref,
        other_ref,
    )


def stepped(vp, w, y, stats, blocks):
    rayleigh = along_lanes(stats, 0, blocks)
    length = length_of(along_lanes(stats, blocks, blocks))
    return vp - (w - rayleigh * vp) * length, w - (y - rayleigh * w) * length


def transform_kernel(
    core_ref, x_ref, stats_ref, in_mine_ref, in_other_ref, old_ref, v_ref, below_ref, above_ref, left_ref,
    right_ref, p_ref, xi_ref, vp_ref, w_ref, mine_ref, other_ref, c_ref, u_ref, packed_ref=None,
):
    blocks = v_ref.shape[0]
    at = 2 * len(pairs_of(blocks))
    by_core(core_ref, in_mine_ref, in_other_ref, lambda a, b: fill_coupling(c_ref, a, b, at))
    local_part(v_ref, (below_ref, above_ref, left_ref, right_ref), p_ref, u_ref)
    xi = joined(xi_ref)
    y = flat_lanes(u_ref) - dot(xi, c_ref[...], (1, 0))
    v, z = stepped(joined(old_ref), flat_lanes(v_ref), y, stats_ref[...], blocks)
    both = transformed(jnp.concatenate([v, z], axis=0), x_ref[...])
    finish(
        core_ref[0], both[: v.shape[0]], both[v.shape[0] :], xi, vp_ref, w_ref, packed_ref, mine_ref,
        other_ref,
    )


def ring(count, by):
    return [(i, (i + by) % count) for i in range(count)]


def neighbours(v):
    near, far = lax.axis_size(BAND), lax.axis_size("grid")
    return (
        lax.ppermute(v, "grid", ring(far, 1)),
        lax.ppermute(v, "grid", ring(far, -1)),
        lax.ppermute(v, BAND, ring(near, 1)),
        lax.ppermute(v, BAND, ring(near, -1)),
    )


def swapped(x):
    return lax.ppermute(x, "band_1", ring(lax.axis_size("band_1"), 1))


def exchange(pieces):
    return lax.all_to_all(pieces, CHIPS, split_axis=0, concat_axis=0, tiled=True)


def from_every_chip(x):
    return exchange(jnp.broadcast_to(x, (lax.axis_size(CHIPS), *x.shape)))


def total_everywhere(mine, other):
    rows, lanes = mine.shape
    count = lax.axis_size(CHIPS)
    pieces = (mine + swapped(other)).reshape(count, rows // count, lanes)
    half = from_every_chip(exchange(pieces).sum(axis=0)).reshape(rows, lanes)
    return half, swapped(half)


def to_cells(*fields):
    count = lax.axis_size(BAND)
    z, x, y, lanes = fields[0].shape
    pieces = jnp.stack([f.reshape(z, count, x // count, y, lanes) for f in fields])
    pieces = lax.all_to_all(jnp.moveaxis(pieces, 2, 0), BAND, split_axis=0, concat_axis=0, tiled=True)
    return [pieces[:, at] for at in range(len(fields))]


def to_bands(field):
    count, z, x, y, lanes = field.shape
    pieces = lax.all_to_all(field, BAND, split_axis=0, concat_axis=0, tiled=True)
    return jnp.moveaxis(pieces, 0, 1).reshape(z, count * x, y, lanes)


def call(kernel, shapes, *args, scratch=(), flops=2_000_000_000):
    core = lax.axis_index("band_1").astype(jnp.int32).reshape(1)
    return pl.pallas_call(
        kernel,
        out_shape=[jax.ShapeDtypeStruct(s, jnp.float32) for s in shapes],
        in_specs=[pl.BlockSpec(memory_space=pltpu.SMEM)] + [WHOLE] * len(args),
        out_specs=[WHOLE] * len(shapes),
        scratch_shapes=[pltpu.VMEM(s, jnp.float32) for s in scratch],
        name=kernel.__name__,
        cost_estimate=pl.CostEstimate(
            flops=flops, bytes_accessed=4 * sum(a.size for a in args), transcendentals=0
        ),
    )(core, *args)


def local(orbitals, projectors, potential):
    v, xi = to_cells(orbitals, projectors)
    full = v.shape
    blocks, planes, rows, columns, lanes = full
    flat = (blocks, planes * rows * columns, lanes)
    total = blocks * lanes
    square = (total, total)
    xi = xi.reshape(flat)
    band = lax.axis_index(BAND)
    own = lax.dynamic_slice_in_dim(potential, band * rows, rows, 1)
    own = jnp.broadcast_to(own[..., None], (planes, rows, columns, lanes))
    pairs = len(pairs_of(blocks))

    def packed(count):
        return (BLOCK * count, BLOCK), (BLOCK * count // 2, BLOCK)

    small, small_half = packed(pairs + blocks * blocks)
    large, large_half = packed(2 * (2 * pairs))
    sums = (3 * blocks // 2, BLOCK)
    stats_shape = (2 * blocks, BLOCK)
    stats_list = []
    around = neighbours(v)
    mine, other = total_everywhere(*call(gram_kernel, [small_half] * 2, v.reshape(flat), xi, scratch=[small]))
    (x,) = call(first_factor_kernel, [square], mine, other, flops=20_000_000_000)
    vp, w, mine, other = call(
        first_transform_kernel, [flat, full, large_half, large_half], x, mine, other, v, *around, own, xi,
        scratch=[square, full, large],
    )
    for iteration in range(1, ITERS):
        around = neighbours(w)
        mine, other = total_everywhere(mine, other)
        x, stats = call(factor_kernel, [square, stats_shape], mine, other, flops=20_000_000_000)
        stats_list.append(stats)
        last = iteration == ITERS - 1
        vp, w, mine, other = call(
            transform_kernel, [flat, full] + [sums if last else large_half] * 2, x, stats, mine, other,
            vp, w, *around, own, xi, scratch=[square, full] + ([] if last else [large]),
        )
    here = from_every_chip(mine + swapped(other))
    v, stats = call(last_kernel, [flat, stats_shape], vp, w.reshape(flat), here, swapped(here))
    stats_list.append(stats)
    stats = jnp.stack(stats_list).reshape(ITERS, 2, blocks, lanes)
    stats = lax.dynamic_slice_in_dim(stats, band, 1, 2)[:, :, 0]
    return (to_bands(v.reshape(full)), stats[:, 0], jnp.sqrt(stats[:, 1]))


def solution(mesh):
    finer = Mesh(mesh.devices.reshape(mesh.shape["grid"], 2, 2), ("grid", "band_0", "band_1"))
    placed = (P("grid", None, None, BAND), P("grid", None, None, BAND), P("grid", None, None))
    return jax.shard_map(
        local,
        mesh=finer,
        in_specs=placed,
        out_specs=(P("grid", None, None, BAND), P(None, BAND), P(None, BAND)),
        check_vma=False,
    )
```

```python
import jax
import jax.numpy as jnp
from jax import lax
from jax.experimental import pallas as pl
from jax.experimental.pallas import tpu as pltpu
from jax.sharding import Mesh
from jax.sharding import PartitionSpec as P

ITERS = 3
BAND = ("band_0", "band_1")
CHIPS = ("grid", "band_0")
BLOCK = 128
TILE = 8
LINES = 2

STENCIL = (-205.0 / 72.0, 8.0 / 5.0, -1.0 / 5.0, 8.0 / 315.0, -1.0 / 560.0)
STEP_LENGTH = 0.25
NORM_EPS = 1e-06
HIGHEST = lax.Precision.HIGHEST
WHOLE = pl.BlockSpec(memory_space=pltpu.VMEM)


def split(x):
    high = x.astype(jnp.bfloat16)
    return high, (x - high.astype(jnp.float32)).astype(jnp.bfloat16)


def dot(left, right, sides):
    (lh, ll), (rh, rl) = split(left), split(right)

    def once(a, b):
        return lax.dot_general(
            a, b, ((sides[:1], sides[1:]), ((), ())), preferred_element_type=jnp.float32
        )

    return once(lh, rl) + once(ll, rh) + once(lh, rh)


def full_dot(left, right, sides):
    return lax.dot_general(
        left, right, ((sides[:1], sides[1:]), ((), ())), precision=HIGHEST,
        preferred_element_type=jnp.float32,
    )


def row_of(tile, j):
    return jnp.broadcast_to(tile[j:j + 1, :], tile.shape)

def lane_of(tile, j):
    return jnp.broadcast_to(tile[:, j:j + 1], tile.shape)

def inverse_factor(tiles):
    count = len(tiles)
    lane = lax.broadcasted_iota(jnp.int32, tiles[0].shape, 1)
    sub = lax.broadcasted_iota(jnp.int32, tiles[0].shape, 0)
    tiles = list(tiles)
    head = [lane_of(tiles[0], j) for j in range(TILE)]
    for p in range(count):
        base = TILE * p
        inside = (lane >= base) & (lane < base + TILE)
        own = jnp.where(inside, (lane == base + sub).astype(jnp.float32), tiles[p])
        ahead = p + 1 < count
        if ahead:
            coming = [lane_of(tiles[p + 1], base + TILE + j) for j in range(TILE)]
        rows, crosses = [], []
        for j in range(TILE):
            scale = lax.rsqrt(row_of(head[j], j))
            row = row_of(own, j) * scale
            column = jnp.where(sub > j, head[j] * scale, 0.0)
            own = jnp.where(sub == j, row, own - column * row)
            cross = [None] * TILE
            for k in range(j + 1, TILE):
                cross[k] = row_of(head[k], j) * scale
                head[k] = head[k] - column * cross[k]
                cross[k] = cross[k] * scale
            rows.append(row * scale)
            crosses.append(cross)
            if ahead:
                if j == 0:
                    parts = [lane_of(tiles[p + 1], base + k) for k in range(TILE)]
                    following = jnp.where(inside, 0.0, tiles[p + 1])
                following = following - parts[j] * rows[j]
                for k in range(j + 1, TILE):
                    parts[k] = parts[k] - parts[j] * crosses[j][k]
                scaled = parts[j] * (scale * scale)
                for k in range(TILE):
                    coming[k] = coming[k] - scaled * row_of(parts[j], k)
        tiles[p] = jnp.where(lane < base + TILE, own, 0.0)
        if ahead:
            tiles[p + 1] = following
            head = coming
        for t in range(p + 2, count):
            parts = [lane_of(tiles[t], base + j) for j in range(TILE)]
            tile = jnp.where(inside, 0.0, tiles[t])
            for j in range(TILE):
                tile = tile - parts[j] * rows[j]
                for k in range(j + 1, TILE):
                    parts[k] = parts[k] - parts[j] * crosses[j][k]
            tiles[t] = tile
    return tiles


def pairs_of(blocks):
    return [(i, j) for i in range(blocks) for j in range(i, blocks)]


def cut(x, b):
    return x[:, BLOCK * b : BLOCK * (b + 1)]


def rows_at(ref, at):
    return ref[BLOCK * at : BLOCK * (at + 1), :]


def block_of(first_ref, second_ref, at):
    half = first_ref.shape[0] // BLOCK
    return rows_at(first_ref, at) if at < half else rows_at(second_ref, at - half)


def factorize(x_ref):
    blocks = x_ref.shape[0] // BLOCK
    for i in range(1, blocks):
        x_ref[BLOCK * i : BLOCK * (i + 1), : BLOCK * i] = jnp.zeros((BLOCK, BLOCK * i), jnp.float32)

    def step(k, carry):
        here = pl.ds(pl.multiple_of(k * BLOCK, BLOCK), BLOCK)
        tiles = [
            x_ref[pl.ds(pl.multiple_of(k * BLOCK + TILE * t, TILE), TILE), here]
            for t in range(BLOCK // TILE)
        ]
        own = jnp.concatenate(inverse_factor(tiles), axis=0)
        x_ref[here, here] = jnp.eye(BLOCK, dtype=jnp.float32)
        x_ref[here, :] = full_dot(own, x_ref[here, :], (1, 0))

        def update(i, carry):
            there = pl.ds(pl.multiple_of(i * BLOCK, BLOCK), BLOCK)
            x_ref[there, here] = jnp.zeros((BLOCK, BLOCK), jnp.float32)
            x_ref[there, :] = x_ref[there, :] - full_dot(x_ref[here, there], x_ref[here, :], (0, 0))
            return carry

        return lax.fori_loop(k + 1, blocks, update, carry)

    lax.fori_loop(0, blocks, step, 0)
    for i in range(blocks - 1):
        x_ref[BLOCK * i : BLOCK * (i + 1), BLOCK * (i + 1) :] = jnp.zeros(
            (BLOCK, BLOCK * (blocks - 1 - i)), jnp.float32
        )


def by_core(core_ref, mine_ref, other_ref, do):
    @pl.when(core_ref[0] == 0)
    def _():
        do(mine_ref, other_ref)

    @pl.when(core_ref[0] != 0)
    def _():
        do(other_ref, mine_ref)


def first_factor_kernel(core_ref, mine_ref, other_ref, x_ref):
    blocks = x_ref.shape[0] // BLOCK

    def fill(first_ref, second_ref):
        for at, (i, j) in enumerate(pairs_of(blocks)):
            x_ref[BLOCK * i : BLOCK * (i + 1), BLOCK * j : BLOCK * (j + 1)] = rows_at(first_ref, at)

    by_core(core_ref, mine_ref, other_ref, fill)
    factorize(x_ref)


def squared_of(rayleigh, energy, weight):
    return jnp.maximum(energy - 2.0 * rayleigh * rayleigh + rayleigh * rayleigh * weight, 0.0)


def length_of(squared):
    return STEP_LENGTH / jnp.sqrt(squared + NORM_EPS)


def factor_kernel(core_ref, mine_ref, other_ref, x_ref, stats_ref):
    blocks = x_ref.shape[0] // BLOCK
    pairs = pairs_of(blocks)
    spot = lax.broadcasted_iota(jnp.int32, (BLOCK, BLOCK), 0) == lax.broadcasted_iota(
        jnp.int32, (BLOCK, BLOCK), 1
    )

    def fill(first_ref, second_ref):
        weight_at = (2 * len(pairs) + blocks * blocks) * BLOCK - first_ref.shape[0]
        parts = {0: [], 1: []}
        for b in range(blocks):
            at = pairs.index((b, b))
            weight = second_ref[weight_at + b : weight_at + b + 1, :]
            for axis in (0, 1):
                rayleigh, energy, share = (
                    jnp.sum(jnp.where(spot, m, 0.0), axis=axis, keepdims=True)
                    for m in (
                        rows_at(first_ref, at),
                        block_of(first_ref, second_ref, len(pairs) + at),
                        jnp.broadcast_to(weight, (BLOCK, BLOCK)),
                    )
                )
                squared = squared_of(rayleigh, energy, share)
                length = length_of(squared)
                parts[axis].append((1.0 + rayleigh * length, length, share))
                if axis == 0:
                    stats_ref[b : b + 1, :] = rayleigh
                    stats_ref[blocks + b : blocks + b + 1, :] = squared
        for at, (i, j) in enumerate(pairs):
            a_i, d_i, _ = parts[1][i]
            a_j, d_j, share = parts[0][j]
            value = (d_i * d_j) * block_of(first_ref, second_ref, len(pairs) + at) - (
                a_i * d_j + d_i * a_j
            ) * rows_at(first_ref, at)
            if i == j:
                value = value + jnp.where(spot, a_j * a_j * share, 0.0)
            x_ref[BLOCK * i : BLOCK * (i + 1), BLOCK * j : BLOCK * (j + 1)] = value

    by_core(core_ref, mine_ref, other_ref, fill)
    factorize(x_ref)


def joined(ref):
    return jnp.concatenate([ref[b] for b in range(ref.shape[0])], axis=1)


def share_out(core, packed_ref, mine_ref, other_ref):
    half = mine_ref.shape[0]
    mine_ref[...] = packed_ref[pl.ds(pl.multiple_of(core * half, TILE), half), :]
    other_ref[...] = packed_ref[pl.ds(pl.multiple_of((1 - core) * half, TILE), half), :]


def write_pairs(left, right, at, packed_ref):
    blocks = left.shape[1] // BLOCK
    for i in range(blocks):
        row = dot(cut(left, i), right[:, BLOCK * i :], (0, 0))
        for j in range(blocks - i):
            packed_ref[BLOCK * at : BLOCK * (at + 1), :] = cut(row, j)
            at += 1
    return at


def write_coupling(xi, v, at, packed_ref):
    blocks = v.shape[1] // BLOCK
    c = dot(xi, v, (0, 0))
    for j in range(blocks):
        packed_ref[BLOCK * at : BLOCK * (at + blocks), :] = cut(c, j)
        at += blocks
    return at


def gram_kernel(core_ref, v_ref, xi_ref, mine_ref, other_ref, packed_ref):
    v = joined(v_ref)
    at = write_pairs(v, v, 0, packed_ref)
    write_coupling(joined(xi_ref), v, at, packed_ref)
    share_out(core_ref[0], packed_ref, mine_ref, other_ref)


def totals_of(core, mine_ref, other_ref):
    mine = jnp.sum(mine_ref[...], axis=0)
    other = jnp.sum(other_ref[...], axis=0)
    first = jnp.full(mine.shape, core, jnp.int32) == 0
    return jnp.concatenate([jnp.where(first, mine, other), jnp.where(first, other, mine)], axis=0)


def along_lanes(rows, at, blocks):
    return jnp.concatenate([rows[at + b : at + b + 1] for b in range(blocks)], axis=1)


def last_kernel(core_ref, vp_ref, w_ref, here_ref, there_ref, v_ref, stats_ref):
    blocks = vp_ref.shape[0]
    totals = totals_of(core_ref[0], here_ref, there_ref)
    rayleigh, energy, weight = (totals[blocks * k : blocks * (k + 1)] for k in range(3))
    squared = squared_of(rayleigh, energy, weight)
    length = length_of(squared)
    for b in range(blocks):
        vp = vp_ref[b]
        v_ref[b] = vp - (w_ref[b] - rayleigh[b : b + 1] * vp) * length[b : b + 1]
    stats_ref[:blocks, :] = rayleigh
    stats_ref[blocks:, :] = squared


def local_part(v_ref, around, p_ref, u_ref):
    below_ref, above_ref, left_ref, right_ref = around
    blocks, planes, rows, columns, lanes = v_ref.shape
    along_z = [(ref, z) for ref in (below_ref, v_ref, above_ref) for z in range(planes)]
    along_x = [(ref, x) for ref in (left_ref, v_ref, right_ref) for x in range(rows)]

    def one(b, carry):
        for z in range(planes):
            for x in range(rows):
                centre = v_ref[b, z, x]
                total = 3.0 * STENCIL[0] * centre
                for d in range(1, 5):
                    group = pltpu.roll(centre, d, 0) + pltpu.roll(centre, columns - d, 0)
                    for way in (d, -d):
                        ref, at = along_z[planes + z + way]
                        group = group + ref[b, at, x]
                        ref, at = along_x[rows + x + way]
                        group = group + ref[b, z, at]
                    total = total + STENCIL[d] * group
                u_ref[b, z, x] = p_ref[z, x] * centre - 0.5 * total
        return carry

    lax.fori_loop(0, blocks, one, 0)


def flat_lanes(ref):
    blocks, planes, rows, columns, lanes = ref.shape
    return jnp.concatenate(
        [ref[b].reshape(planes * rows * columns, lanes) for b in range(blocks)], axis=1
    )


def fill_coupling(c_ref, first_ref, second_ref, at):
    blocks = c_ref.shape[1] // BLOCK
    for j in range(blocks):
        for i in range(blocks):
            c_ref[BLOCK * i : BLOCK * (i + 1), BLOCK * j : BLOCK * (j + 1)] = block_of(
                first_ref, second_ref, at
            )
            at += 1


def transformed(v, x):
    middle = x.shape[0] // 2
    return jnp.concatenate(
        [dot(v[:, :middle], x[:middle, :middle], (1, 1)), dot(v, x[middle:, :], (1, 1))], axis=1
    )


def line_sums(product):
    total = jnp.sum(product, axis=0, keepdims=True)
    return [cut(total, b) for b in range(product.shape[1] // BLOCK)]


def finish(core, vp, w, xi, vp_ref, w_ref, packed_ref, mine_ref, other_ref):
    blocks = vp_ref.shape[0]
    for b in range(blocks):
        vp_ref[b] = cut(vp, b)
        w_ref[b] = cut(w, b).reshape(w_ref.shape[1:])
    if packed_ref is None:
        lines = line_sums(vp * w) + line_sums(w * w) + line_sums(vp * vp)
        half = len(lines) // 2
        first, second = (jnp.concatenate(part, axis=0) for part in (lines[:half], lines[half:]))
        front = jnp.full(first.shape, core, jnp.int32) == 0
        mine_ref[...] = jnp.where(front, first, second)
        other_ref[...] = jnp.where(front, second, first)
        return
    at = write_pairs(vp, w, 0, packed_ref)
    at = write_pairs(w, w, at, packed_ref)
    at = write_coupling(xi, w, at, packed_ref)
    packed_ref[BLOCK * at :, :] = jnp.zeros((packed_ref.shape[0] - BLOCK * at, BLOCK), jnp.float32)
    packed_ref[BLOCK * at : BLOCK * at + blocks, :] = jnp.concatenate(line_sums(vp * vp), axis=0)
    share_out(core, packed_ref, mine_ref, other_ref)


def first_transform_kernel(
    core_ref, x_ref, in_mine_ref, in_other_ref, v_ref, below_ref, above_ref, left_ref, right_ref, p_ref,
    xi_ref, vp_ref, w_ref, mine_ref, other_ref, c_ref, u_ref, packed_ref,
):
    blocks = v_ref.shape[0]
    at = len(pairs_of(blocks))
    by_core(core_ref, in_mine_ref, in_other_ref, lambda a, b: fill_coupling(c_ref, a, b, at))
    local_part(v_ref, (below_ref, above_ref, left_ref, right_ref), p_ref, u_ref)
    v = flat_lanes(v_ref)
    xi = joined(xi_ref)
    z = flat_lanes(u_ref) - dot(xi, c_ref[...], (1, 0))
    both = transformed(jnp.concatenate([v, z], axis=0), x_ref[...])
    finish(
        core_ref[0], both[: v.shape[0]], both[v.shape[0] :], xi, vp_ref, w_ref, packed_ref, mine_ref,
        other_ref,
    )


def stepped(vp, w, y, stats, blocks):
    rayleigh = along_lanes(stats, 0, blocks)
    length = length_of(along_lanes(stats, blocks, blocks))
    return vp - (w - rayleigh * vp) * length, w - (y - rayleigh * w) * length


def transform_kernel(
    core_ref, x_ref, stats_ref, in_mine_ref, in_other_ref, old_ref, v_ref, below_ref, above_ref, left_ref,
    right_ref, p_ref, xi_ref, vp_ref, w_ref, mine_ref, other_ref, c_ref, u_ref, packed_ref=None,
):
    blocks = v_ref.shape[0]
    at = 2 * len(pairs_of(blocks))
    by_core(core_ref, in_mine_ref, in_other_ref, lambda a, b: fill_coupling(c_ref, a, b, at))
    local_part(v_ref, (below_ref, above_ref, left_ref, right_ref), p_ref, u_ref)
    xi = joined(xi_ref)
    y = flat_lanes(u_ref) - dot(xi, c_ref[...], (1, 0))
    v, z = stepped(joined(old_ref), flat_lanes(v_ref), y, stats_ref[...], blocks)
    both = transformed(jnp.concatenate([v, z], axis=0), x_ref[...])
    finish(
        core_ref[0], both[: v.shape[0]], both[v.shape[0] :], xi, vp_ref, w_ref, packed_ref, mine_ref,
        other_ref,
    )


def ring(count, by):
    return [(i, (i + by) % count) for i in range(count)]


def neighbours(v):
    near, far = lax.axis_size(BAND), lax.axis_size("grid")
    return (
        lax.ppermute(v, "grid", ring(far, 1)),
        lax.ppermute(v, "grid", ring(far, -1)),
        lax.ppermute(v, BAND, ring(near, 1)),
        lax.ppermute(v, BAND, ring(near, -1)),
    )


def swapped(x):
    return lax.ppermute(x, "band_1", ring(lax.axis_size("band_1"), 1))


def exchange(pieces):
    return lax.all_to_all(pieces, CHIPS, split_axis=0, concat_axis=0, tiled=True)


def from_every_chip(x):
    count = lax.axis_size(CHIPS)
    copies = jnp.broadcast_to(x, (count, *x.shape)).reshape(count * x.shape[0], *x.shape[1:])
    return exchange(copies)


def total_everywhere(mine, other):
    rows, lanes = mine.shape
    count = lax.axis_size(CHIPS)
    arrived = exchange((mine + swapped(other)).reshape(rows // LINES, LINES, lanes))
    total = arrived.reshape(count, rows // LINES // count, LINES, lanes).sum(axis=0)
    half = from_every_chip(total).reshape(rows, lanes)
    return half, swapped(half)


def to_cells(*fields):
    count = lax.axis_size(BAND)
    z, x, y, lanes = fields[0].shape
    pieces = jnp.stack([f.reshape(z, count, x // count, y, lanes) for f in fields])
    pieces = lax.all_to_all(jnp.moveaxis(pieces, 2, 0), BAND, split_axis=0, concat_axis=0, tiled=True)
    return [pieces[:, at] for at in range(len(fields))]


def to_bands(field):
    count, z, x, y, lanes = field.shape
    pieces = lax.all_to_all(field, BAND, split_axis=0, concat_axis=0, tiled=True)
    return jnp.moveaxis(pieces, 0, 1).reshape(z, count * x, y, lanes)


def call(kernel, shapes, *args, scratch=(), flops=2_000_000_000, room=32):
    core = lax.axis_index("band_1").astype(jnp.int32).reshape(1)
    return pl.pallas_call(
        kernel,
        out_shape=[jax.ShapeDtypeStruct(s, jnp.float32) for s in shapes],
        in_specs=[pl.BlockSpec(memory_space=pltpu.SMEM)] + [WHOLE] * len(args),
        out_specs=[WHOLE] * len(shapes),
        scratch_shapes=[pltpu.VMEM(s, jnp.float32) for s in scratch],
        compiler_params=pltpu.CompilerParams(vmem_limit_bytes=room << 20),
        name=kernel.__name__,
        cost_estimate=pl.CostEstimate(
            flops=flops, bytes_accessed=4 * sum(a.size for a in args), transcendentals=0
        ),
    )(core, *args)


def local(orbitals, projectors, potential):
    v, xi = to_cells(orbitals, projectors)
    full = v.shape
    blocks, planes, rows, columns, lanes = full
    flat = (blocks, planes * rows * columns, lanes)
    total = blocks * lanes
    square = (total, total)
    xi = xi.reshape(flat)
    band = lax.axis_index(BAND)
    own = lax.dynamic_slice_in_dim(potential, band * rows, rows, 1)
    own = jnp.broadcast_to(own[..., None], (planes, rows, columns, lanes))
    pairs = len(pairs_of(blocks))

    def packed(count):
        return (BLOCK * count, BLOCK), (BLOCK * count // 2, BLOCK)

    small, small_half = packed(pairs + blocks * blocks)
    large, large_half = packed(2 * pairs + blocks * blocks + 2)
    sums = (3 * blocks // 2, BLOCK)
    stats_shape = (2 * blocks, BLOCK)
    stats_list = []
    around = neighbours(v)
    mine, other = total_everywhere(*call(gram_kernel, [small_half] * 2, v.reshape(flat), xi, scratch=[small]))
    (x,) = call(first_factor_kernel, [square], mine, other, flops=20_000_000_000, room=16)
    vp, w, mine, other = call(
        first_transform_kernel, [flat, full, large_half, large_half], x, mine, other, v, *around, own, xi,
        scratch=[square, full, large],
    )
    for iteration in range(1, ITERS):
        around = neighbours(w)
        mine, other = total_everywhere(mine, other)
        x, stats = call(factor_kernel, [square, stats_shape], mine, other, flops=20_000_000_000, room=16)
        stats_list.append(stats)
        last = iteration == ITERS - 1
        vp, w, mine, other = call(
            transform_kernel, [flat, full] + [sums if last else large_half] * 2, x, stats, mine, other,
            vp, w, *around, own, xi, scratch=[square, full] + ([] if last else [large]),
        )
    here = from_every_chip((mine + swapped(other)).reshape(-1, LINES, lanes))
    here = here.reshape(lax.axis_size(CHIPS), *sums)
    v, stats = call(last_kernel, [flat, stats_shape], vp, w.reshape(flat), here, swapped(here))
    stats_list.append(stats)
    stats = jnp.stack(stats_list).reshape(ITERS, 2, blocks, lanes)
    stats = lax.dynamic_slice_in_dim(stats, band, 1, 2)[:, :, 0]
    return (to_bands(v.reshape(full)), stats[:, 0], jnp.sqrt(stats[:, 1]))


def solution(mesh):
    finer = Mesh(mesh.devices.reshape(mesh.shape["grid"], 2, 2), ("grid", "band_0", "band_1"))
    placed = (P("grid", None, None, BAND), P("grid", None, None, BAND), P("grid", None, None))
    return jax.shard_map(
        local,
        mesh=finer,
        in_specs=placed,
        out_specs=(P("grid", None, None, BAND), P(None, BAND), P(None, BAND)),
        check_vma=False,
    )
```

```python
import jax
import jax.numpy as jnp
from jax import lax
from jax.experimental import pallas as pl
from jax.experimental.pallas import tpu as pltpu
from jax.sharding import Mesh
from jax.sharding import PartitionSpec as P

ITERS = 3
BAND = ("band_0", "band_1")
CHIPS = ("grid", "band_0")
BLOCK = 128
TILE = 8
LINES = 2

STENCIL = (-205.0 / 72.0, 8.0 / 5.0, -1.0 / 5.0, 8.0 / 315.0, -1.0 / 560.0)
STEP_LENGTH = 0.25
NORM_EPS = 1e-06
WHOLE = pl.BlockSpec(memory_space=pltpu.VMEM)


def split(x):
    high = x.astype(jnp.bfloat16)
    return high, (x - high.astype(jnp.float32)).astype(jnp.bfloat16)


def dot(left, right, sides):
    (lh, ll), (rh, rl) = split(left), split(right)

    def once(a, b):
        return lax.dot_general(
            a, b, ((sides[:1], sides[1:]), ((), ())), preferred_element_type=jnp.float32
        )

    return once(lh, rl) + once(ll, rh) + once(lh, rh)


def row_of(tile, j):
    return jnp.broadcast_to(tile[j:j + 1, :], tile.shape)


def lane_of(tile, j):
    return jnp.broadcast_to(tile[:, j:j + 1], tile.shape)


def inverse_factor(tiles):
    count = len(tiles)
    lane = lax.broadcasted_iota(jnp.int32, tiles[0].shape, 1)
    sub = lax.broadcasted_iota(jnp.int32, tiles[0].shape, 0)
    tiles = list(tiles)
    head = [lane_of(tiles[0], j) for j in range(TILE)]
    for p in range(count):
        base = TILE * p
        inside = (lane >= base) & (lane < base + TILE)
        own = jnp.where(inside, (lane == base + sub).astype(jnp.float32), tiles[p])
        ahead = p + 1 < count
        if ahead:
            coming = [lane_of(tiles[p + 1], base + TILE + j) for j in range(TILE)]
        rows, crosses = [], []
        for j in range(TILE):
            scale = lax.rsqrt(row_of(head[j], j))
            row = row_of(own, j) * scale
            column = jnp.where(sub > j, head[j] * scale, 0.0)
            own = jnp.where(sub == j, row, own - column * row)
            cross = [None] * TILE
            for k in range(j + 1, TILE):
                cross[k] = row_of(head[k], j) * scale
                head[k] = head[k] - column * cross[k]
                cross[k] = cross[k] * scale
            rows.append(row * scale)
            crosses.append(cross)
            if ahead:
                if j == 0:
                    parts = [lane_of(tiles[p + 1], base + k) for k in range(TILE)]
                    following = jnp.where(inside, 0.0, tiles[p + 1])
                following = following - parts[j] * rows[j]
                for k in range(j + 1, TILE):
                    parts[k] = parts[k] - parts[j] * crosses[j][k]
                scaled = parts[j] * (scale * scale)
                for k in range(TILE):
                    coming[k] = coming[k] - scaled * row_of(parts[j], k)
        tiles[p] = jnp.where(lane < base + TILE, own, 0.0)
        if ahead:
            tiles[p + 1] = following
            head = coming
        for t in range(p + 2, count):
            parts = [lane_of(tiles[t], base + j) for j in range(TILE)]
            tile = jnp.where(inside, 0.0, tiles[t])
            for j in range(TILE):
                tile = tile - parts[j] * rows[j]
                for k in range(j + 1, TILE):
                    parts[k] = parts[k] - parts[j] * crosses[j][k]
            tiles[t] = tile
    return tiles


def pairs_of(blocks):
    return [(i, j) for i in range(blocks) for j in range(i, blocks)]


def cut(x, b):
    return x[:, BLOCK * b : BLOCK * (b + 1)]


def rows_at(ref, at):
    return ref[BLOCK * at : BLOCK * (at + 1), :]


def block_of(first_ref, second_ref, at):
    half = first_ref.shape[0] // BLOCK
    return rows_at(first_ref, at) if at < half else rows_at(second_ref, at - half)


def factorize(x_ref):
    blocks = x_ref.shape[0] // BLOCK
    for i in range(1, blocks):
        x_ref[BLOCK * i : BLOCK * (i + 1), : BLOCK * i] = jnp.zeros((BLOCK, BLOCK * i), jnp.float32)

    def step(k, carry):
        here = pl.ds(pl.multiple_of(k * BLOCK, BLOCK), BLOCK)
        tiles = [
            x_ref[pl.ds(pl.multiple_of(k * BLOCK + TILE * t, TILE), TILE), here]
            for t in range(BLOCK // TILE)
        ]
        own = jnp.concatenate(inverse_factor(tiles), axis=0)
        x_ref[here, here] = jnp.eye(BLOCK, dtype=jnp.float32)
        x_ref[here, :] = dot(own, x_ref[here, :], (1, 0))

        def update(i, carry):
            there = pl.ds(pl.multiple_of(i * BLOCK, BLOCK), BLOCK)
            x_ref[there, here] = jnp.zeros((BLOCK, BLOCK), jnp.float32)
            x_ref[there, :] = x_ref[there, :] - dot(x_ref[here, there], x_ref[here, :], (0, 0))
            return carry

        return lax.fori_loop(k + 1, blocks, update, carry)

    lax.fori_loop(0, blocks, step, 0)
    for i in range(blocks - 1):
        x_ref[BLOCK * i : BLOCK * (i + 1), BLOCK * (i + 1) :] = jnp.zeros(
            (BLOCK, BLOCK * (blocks - 1 - i)), jnp.float32
        )


def by_core(core_ref, mine_ref, other_ref, do):
    @pl.when(core_ref[0] == 0)
    def _():
        do(mine_ref, other_ref)

    @pl.when(core_ref[0] != 0)
    def _():
        do(other_ref, mine_ref)


def first_factor_kernel(core_ref, mine_ref, other_ref, x_ref):
    blocks = x_ref.shape[0] // BLOCK

    def fill(first_ref, second_ref):
        for at, (i, j) in enumerate(pairs_of(blocks)):
            x_ref[BLOCK * i : BLOCK * (i + 1), BLOCK * j : BLOCK * (j + 1)] = rows_at(first_ref, at)

    by_core(core_ref, mine_ref, other_ref, fill)
    factorize(x_ref)


def squared_of(rayleigh, energy, weight):
    return jnp.maximum(energy - 2.0 * rayleigh * rayleigh + rayleigh * rayleigh * weight, 0.0)


def length_of(squared):
    return STEP_LENGTH / jnp.sqrt(squared + NORM_EPS)


def factor_kernel(core_ref, mine_ref, other_ref, x_ref, stats_ref):
    blocks = x_ref.shape[0] // BLOCK
    pairs = pairs_of(blocks)
    spot = lax.broadcasted_iota(jnp.int32, (BLOCK, BLOCK), 0) == lax.broadcasted_iota(
        jnp.int32, (BLOCK, BLOCK), 1
    )

    def fill(first_ref, second_ref):
        weight_at = (2 * len(pairs) + blocks * blocks) * BLOCK - first_ref.shape[0]
        parts = {0: [], 1: []}
        for b in range(blocks):
            at = pairs.index((b, b))
            weight = second_ref[weight_at + b : weight_at + b + 1, :]
            for axis in (0, 1):
                rayleigh, energy, share = (
                    jnp.sum(jnp.where(spot, m, 0.0), axis=axis, keepdims=True)
                    for m in (
                        rows_at(first_ref, at),
                        block_of(first_ref, second_ref, len(pairs) + at),
                        jnp.broadcast_to(weight, (BLOCK, BLOCK)),
                    )
                )
                squared = squared_of(rayleigh, energy, share)
                length = length_of(squared)
                parts[axis].append((1.0 + rayleigh * length, length, share))
                if axis == 0:
                    stats_ref[b : b + 1, :] = rayleigh
                    stats_ref[blocks + b : blocks + b + 1, :] = squared
        for at, (i, j) in enumerate(pairs):
            a_i, d_i, _ = parts[1][i]
            a_j, d_j, share = parts[0][j]
            value = (d_i * d_j) * block_of(first_ref, second_ref, len(pairs) + at) - (
                a_i * d_j + d_i * a_j
            ) * rows_at(first_ref, at)
            if i == j:
                value = value + jnp.where(spot, a_j * a_j * share, 0.0)
            x_ref[BLOCK * i : BLOCK * (i + 1), BLOCK * j : BLOCK * (j + 1)] = value

    by_core(core_ref, mine_ref, other_ref, fill)
    factorize(x_ref)


def joined(ref):
    return jnp.concatenate([ref[b] for b in range(ref.shape[0])], axis=1)


def share_out(core, packed_ref, mine_ref, other_ref):
    half = mine_ref.shape[0]
    mine_ref[...] = packed_ref[pl.ds(pl.multiple_of(core * half, TILE), half), :]
    other_ref[...] = packed_ref[pl.ds(pl.multiple_of((1 - core) * half, TILE), half), :]


def write_pairs(left, right, at, packed_ref):
    blocks = left.shape[1] // BLOCK
    for i in range(blocks):
        row = dot(cut(left, i), right[:, BLOCK * i :], (0, 0))
        for j in range(blocks - i):
            packed_ref[BLOCK * at : BLOCK * (at + 1), :] = cut(row, j)
            at += 1
    return at


def write_coupling(xi, v, at, packed_ref):
    blocks = v.shape[1] // BLOCK
    c = dot(xi, v, (0, 0))
    for j in range(blocks):
        packed_ref[BLOCK * at : BLOCK * (at + blocks), :] = cut(c, j)
        at += blocks
    return at


def gram_kernel(core_ref, v_ref, xi_ref, mine_ref, other_ref, packed_ref):
    v = joined(v_ref)
    at = write_pairs(v, v, 0, packed_ref)
    write_coupling(joined(xi_ref), v, at, packed_ref)
    share_out(core_ref[0], packed_ref, mine_ref, other_ref)


def totals_of(core, mine_ref, other_ref):
    mine = jnp.sum(mine_ref[...], axis=0)
    other = jnp.sum(other_ref[...], axis=0)
    first = jnp.full(mine.shape, core, jnp.int32) == 0
    return jnp.concatenate([jnp.where(first, mine, other), jnp.where(first, other, mine)], axis=0)


def along_lanes(rows, at, blocks):
    return jnp.concatenate([rows[at + b : at + b + 1] for b in range(blocks)], axis=1)


def last_kernel(core_ref, own_ref, near_ref, across_ref, far_ref, here_ref, there_ref, v_ref, stats_ref):
    planes, rows = own_ref.shape[1:3]
    totals = totals_of(core_ref[0], here_ref, there_ref)
    blocks = totals.shape[0] // 3
    rayleigh, energy, weight = (totals[blocks * k : blocks * (k + 1)] for k in range(3))
    stats_ref[:blocks, :] = rayleigh
    stats_ref[blocks:, :] = squared_of(rayleigh, energy, weight)
    rayleigh = stats_ref[pl.ds(core_ref[1], 1), :]
    length = length_of(stats_ref[pl.ds(blocks + core_ref[1], 1), :])
    for away, ref in enumerate((own_ref, near_ref, across_ref, far_ref)):
        first_row = rows * lax.rem(core_ref[1] + blocks - away, blocks)
        for z in range(planes):
            for x in range(rows):
                vp = ref[0, z, x]
                v_ref[z, first_row + x] = vp - (ref[1, z, x] - rayleigh * vp) * length


def local_part(v_ref, around, p_ref, u_ref):
    below_ref, above_ref, left_ref, right_ref = around
    blocks, planes, rows, columns, _ = v_ref.shape
    along_z = [(ref, z) for ref in (below_ref, v_ref, above_ref) for z in range(planes)]
    along_x = [(ref, x) for ref in (left_ref, v_ref, right_ref) for x in range(rows)]

    def one(b, carry):
        for z in range(planes):
            for x in range(rows):
                centre = v_ref[b, z, x]
                total = 3.0 * STENCIL[0] * centre
                for d in range(1, 5):
                    group = pltpu.roll(centre, d, 0) + pltpu.roll(centre, columns - d, 0)
                    for way in (d, -d):
                        ref, at = along_z[planes + z + way]
                        group = group + ref[b, at, x]
                        ref, at = along_x[rows + x + way]
                        group = group + ref[b, z, at]
                    total = total + STENCIL[d] * group
                u_ref[b, z, x] = p_ref[z, x] * centre - 0.5 * total
        return carry

    lax.fori_loop(0, blocks, one, 0)


def flat_lanes(ref):
    blocks, planes, rows, columns, lanes = ref.shape
    return jnp.concatenate(
        [ref[b].reshape(planes * rows * columns, lanes) for b in range(blocks)], axis=1
    )


def fill_coupling(c_ref, first_ref, second_ref, at):
    blocks = c_ref.shape[1] // BLOCK
    for j in range(blocks):
        for i in range(blocks):
            c_ref[BLOCK * i : BLOCK * (i + 1), BLOCK * j : BLOCK * (j + 1)] = block_of(
                first_ref, second_ref, at
            )
            at += 1


def transformed(v, x):
    middle = x.shape[0] // 2
    return jnp.concatenate(
        [dot(v[:, :middle], x[:middle, :middle], (1, 1)), dot(v, x[middle:, :], (1, 1))], axis=1
    )


def line_sums(product):
    total = jnp.sum(product, axis=0, keepdims=True)
    return [cut(total, b) for b in range(product.shape[1] // BLOCK)]


def finish(core, band, vp, w, xi, vp_ref, w_ref, packed_ref, mine_ref, other_ref):
    blocks = vp.shape[1] // BLOCK
    if packed_ref is None:
        for b in range(blocks):
            away = lax.rem(b + blocks - band, blocks)
            vp_ref[away, 0] = cut(vp, b).reshape(vp_ref.shape[2:])
            vp_ref[away, 1] = cut(w, b).reshape(vp_ref.shape[2:])
        lines = line_sums(vp * w) + line_sums(w * w) + line_sums(vp * vp)
        half = len(lines) // 2
        first, second = (jnp.concatenate(part, axis=0) for part in (lines[:half], lines[half:]))
        front = jnp.full(first.shape, core, jnp.int32) == 0
        mine_ref[...] = jnp.where(front, first, second)
        other_ref[...] = jnp.where(front, second, first)
        return
    for b in range(blocks):
        vp_ref[b] = cut(vp, b)
        w_ref[b] = cut(w, b).reshape(w_ref.shape[1:])
    at = write_pairs(vp, w, 0, packed_ref)
    at = write_pairs(w, w, at, packed_ref)
    at = write_coupling(xi, w, at, packed_ref)
    packed_ref[BLOCK * at :, :] = jnp.zeros((packed_ref.shape[0] - BLOCK * at, BLOCK), jnp.float32)
    packed_ref[BLOCK * at : BLOCK * at + blocks, :] = jnp.concatenate(line_sums(vp * vp), axis=0)
    share_out(core, packed_ref, mine_ref, other_ref)


def first_transform_kernel(
    core_ref, x_ref, in_mine_ref, in_other_ref, v_ref, below_ref, above_ref, left_ref, right_ref, p_ref,
    xi_ref, vp_ref, w_ref, mine_ref, other_ref, c_ref, u_ref, packed_ref,
):
    blocks = v_ref.shape[0]
    at = len(pairs_of(blocks))
    by_core(core_ref, in_mine_ref, in_other_ref, lambda a, b: fill_coupling(c_ref, a, b, at))
    local_part(v_ref, (below_ref, above_ref, left_ref, right_ref), p_ref, u_ref)
    v = flat_lanes(v_ref)
    xi = joined(xi_ref)
    z = flat_lanes(u_ref) - dot(xi, c_ref[...], (1, 0))
    both = transformed(jnp.concatenate([v, z], axis=0), x_ref[...])
    finish(
        core_ref[0], core_ref[1], both[: v.shape[0]], both[v.shape[0] :], xi, vp_ref, w_ref, packed_ref, mine_ref,
        other_ref,
    )


def stepped(vp, w, y, stats, blocks):
    rayleigh = along_lanes(stats, 0, blocks)
    length = length_of(along_lanes(stats, blocks, blocks))
    return vp - (w - rayleigh * vp) * length, w - (y - rayleigh * w) * length


def last_transform_kernel(*refs):
    outs = 14
    transform_kernel(*refs[:outs], None, *refs[outs:], None)


def transform_kernel(
    core_ref, x_ref, stats_ref, in_mine_ref, in_other_ref, old_ref, v_ref, below_ref, above_ref, left_ref,
    right_ref, p_ref, xi_ref, vp_ref, w_ref, mine_ref, other_ref, c_ref, u_ref, packed_ref,
):
    blocks = v_ref.shape[0]
    at = 2 * len(pairs_of(blocks))
    by_core(core_ref, in_mine_ref, in_other_ref, lambda a, b: fill_coupling(c_ref, a, b, at))
    local_part(v_ref, (below_ref, above_ref, left_ref, right_ref), p_ref, u_ref)
    xi = joined(xi_ref)
    y = flat_lanes(u_ref) - dot(xi, c_ref[...], (1, 0))
    v, z = stepped(joined(old_ref), flat_lanes(v_ref), y, stats_ref[...], blocks)
    both = transformed(jnp.concatenate([v, z], axis=0), x_ref[...])
    finish(
        core_ref[0], core_ref[1], both[: v.shape[0]], both[v.shape[0] :], xi, vp_ref, w_ref, packed_ref, mine_ref,
        other_ref,
    )


def ring(count, by):
    return [(i, (i + by) % count) for i in range(count)]


def all_neighbours(v):
    near, far = lax.axis_size(BAND), lax.axis_size("grid")
    return (
        lax.ppermute(v, "grid", ring(far, 1)),
        lax.ppermute(v, "grid", ring(far, -1)),
        lax.ppermute(v, BAND, ring(near, 1)),
        lax.ppermute(v, BAND, ring(near, -1)),
    )


def swapped(x):
    return lax.ppermute(x, "band_1", ring(lax.axis_size("band_1"), 1))


def exchange(pieces):
    return lax.all_to_all(pieces, CHIPS, split_axis=0, concat_axis=0, tiled=True)


def from_every_chip(x):
    count = lax.axis_size(CHIPS)
    copies = jnp.broadcast_to(x, (count, *x.shape)).reshape(count * x.shape[0], *x.shape[1:])
    return exchange(copies)


def total_everywhere(mine, other):
    rows, lanes = mine.shape
    count = lax.axis_size(CHIPS)
    pieces = (mine + swapped(other)).reshape(rows // LINES, LINES, lanes)
    arrived = exchange(pieces)
    total = arrived.reshape(count, rows // LINES // count, LINES, lanes).sum(axis=0)
    half = from_every_chip(total).reshape(rows, lanes)
    return half, swapped(half)


def to_cells(*fields):
    count = lax.axis_size(BAND)
    z, x, y, lanes = fields[0].shape
    pieces = jnp.stack([f.reshape(z, count, x // count, y, lanes) for f in fields])
    pieces = lax.all_to_all(jnp.moveaxis(pieces, 2, 0), BAND, split_axis=0, concat_axis=0, tiled=True)
    return [pieces[:, at] for at in range(len(fields))]


def call(kernel, shapes, *args, scratch=(), flops=2_000_000_000, room=32):
    place = jnp.stack([lax.axis_index("band_1"), lax.axis_index(BAND)]).astype(jnp.int32)
    return pl.pallas_call(
        kernel,
        out_shape=[jax.ShapeDtypeStruct(s, jnp.float32) for s in shapes],
        in_specs=[pl.BlockSpec(memory_space=pltpu.SMEM)] + [WHOLE] * len(args),
        out_specs=[WHOLE] * len(shapes),
        scratch_shapes=[pltpu.VMEM(s, jnp.float32) for s in scratch],
        compiler_params=pltpu.CompilerParams(vmem_limit_bytes=room << 20),
        cost_estimate=pl.CostEstimate(
            flops=flops, bytes_accessed=4 * sum(a.size for a in args), transcendentals=0
        ),
    )(place, *args)


def local(orbitals, projectors, potential):
    v, xi = to_cells(orbitals, projectors)
    full = v.shape
    blocks, planes, rows, columns, lanes = full
    flat = (blocks, planes * rows * columns, lanes)
    total = blocks * lanes
    square = (total, total)
    xi = xi.reshape(flat)
    band = lax.axis_index(BAND)
    own = lax.dynamic_slice_in_dim(potential, band * rows, rows, 1)
    own = jnp.broadcast_to(own[..., None], (planes, rows, columns, lanes))
    pairs = len(pairs_of(blocks))

    def packed(count):
        return (BLOCK * count, BLOCK), (BLOCK * count // 2, BLOCK)

    small, small_half = packed(pairs + blocks * blocks)
    large, large_half = packed(2 * pairs + blocks * blocks + 2)
    sums = (3 * blocks // 2, BLOCK)
    stats_shape = (2 * blocks, BLOCK)
    stats_list = []
    around = all_neighbours(v)
    mine, other = total_everywhere(*call(gram_kernel, [small_half] * 2, v.reshape(flat), xi, scratch=[small]))
    (x,) = call(first_factor_kernel, [square], mine, other, flops=20_000_000_000, room=16)
    vp, w, mine, other = call(
        first_transform_kernel, [flat, full, large_half, large_half], x, mine, other, v, *around, own, xi,
        scratch=[square, full, large],
    )
    for iteration in range(1, ITERS):
        around = all_neighbours(w)
        mine, other = total_everywhere(mine, other)
        x, stats = call(factor_kernel, [square, stats_shape], mine, other, flops=20_000_000_000, room=16)
        stats_list.append(stats)
        given = (x, stats, mine, other, vp, w, *around, own, xi)
        if iteration < ITERS - 1:
            vp, w, mine, other = call(
                transform_kernel, [flat, full, large_half, large_half], *given,
                scratch=[square, full, large],
            )
    both = (blocks, 2, planes, rows, columns, lanes)
    parts, mine, other = call(
        last_transform_kernel, [both, sums, sums], *given, scratch=[square, full]
    )
    parts = [parts[0]] + [lax.ppermute(parts[k], BAND, ring(blocks, k)) for k in range(1, blocks)]
    lines = (mine + swapped(other)).reshape(-1, LINES, lanes)
    here = from_every_chip(lines)
    here = here.reshape(lax.axis_size(CHIPS), *sums)
    v, stats = call(
        last_kernel, [(planes, blocks * rows, columns, lanes), stats_shape], *parts, here, swapped(here)
    )
    stats_list.append(stats)
    stats = jnp.stack(stats_list).reshape(ITERS, 2, blocks, lanes)
    stats = lax.dynamic_slice_in_dim(stats, band, 1, 2)[:, :, 0]
    return (v, stats[:, 0], jnp.sqrt(stats[:, 1]))


def solution(mesh):
    finer = Mesh(mesh.devices.reshape(mesh.shape["grid"], 2, 2), ("grid", "band_0", "band_1"))
    placed = (P("grid", None, None, BAND), P("grid", None, None, BAND), P("grid", None, None))
    return jax.shard_map(
        local,
        mesh=finer,
        in_specs=placed,
        out_specs=(P("grid", None, None, BAND), P(None, BAND), P(None, BAND)),
        check_vma=False,
    )
```

```python
import jax
import jax.numpy as jnp
from jax import lax
from jax.experimental import pallas as pl
from jax.experimental.pallas import tpu as pltpu
from jax.sharding import Mesh
from jax.sharding import PartitionSpec as P

ITERS = 3
BAND = ("band_0", "band_1")
CHIPS = ("grid", "band_0")
EVERY = ("grid", "band_0", "band_1")
BLOCK = 128
TILE = 8
HALF = 64
LINES = 2

STENCIL = (-205.0 / 72.0, 8.0 / 5.0, -1.0 / 5.0, 8.0 / 315.0, -1.0 / 560.0)
STEP_LENGTH = 0.25
NORM_EPS = 1e-06
WHOLE = pl.BlockSpec(memory_space=pltpu.VMEM)


def split(x):
    high = x.astype(jnp.bfloat16)
    return high, (x - high.astype(jnp.float32)).astype(jnp.bfloat16)


def dot(left, right, sides):
    (lh, ll), (rh, rl) = split(left), split(right)

    def once(a, b):
        return lax.dot_general(
            a, b, ((sides[:1], sides[1:]), ((), ())), preferred_element_type=jnp.float32
        )

    return once(lh, rl) + once(ll, rh) + once(lh, rh)


def row_of(tile, j):
    return jnp.broadcast_to(tile[j:j + 1, :], tile.shape)


def lane_of(tile, j):
    return jnp.broadcast_to(tile[:, j:j + 1], tile.shape)


def inverse_factor(tiles):
    count = len(tiles)
    lane = lax.broadcasted_iota(jnp.int32, tiles[0].shape, 1)
    sub = lax.broadcasted_iota(jnp.int32, tiles[0].shape, 0)
    tiles = list(tiles)
    head = [lane_of(tiles[0], j) for j in range(TILE)]
    for p in range(count):
        base = TILE * p
        inside = (lane >= base) & (lane < base + TILE)
        own = jnp.where(inside, (lane == base + sub).astype(jnp.float32), tiles[p])
        ahead = p + 1 < count
        if ahead:
            coming = [lane_of(tiles[p + 1], base + TILE + j) for j in range(TILE)]
        rows, crosses = [], []
        for j in range(TILE):
            scale = lax.rsqrt(row_of(head[j], j))
            row = row_of(own, j) * scale
            column = jnp.where(sub > j, head[j] * scale, 0.0)
            own = jnp.where(sub == j, row, own - column * row)
            cross = [None] * TILE
            for k in range(j + 1, TILE):
                cross[k] = row_of(head[k], j) * scale
                head[k] = head[k] - column * cross[k]
                cross[k] = cross[k] * scale
            rows.append(row * scale)
            crosses.append(cross)
            if ahead:
                if j == 0:
                    parts = [lane_of(tiles[p + 1], base + k) for k in range(TILE)]
                    following = jnp.where(inside, 0.0, tiles[p + 1])
                following = following - parts[j] * rows[j]
                for k in range(j + 1, TILE):
                    parts[k] = parts[k] - parts[j] * crosses[j][k]
                scaled = parts[j] * (scale * scale)
                for k in range(TILE):
                    coming[k] = coming[k] - scaled * row_of(parts[j], k)
        tiles[p] = jnp.where((lane < base + TILE) | (lane >= TILE * count), own, 0.0)
        if ahead:
            tiles[p + 1] = following
            head = coming
        for t in range(p + 2, count):
            parts = [lane_of(tiles[t], base + j) for j in range(TILE)]
            tile = jnp.where(inside, 0.0, tiles[t])
            for j in range(TILE):
                tile = tile - parts[j] * rows[j]
                for k in range(j + 1, TILE):
                    parts[k] = parts[k] - parts[j] * crosses[j][k]
            tiles[t] = tile
    return tiles


def pairs_of(blocks):
    return [(i, j) for i in range(blocks) for j in range(i, blocks)]


def cut(x, b):
    return x[:, BLOCK * b : BLOCK * (b + 1)]


def rows_at(ref, at):
    return ref[BLOCK * at : BLOCK * (at + 1), :]


def block_of(core, mine_ref, other_ref, at):
    half = mine_ref.shape[0] // BLOCK
    mine, other = rows_at(mine_ref, at % half), rows_at(other_ref, at % half)
    here = jnp.full(mine.shape, core, jnp.int32) == at // half
    return jnp.where(here, mine, other)


def factorize(x_ref):
    blocks = x_ref.shape[0] // BLOCK
    for i in range(1, blocks):
        x_ref[BLOCK * i : BLOCK * (i + 1), : BLOCK * i] = jnp.zeros((BLOCK, BLOCK * i), jnp.float32)
    block_row = lax.broadcasted_iota(jnp.int32, (BLOCK, BLOCK), 0)
    block_lane = lax.broadcasted_iota(jnp.int32, (BLOCK, BLOCK), 1)

    def step(k, carry):
        first = pl.multiple_of(k * BLOCK, BLOCK)
        here = pl.ds(first, BLOCK)

        def part(h, carry):
            top = first + HALF * h
            rows = [pl.ds(pl.multiple_of(top + TILE * t, TILE), TILE) for t in range(HALF // TILE)]
            tiles = inverse_factor([pltpu.roll(x_ref[r, here], HALF * h, 1) for r in rows])
            for r, tile in zip(rows, tiles):
                x_ref[r, here] = pltpu.roll(tile, HALF * h, 1)

            @pl.when(h == 0)
            def _():
                upper = x_ref[pl.ds(first, HALF), here]
                below = pl.ds(pl.multiple_of(first + HALF, HALF), HALF)
                change = dot(upper, upper, (0, 0))[HALF:, :]
                lane = lax.broadcasted_iota(jnp.int32, change.shape, 1)
                x_ref[below, here] = jnp.where(lane < HALF, 0.0, x_ref[below, here]) - change

            return carry

        lax.fori_loop(0, 2, part, 0)
        own = jnp.where((block_row < HALF) & (block_lane >= HALF), 0.0, x_ref[here, here])
        x_ref[here, here] = jnp.where(block_row == block_lane, 1.0, 0.0)
        x_ref[here, :] = dot(own, x_ref[here, :], (1, 0))

        def update(i, carry):
            there = pl.ds(pl.multiple_of(i * BLOCK, BLOCK), BLOCK)
            x_ref[there, here] = jnp.zeros((BLOCK, BLOCK), jnp.float32)
            x_ref[there, :] = x_ref[there, :] - dot(x_ref[here, there], x_ref[here, :], (0, 0))
            return carry

        return lax.fori_loop(k + 1, blocks, update, carry)

    lax.fori_loop(0, blocks, step, 0)
    for i in range(blocks - 1):
        x_ref[BLOCK * i : BLOCK * (i + 1), BLOCK * (i + 1) :] = jnp.zeros(
            (BLOCK, BLOCK * (blocks - 1 - i)), jnp.float32
        )


def first_factor_kernel(core_ref, mine_ref, other_ref, x_ref):
    blocks = x_ref.shape[0] // BLOCK
    for at, (i, j) in enumerate(pairs_of(blocks)):
        x_ref[BLOCK * i : BLOCK * (i + 1), BLOCK * j : BLOCK * (j + 1)] = block_of(
            core_ref[0], mine_ref, other_ref, at
        )
    factorize(x_ref)


def squared_of(rayleigh, energy, weight):
    return jnp.maximum(energy - 2.0 * rayleigh * rayleigh + rayleigh * rayleigh * weight, 0.0)


def length_of(squared):
    return STEP_LENGTH / jnp.sqrt(squared + NORM_EPS)


def factor_kernel(core_ref, mine_ref, other_ref, x_ref, stats_ref):
    blocks = x_ref.shape[0] // BLOCK
    pairs = pairs_of(blocks)
    spot = lax.broadcasted_iota(jnp.int32, (BLOCK, BLOCK), 0) == lax.broadcasted_iota(
        jnp.int32, (BLOCK, BLOCK), 1
    )

    def block(at):
        return block_of(core_ref[0], mine_ref, other_ref, at)

    weights = block(2 * len(pairs) + blocks * blocks)[:TILE]
    parts = {0: [], 1: []}
    for b in range(blocks):
        at = pairs.index((b, b))
        products, energies = block(at), block(len(pairs) + at)
        weight = jnp.broadcast_to(weights[b : b + 1], (BLOCK, BLOCK))
        for axis in (0, 1):
            rayleigh, energy, share = (
                jnp.sum(jnp.where(spot, m, 0.0), axis=axis, keepdims=True)
                for m in (products, energies, weight)
            )
            squared = squared_of(rayleigh, energy, share)
            length = length_of(squared)
            parts[axis].append((1.0 + rayleigh * length, length, share))
            if axis == 0:
                stats_ref[b : b + 1, :] = rayleigh
                stats_ref[blocks + b : blocks + b + 1, :] = squared
    for at, (i, j) in enumerate(pairs):
        a_i, d_i, _ = parts[1][i]
        a_j, d_j, share = parts[0][j]
        value = (d_i * d_j) * block(len(pairs) + at) - (a_i * d_j + d_i * a_j) * block(at)
        if i == j:
            value = value + jnp.where(spot, a_j * a_j * share, 0.0)
        x_ref[BLOCK * i : BLOCK * (i + 1), BLOCK * j : BLOCK * (j + 1)] = value
    factorize(x_ref)


def joined(ref):
    return jnp.concatenate([ref[b] for b in range(ref.shape[0])], axis=1)


def share_out(core, packed_ref, mine_ref, other_ref):
    half = mine_ref.shape[0]
    mine_ref[...] = packed_ref[pl.ds(pl.multiple_of(core * half, TILE), half), :]
    other_ref[...] = packed_ref[pl.ds(pl.multiple_of((1 - core) * half, TILE), half), :]


def write_pairs(left, right, at, packed_ref):
    blocks = left.shape[1] // BLOCK
    for i in range(blocks):
        row = dot(cut(left, i), right[:, BLOCK * i :], (0, 0))
        for j in range(blocks - i):
            packed_ref[BLOCK * at : BLOCK * (at + 1), :] = cut(row, j)
            at += 1
    return at


def write_coupling(xi, v, at, packed_ref):
    blocks = v.shape[1] // BLOCK
    c = dot(xi, v, (0, 0))
    for j in range(blocks):
        packed_ref[BLOCK * at : BLOCK * (at + blocks), :] = cut(c, j)
        at += blocks
    return at


def gram_kernel(core_ref, v_ref, xi_ref, mine_ref, other_ref, packed_ref):
    v = joined(v_ref)
    at = write_pairs(v, v, 0, packed_ref)
    write_coupling(joined(xi_ref), v, at, packed_ref)
    share_out(core_ref[0], packed_ref, mine_ref, other_ref)


def totals_of(core, mine_ref, other_ref):
    mine = jnp.sum(mine_ref[...], axis=0)
    other = jnp.sum(other_ref[...], axis=0)
    first = jnp.full(mine.shape, core, jnp.int32) == 0
    return jnp.concatenate([jnp.where(first, mine, other), jnp.where(first, other, mine)], axis=0)


def along_lanes(rows, at, blocks):
    return jnp.concatenate([rows[at + b : at + b + 1] for b in range(blocks)], axis=1)


def last_kernel(core_ref, own_ref, near_ref, across_ref, far_ref, here_ref, there_ref, v_ref, stats_ref):
    planes, rows = own_ref.shape[1:3]
    totals = totals_of(core_ref[0], here_ref, there_ref)
    blocks = totals.shape[0] // 3
    rayleigh, energy, weight = (totals[blocks * k : blocks * (k + 1)] for k in range(3))
    stats_ref[:blocks, :] = rayleigh
    stats_ref[blocks:, :] = squared_of(rayleigh, energy, weight)
    rayleigh = stats_ref[pl.ds(core_ref[1], 1), :]
    length = length_of(stats_ref[pl.ds(blocks + core_ref[1], 1), :])
    for away, ref in enumerate((own_ref, near_ref, across_ref, far_ref)):
        first_row = rows * lax.rem(core_ref[1] + core_ref[2] + blocks - away, blocks)
        for z in range(planes):
            for x in range(rows):
                vp = ref[0, z, x]
                v_ref[z, first_row + x] = vp - (ref[1, z, x] - rayleigh * vp) * length


def local_part(v_ref, around, p_ref, u_ref):
    below_ref, above_ref, left_ref, right_ref = around
    blocks, planes, rows, columns, _ = v_ref.shape
    along_z = [(ref, z) for ref in (below_ref, v_ref, above_ref) for z in range(planes)]
    along_x = [(ref, x) for ref in (left_ref, v_ref, right_ref) for x in range(rows)]

    def one(b, carry):
        for z in range(planes):
            for x in range(rows):
                centre = v_ref[b, z, x]
                total = 3.0 * STENCIL[0] * centre
                for d in range(1, 5):
                    group = pltpu.roll(centre, d, 0) + pltpu.roll(centre, columns - d, 0)
                    for way in (d, -d):
                        ref, at = along_z[planes + z + way]
                        group = group + ref[b, at, x]
                        ref, at = along_x[rows + x + way]
                        group = group + ref[b, z, at]
                    total = total + STENCIL[d] * group
                u_ref[b, z, x] = p_ref[z, x] * centre - 0.5 * total
        return carry

    lax.fori_loop(0, blocks, one, 0)


def flat_lanes(ref):
    blocks, planes, rows, columns, lanes = ref.shape
    return jnp.concatenate(
        [ref[b].reshape(planes * rows * columns, lanes) for b in range(blocks)], axis=1
    )


def fill_coupling(c_ref, core, mine_ref, other_ref, at):
    blocks = c_ref.shape[1] // BLOCK
    for j in range(blocks):
        for i in range(blocks):
            c_ref[BLOCK * i : BLOCK * (i + 1), BLOCK * j : BLOCK * (j + 1)] = block_of(
                core, mine_ref, other_ref, at
            )
            at += 1


def transformed(v, x):
    middle = x.shape[0] // 2
    return jnp.concatenate(
        [dot(v[:, :middle], x[:middle, :middle], (1, 1)), dot(v, x[middle:, :], (1, 1))], axis=1
    )


def line_sums(product):
    total = jnp.sum(product, axis=0, keepdims=True)
    return [cut(total, b) for b in range(product.shape[1] // BLOCK)]


def finish(core, band, vp, w, xi, vp_ref, w_ref, packed_ref, mine_ref, other_ref):
    blocks = vp.shape[1] // BLOCK
    if packed_ref is None:
        for b in range(blocks):
            away = lax.rem(b + blocks - band, blocks)
            vp_ref[away, 0] = cut(vp, b).reshape(vp_ref.shape[2:])
            vp_ref[away, 1] = cut(w, b).reshape(vp_ref.shape[2:])
        lines = line_sums(vp * w) + line_sums(w * w) + line_sums(vp * vp)
        half = len(lines) // 2
        first, second = (jnp.concatenate(part, axis=0) for part in (lines[:half], lines[half:]))
        front = jnp.full(first.shape, core, jnp.int32) == 0
        mine_ref[...] = jnp.where(front, first, second)
        other_ref[...] = jnp.where(front, second, first)
        return
    for b in range(blocks):
        vp_ref[b] = cut(vp, b)
        w_ref[b] = cut(w, b).reshape(w_ref.shape[1:])
    at = write_pairs(vp, w, 0, packed_ref)
    at = write_pairs(w, w, at, packed_ref)
    at = write_coupling(xi, w, at, packed_ref)
    packed_ref[BLOCK * at :, :] = jnp.zeros((packed_ref.shape[0] - BLOCK * at, BLOCK), jnp.float32)
    packed_ref[BLOCK * at : BLOCK * at + blocks, :] = jnp.concatenate(line_sums(vp * vp), axis=0)
    share_out(core, packed_ref, mine_ref, other_ref)


def first_transform_kernel(
    core_ref, x_ref, in_mine_ref, in_other_ref, v_ref, below_ref, above_ref, left_ref, right_ref, p_ref,
    xi_ref, vp_ref, w_ref, mine_ref, other_ref, c_ref, u_ref, packed_ref,
):
    blocks = v_ref.shape[0]
    at = len(pairs_of(blocks))
    fill_coupling(c_ref, core_ref[0], in_mine_ref, in_other_ref, at)
    local_part(v_ref, (below_ref, above_ref, left_ref, right_ref), p_ref, u_ref)
    v = flat_lanes(v_ref)
    xi = joined(xi_ref)
    z = flat_lanes(u_ref) - dot(xi, c_ref[...], (1, 0))
    both = transformed(jnp.concatenate([v, z], axis=0), x_ref[...])
    finish(
        core_ref[0], core_ref[1], both[: v.shape[0]], both[v.shape[0] :], xi, vp_ref, w_ref, packed_ref, mine_ref,
        other_ref,
    )


def stepped(vp, w, y, stats, blocks):
    rayleigh = along_lanes(stats, 0, blocks)
    length = length_of(along_lanes(stats, blocks, blocks))
    return vp - (w - rayleigh * vp) * length, w - (y - rayleigh * w) * length


def last_transform_kernel(*refs):
    outs = 14
    transform_kernel(*refs[:outs], None, *refs[outs:], None)


def transform_kernel(
    core_ref, x_ref, stats_ref, in_mine_ref, in_other_ref, old_ref, v_ref, below_ref, above_ref, left_ref,
    right_ref, p_ref, xi_ref, vp_ref, w_ref, mine_ref, other_ref, c_ref, u_ref, packed_ref,
):
    blocks = v_ref.shape[0]
    at = 2 * len(pairs_of(blocks))
    fill_coupling(c_ref, core_ref[0], in_mine_ref, in_other_ref, at)
    local_part(v_ref, (below_ref, above_ref, left_ref, right_ref), p_ref, u_ref)
    xi = joined(xi_ref)
    y = flat_lanes(u_ref) - dot(xi, c_ref[...], (1, 0))
    v, z = stepped(joined(old_ref), flat_lanes(v_ref), y, stats_ref[...], blocks)
    both = transformed(jnp.concatenate([v, z], axis=0), x_ref[...])
    finish(
        core_ref[0], core_ref[1], both[: v.shape[0]], both[v.shape[0] :], xi, vp_ref, w_ref, packed_ref, mine_ref,
        other_ref,
    )


def ring(count, by):
    return [(i, (i + by) % count) for i in range(count)]


def turn():
    far = lax.axis_index("grid") // (lax.axis_size("grid") // 2)
    return far * (lax.axis_size(BAND) // 2)


def slab_ring(by):
    slabs, quarters = lax.axis_size("grid"), lax.axis_size(BAND)

    def pair(g, b):
        there = (g + by) % slabs
        crosses = g // (slabs // 2) != there // (slabs // 2)
        return g * quarters + b, there * quarters + (b + crosses * (quarters // 2)) % quarters

    return [pair(g, b) for g in range(slabs) for b in range(quarters)]


def neighbours(v):
    near = lax.axis_size(BAND)
    return (
        lax.ppermute(v, EVERY, slab_ring(1)),
        lax.ppermute(v, EVERY, slab_ring(-1)),
        lax.ppermute(v, BAND, ring(near, 1)),
        lax.ppermute(v, BAND, ring(near, -1)),
    )


def swapped(x):
    return lax.ppermute(x, "band_1", ring(lax.axis_size("band_1"), 1))


def exchange(pieces):
    return lax.all_to_all(pieces, CHIPS, split_axis=0, concat_axis=0, tiled=True)


def from_every_chip(x):
    count = lax.axis_size(CHIPS)
    copies = jnp.broadcast_to(x, (count, *x.shape)).reshape(count * x.shape[0], *x.shape[1:])
    return exchange(copies)


def total_everywhere(mine, other):
    rows, lanes = mine.shape
    count = lax.axis_size(CHIPS)
    pieces = (mine + swapped(other)).reshape(rows // LINES, LINES, lanes)
    arrived = exchange(pieces)
    total = arrived.reshape(count, rows // LINES // count, LINES, lanes).sum(axis=0)
    half = from_every_chip(total).reshape(rows, lanes)
    return half, swapped(half)


def to_cells(*fields):
    count = lax.axis_size(BAND)
    z, x, y, lanes = fields[0].shape
    pieces = jnp.stack([f.reshape(z, 2, count // 2, x // count, y, lanes) for f in fields])
    pieces = jnp.where(turn() == 0, pieces, pieces[:, :, ::-1])
    pieces = pieces.reshape(len(fields), z, count, x // count, y, lanes)
    pieces = lax.all_to_all(jnp.moveaxis(pieces, 2, 0), BAND, split_axis=0, concat_axis=0, tiled=True)
    return [pieces[:, at] for at in range(len(fields))]


def call(kernel, shapes, *args, scratch=(), flops=2_000_000_000, room=32):
    place = jnp.stack([lax.axis_index("band_1"), lax.axis_index(BAND), turn()]).astype(jnp.int32)
    return pl.pallas_call(
        kernel,
        out_shape=[jax.ShapeDtypeStruct(s, jnp.float32) for s in shapes],
        in_specs=[pl.BlockSpec(memory_space=pltpu.SMEM)] + [WHOLE] * len(args),
        out_specs=[WHOLE] * len(shapes),
        scratch_shapes=[pltpu.VMEM(s, jnp.float32) for s in scratch],
        compiler_params=pltpu.CompilerParams(vmem_limit_bytes=room << 20),
        cost_estimate=pl.CostEstimate(
            flops=flops, bytes_accessed=4 * sum(a.size for a in args), transcendentals=0
        ),
    )(place, *args)


def local(orbitals, projectors, potential):
    v, xi = to_cells(orbitals, projectors)
    full = v.shape
    blocks, planes, rows, columns, lanes = full
    flat = (blocks, planes * rows * columns, lanes)
    total = blocks * lanes
    square = (total, total)
    xi = xi.reshape(flat)
    band = lax.axis_index(BAND)
    own = lax.dynamic_slice_in_dim(potential, (band + turn()) % blocks * rows, rows, 1)
    own = jnp.broadcast_to(own[..., None], (planes, rows, columns, lanes))
    pairs = len(pairs_of(blocks))

    def packed(count):
        return (BLOCK * count, BLOCK), (BLOCK * count // 2, BLOCK)

    small, small_half = packed(pairs + blocks * blocks)
    large, large_half = packed(2 * pairs + blocks * blocks + 2)
    sums = (3 * blocks // 2, BLOCK)
    stats_shape = (2 * blocks, BLOCK)
    stats_list = []
    around = neighbours(v)
    mine, other = total_everywhere(*call(gram_kernel, [small_half] * 2, v.reshape(flat), xi, scratch=[small]))
    (x,) = call(first_factor_kernel, [square], mine, other, flops=20_000_000_000, room=16)
    vp, w, mine, other = call(
        first_transform_kernel, [flat, full, large_half, large_half], x, mine, other, v, *around, own, xi,
        scratch=[square, full, large],
    )
    for iteration in range(1, ITERS):
        around = neighbours(w)
        mine, other = total_everywhere(mine, other)
        x, stats = call(factor_kernel, [square, stats_shape], mine, other, flops=20_000_000_000, room=16)
        stats_list.append(stats)
        given = (x, stats, mine, other, vp, w, *around, own, xi)
        if iteration < ITERS - 1:
            vp, w, mine, other = call(
                transform_kernel, [flat, full, large_half, large_half], *given,
                scratch=[square, full, large],
            )
    both = (blocks, 2, planes, rows, columns, lanes)
    parts, mine, other = call(
        last_transform_kernel, [both, sums, sums], *given, scratch=[square, full]
    )
    parts = [parts[0]] + [lax.ppermute(parts[k], BAND, ring(blocks, k)) for k in range(1, blocks)]
    lines = (mine + swapped(other)).reshape(-1, LINES, lanes)
    here = from_every_chip(lines)
    here = here.reshape(lax.axis_size(CHIPS), *sums)
    v, stats = call(
        last_kernel, [(planes, blocks * rows, columns, lanes), stats_shape], *parts, here, swapped(here)
    )
    stats_list.append(stats)
    stats = jnp.stack(stats_list).reshape(ITERS, 2, blocks, lanes)
    stats = lax.dynamic_slice_in_dim(stats, band, 1, 2)[:, :, 0]
    return (v, stats[:, 0], jnp.sqrt(stats[:, 1]))


def solution(mesh):
    finer = Mesh(mesh.devices.reshape(mesh.shape["grid"], 2, 2), ("grid", "band_0", "band_1"))
    placed = (P("grid", None, None, BAND), P("grid", None, None, BAND), P("grid", None, None))
    return jax.shard_map(
        local,
        mesh=finer,
        in_specs=placed,
        out_specs=(P("grid", None, None, BAND), P(None, BAND), P(None, BAND)),
        check_vma=False,
    )
```

```python
import jax
import jax.numpy as jnp
from jax import lax
from jax.experimental import pallas as pl
from jax.experimental.pallas import tpu as pltpu
from jax.sharding import Mesh
from jax.sharding import PartitionSpec as P

ITERS = 3
BAND = ("band_0", "band_1")
CHIPS = ("grid", "band_0")
EVERY = ("grid", "band_0", "band_1")
BLOCK = 128
TILE = 8
HALF = 64
LINES = 2

STENCIL = (-205.0 / 72.0, 8.0 / 5.0, -1.0 / 5.0, 8.0 / 315.0, -1.0 / 560.0)
STEP_LENGTH = 0.25
NORM_EPS = 1e-06
WHOLE = pl.BlockSpec(memory_space=pltpu.VMEM)


def split(x):
    high = x.astype(jnp.bfloat16)
    return high, (x - high.astype(jnp.float32)).astype(jnp.bfloat16)


def dot(left, right, sides):
    (lh, ll), (rh, rl) = split(left), split(right)

    def once(a, b):
        return lax.dot_general(
            a, b, ((sides[:1], sides[1:]), ((), ())), preferred_element_type=jnp.float32
        )

    return once(lh, rl) + once(ll, rh) + once(lh, rh)


def row_of(tile, j):
    return jnp.broadcast_to(tile[j:j + 1, :], tile.shape)


def lane_of(tile, j):
    return jnp.broadcast_to(tile[:, j:j + 1], tile.shape)


def inverse_factor(tiles):
    count = len(tiles)
    lane = lax.broadcasted_iota(jnp.int32, tiles[0].shape, 1)
    sub = lax.broadcasted_iota(jnp.int32, tiles[0].shape, 0)
    tiles = list(tiles)
    head = [lane_of(tiles[0], j) for j in range(TILE)]
    for p in range(count):
        base = TILE * p
        inside = (lane >= base) & (lane < base + TILE)
        own = jnp.where(inside, (lane == base + sub).astype(jnp.float32), tiles[p])
        ahead = p + 1 < count
        if ahead:
            coming = [lane_of(tiles[p + 1], base + TILE + j) for j in range(TILE)]
        rows, crosses = [], []
        for j in range(TILE):
            scale = lax.rsqrt(row_of(head[j], j))
            row = row_of(own, j) * scale
            column = jnp.where(sub > j, head[j] * scale, 0.0)
            own = jnp.where(sub == j, row, own - column * row)
            cross = [None] * TILE
            for k in range(j + 1, TILE):
                cross[k] = row_of(head[k], j) * scale
                head[k] = head[k] - column * cross[k]
                cross[k] = cross[k] * scale
            rows.append(row * scale)
            crosses.append(cross)
            if ahead:
                if j == 0:
                    parts = [lane_of(tiles[p + 1], base + k) for k in range(TILE)]
                    following = jnp.where(inside, 0.0, tiles[p + 1])
                following = following - parts[j] * rows[j]
                for k in range(j + 1, TILE):
                    parts[k] = parts[k] - parts[j] * crosses[j][k]
                scaled = parts[j] * (scale * scale)
                for k in range(TILE):
                    coming[k] = coming[k] - scaled * row_of(parts[j], k)
        tiles[p] = jnp.where((lane < base + TILE) | (lane >= TILE * count), own, 0.0)
        if ahead:
            tiles[p + 1] = following
            head = coming
        for t in range(p + 2, count):
            parts = [lane_of(tiles[t], base + j) for j in range(TILE)]
            tile = jnp.where(inside, 0.0, tiles[t])
            for j in range(TILE):
                tile = tile - parts[j] * rows[j]
                for k in range(j + 1, TILE):
                    parts[k] = parts[k] - parts[j] * crosses[j][k]
            tiles[t] = tile
    return tiles


def pairs_of(blocks):
    return [(i, j) for i in range(blocks) for j in range(i, blocks)]


def cut(x, b):
    return x[:, BLOCK * b : BLOCK * (b + 1)]


def rows_at(ref, at):
    return ref[BLOCK * at : BLOCK * (at + 1), :]


def block_of(core, mine_ref, other_ref, at):
    half = mine_ref.shape[0] // BLOCK
    mine, other = rows_at(mine_ref, at % half), rows_at(other_ref, at % half)
    here = jnp.full(mine.shape, core, jnp.int32) == at // half
    return jnp.where(here, mine, other)


def factorize(x_ref):
    blocks = x_ref.shape[0] // BLOCK
    for i in range(1, blocks):
        x_ref[BLOCK * i : BLOCK * (i + 1), : BLOCK * i] = jnp.zeros((BLOCK, BLOCK * i), jnp.float32)
    block_row = lax.broadcasted_iota(jnp.int32, (BLOCK, BLOCK), 0)
    block_lane = lax.broadcasted_iota(jnp.int32, (BLOCK, BLOCK), 1)

    def step(k, carry):
        first = pl.multiple_of(k * BLOCK, BLOCK)
        here = pl.ds(first, BLOCK)

        def part(h, carry):
            top = first + HALF * h
            rows = [pl.ds(pl.multiple_of(top + TILE * t, TILE), TILE) for t in range(HALF // TILE)]
            tiles = inverse_factor([pltpu.roll(x_ref[r, here], HALF * h, 1) for r in rows])
            for r, tile in zip(rows, tiles):
                x_ref[r, here] = pltpu.roll(tile, HALF * h, 1)

            @pl.when(h == 0)
            def _():
                upper = x_ref[pl.ds(first, HALF), here]
                below = pl.ds(pl.multiple_of(first + HALF, HALF), HALF)
                change = dot(upper, upper, (0, 0))[HALF:, :]
                lane = lax.broadcasted_iota(jnp.int32, change.shape, 1)
                x_ref[below, here] = jnp.where(lane < HALF, 0.0, x_ref[below, here]) - change

            return carry

        lax.fori_loop(0, 2, part, 0)
        own = jnp.where((block_row < HALF) & (block_lane >= HALF), 0.0, x_ref[here, here])
        x_ref[here, here] = jnp.where(block_row == block_lane, 1.0, 0.0)
        x_ref[here, :] = dot(own, x_ref[here, :], (1, 0))

        def update(i, carry):
            there = pl.ds(pl.multiple_of(i * BLOCK, BLOCK), BLOCK)
            x_ref[there, here] = jnp.zeros((BLOCK, BLOCK), jnp.float32)
            x_ref[there, :] = x_ref[there, :] - dot(x_ref[here, there], x_ref[here, :], (0, 0))
            return carry

        return lax.fori_loop(k + 1, blocks, update, carry)

    lax.fori_loop(0, blocks, step, 0)
    for i in range(blocks - 1):
        x_ref[BLOCK * i : BLOCK * (i + 1), BLOCK * (i + 1) :] = jnp.zeros(
            (BLOCK, BLOCK * (blocks - 1 - i)), jnp.float32
        )


def first_factor_kernel(core_ref, mine_ref, other_ref, x_ref):
    blocks = x_ref.shape[0] // BLOCK
    for at, (i, j) in enumerate(pairs_of(blocks)):
        x_ref[BLOCK * i : BLOCK * (i + 1), BLOCK * j : BLOCK * (j + 1)] = block_of(
            core_ref[0], mine_ref, other_ref, at
        )
    factorize(x_ref)


def squared_of(rayleigh, energy, weight):
    return jnp.maximum(energy - 2.0 * rayleigh * rayleigh + rayleigh * rayleigh * weight, 0.0)


def length_of(squared):
    return STEP_LENGTH / jnp.sqrt(squared + NORM_EPS)


def apart_of(blocks):
    return [(i, j) for i in range(blocks) for j in range(i + 1, blocks)]


def factor_kernel(core_ref, mine_ref, other_ref, x_ref, stats_ref):
    blocks = x_ref.shape[0] // BLOCK
    apart = apart_of(blocks)
    row = lax.broadcasted_iota(jnp.int32, (BLOCK, BLOCK), 0)
    lane = lax.broadcasted_iota(jnp.int32, (BLOCK, BLOCK), 1)

    def block(at):
        return block_of(core_ref[0], mine_ref, other_ref, at)

    def upright(line):
        return jnp.sum(jnp.where(row == lane, line, 0.0), axis=1, keepdims=True)

    lines = block(2 * len(apart) + blocks)[: 3 * blocks]
    rayleigh, energy, weight = (lines[blocks * k : blocks * (k + 1)] for k in range(3))
    squared = squared_of(rayleigh, energy, weight)
    stats_ref[:blocks, :] = rayleigh
    stats_ref[blocks:, :] = squared
    length = length_of(squared)
    gain = 1.0 + rayleigh * length
    diagonal = (length * energy - 2.0 * gain * rayleigh) * length + gain * gain * weight
    d = [length[b : b + 1] for b in range(blocks)]
    a = [gain[b : b + 1] for b in range(blocks)]
    d_up = [upright(line) for line in d]
    a_up = [upright(line) for line in a]
    for at, (i, j) in enumerate(apart):
        x_ref[BLOCK * i : BLOCK * (i + 1), BLOCK * j : BLOCK * (j + 1)] = (
            d_up[i] * d[j]
        ) * block(len(apart) + at) - (a_up[i] * d[j] + d_up[i] * a[j]) * block(at)
    for b in range(blocks):
        both = block(2 * len(apart) + b)
        energies = jnp.transpose(jnp.where(row > lane, both, 0.0))
        upper = (d_up[b] * d[b]) * energies - (a_up[b] * d[b] + d_up[b] * a[b]) * both
        upper = jnp.where(row < lane, upper, 0.0)
        x_ref[BLOCK * b : BLOCK * (b + 1), BLOCK * b : BLOCK * (b + 1)] = (
            upper + jnp.transpose(upper) + jnp.where(row == lane, diagonal[b : b + 1], 0.0)
        )
    factorize(x_ref)


def joined(ref):
    return jnp.concatenate([ref[b] for b in range(ref.shape[0])], axis=1)


def share_out(core, packed_ref, mine_ref, other_ref):
    half = mine_ref.shape[0]
    mine_ref[...] = packed_ref[pl.ds(pl.multiple_of(core * half, TILE), half), :]
    other_ref[...] = packed_ref[pl.ds(pl.multiple_of((1 - core) * half, TILE), half), :]


def write_pairs(left, right, at, packed_ref):
    blocks = left.shape[1] // BLOCK
    for i in range(blocks):
        row = dot(cut(left, i), right[:, BLOCK * i :], (0, 0))
        for j in range(blocks - i):
            packed_ref[BLOCK * at : BLOCK * (at + 1), :] = cut(row, j)
            at += 1
    return at


def write_coupling(xi, v, at, packed_ref):
    blocks = v.shape[1] // BLOCK
    c = dot(xi, v, (0, 0))
    for j in range(blocks):
        packed_ref[BLOCK * at : BLOCK * (at + blocks), :] = cut(c, j)
        at += blocks
    return at


def gram_kernel(core_ref, v_ref, xi_ref, mine_ref, other_ref, packed_ref):
    v = joined(v_ref)
    at = write_pairs(v, v, 0, packed_ref)
    write_coupling(joined(xi_ref), v, at, packed_ref)
    share_out(core_ref[0], packed_ref, mine_ref, other_ref)


def totals_of(core, mine_ref, other_ref):
    mine = jnp.sum(mine_ref[...], axis=0)
    other = jnp.sum(other_ref[...], axis=0)
    first = jnp.full(mine.shape, core, jnp.int32) == 0
    return jnp.concatenate([jnp.where(first, mine, other), jnp.where(first, other, mine)], axis=0)


def along_lanes(rows, at, blocks):
    return jnp.concatenate([rows[at + b : at + b + 1] for b in range(blocks)], axis=1)


def last_kernel(core_ref, own_ref, near_ref, across_ref, far_ref, here_ref, there_ref, v_ref, stats_ref):
    planes, rows = own_ref.shape[1:3]
    totals = totals_of(core_ref[0], here_ref, there_ref)
    blocks = totals.shape[0] // 3
    rayleigh, energy, weight = (totals[blocks * k : blocks * (k + 1)] for k in range(3))
    stats_ref[:blocks, :] = rayleigh
    stats_ref[blocks:, :] = squared_of(rayleigh, energy, weight)
    rayleigh = stats_ref[pl.ds(core_ref[1], 1), :]
    length = length_of(stats_ref[pl.ds(blocks + core_ref[1], 1), :])
    for away, ref in enumerate((own_ref, near_ref, across_ref, far_ref)):
        first_row = rows * lax.rem(core_ref[1] + core_ref[2] + blocks - away, blocks)
        for z in range(planes):
            for x in range(rows):
                vp = ref[0, z, x]
                v_ref[z, first_row + x] = vp - (ref[1, z, x] - rayleigh * vp) * length


def local_part(v_ref, around, p_ref, u_ref):
    below_ref, above_ref, left_ref, right_ref = around
    blocks, planes, rows, columns, _ = v_ref.shape
    along_z = [(ref, z) for ref in (below_ref, v_ref, above_ref) for z in range(planes)]
    along_x = [(ref, x) for ref in (left_ref, v_ref, right_ref) for x in range(rows)]

    def one(b, carry):
        for z in range(planes):
            for x in range(rows):
                centre = v_ref[b, z, x]
                total = 3.0 * STENCIL[0] * centre
                for d in range(1, 5):
                    group = pltpu.roll(centre, d, 0) + pltpu.roll(centre, columns - d, 0)
                    for way in (d, -d):
                        ref, at = along_z[planes + z + way]
                        group = group + ref[b, at, x]
                        ref, at = along_x[rows + x + way]
                        group = group + ref[b, z, at]
                    total = total + STENCIL[d] * group
                u_ref[b, z, x] = p_ref[z, x] * centre - 0.5 * total
        return carry

    lax.fori_loop(0, blocks, one, 0)


def flat_lanes(ref):
    blocks, planes, rows, columns, lanes = ref.shape
    return jnp.concatenate(
        [ref[b].reshape(planes * rows * columns, lanes) for b in range(blocks)], axis=1
    )


def fill_coupling(c_ref, core, mine_ref, other_ref, at):
    blocks = c_ref.shape[1] // BLOCK
    for j in range(blocks):
        for i in range(blocks):
            c_ref[BLOCK * i : BLOCK * (i + 1), BLOCK * j : BLOCK * (j + 1)] = block_of(
                core, mine_ref, other_ref, at
            )
            at += 1


def transformed(v, x):
    middle = x.shape[0] // 2
    return jnp.concatenate(
        [dot(v[:, :middle], x[:middle, :middle], (1, 1)), dot(v, x[middle:, :], (1, 1))], axis=1
    )


def line_sums(product):
    total = jnp.sum(product, axis=0, keepdims=True)
    return [cut(total, b) for b in range(product.shape[1] // BLOCK)]


def finish(core, band, vp, w, xi, vp_ref, w_ref, packed_ref, mine_ref, other_ref):
    blocks = vp.shape[1] // BLOCK
    if packed_ref is None:
        for b in range(blocks):
            away = lax.rem(b + blocks - band, blocks)
            vp_ref[away, 0] = cut(vp, b).reshape(vp_ref.shape[2:])
            vp_ref[away, 1] = cut(w, b).reshape(vp_ref.shape[2:])
        lines = line_sums(vp * w) + line_sums(w * w) + line_sums(vp * vp)
        half = len(lines) // 2
        first, second = (jnp.concatenate(part, axis=0) for part in (lines[:half], lines[half:]))
        front = jnp.full(first.shape, core, jnp.int32) == 0
        mine_ref[...] = jnp.where(front, first, second)
        other_ref[...] = jnp.where(front, second, first)
        return
    for b in range(blocks):
        vp_ref[b] = cut(vp, b)
        w_ref[b] = cut(w, b).reshape(w_ref.shape[1:])
    row = lax.broadcasted_iota(jnp.int32, (BLOCK, BLOCK), 0)
    lane = lax.broadcasted_iota(jnp.int32, (BLOCK, BLOCK), 1)
    count = blocks * (blocks - 1) // 2
    at = 0

    def put(at, value):
        packed_ref[BLOCK * at : BLOCK * (at + 1), :] = value

    for i in range(blocks):
        right = w[:, BLOCK * i :]
        products = dot(cut(vp, i), right, (0, 0))
        energies = dot(cut(w, i), right, (0, 0))
        put(2 * count + i, jnp.where(row <= lane, cut(products, 0), cut(energies, 0)))
        for j in range(1, blocks - i):
            put(at, cut(products, j))
            put(count + at, cut(energies, j))
            at += 1
    at = 2 * count + blocks
    put(at, jnp.zeros((BLOCK, BLOCK), jnp.float32))
    lines = line_sums(vp * w) + line_sums(w * w) + line_sums(vp * vp)
    packed_ref[BLOCK * at : BLOCK * at + len(lines), :] = jnp.concatenate(lines, axis=0)
    at = write_coupling(xi, w, at + 1, packed_ref)
    put(at, jnp.zeros((BLOCK, BLOCK), jnp.float32))
    share_out(core, packed_ref, mine_ref, other_ref)


def first_transform_kernel(
    core_ref, x_ref, in_mine_ref, in_other_ref, v_ref, below_ref, above_ref, left_ref, right_ref, p_ref,
    xi_ref, vp_ref, w_ref, mine_ref, other_ref, c_ref, u_ref, packed_ref,
):
    blocks = v_ref.shape[0]
    at = len(pairs_of(blocks))
    fill_coupling(c_ref, core_ref[0], in_mine_ref, in_other_ref, at)
    local_part(v_ref, (below_ref, above_ref, left_ref, right_ref), p_ref, u_ref)
    v = flat_lanes(v_ref)
    xi = joined(xi_ref)
    z = flat_lanes(u_ref) - dot(xi, c_ref[...], (1, 0))
    both = transformed(jnp.concatenate([v, z], axis=0), x_ref[...])
    finish(
        core_ref[0], core_ref[1], both[: v.shape[0]], both[v.shape[0] :], xi, vp_ref, w_ref, packed_ref, mine_ref,
        other_ref,
    )


def stepped(vp, w, y, stats, blocks):
    rayleigh = along_lanes(stats, 0, blocks)
    length = length_of(along_lanes(stats, blocks, blocks))
    return vp - (w - rayleigh * vp) * length, w - (y - rayleigh * w) * length


def last_transform_kernel(*refs):
    outs = 14
    transform_kernel(*refs[:outs], None, *refs[outs:], None)


def transform_kernel(
    core_ref, x_ref, stats_ref, in_mine_ref, in_other_ref, old_ref, v_ref, below_ref, above_ref, left_ref,
    right_ref, p_ref, xi_ref, vp_ref, w_ref, mine_ref, other_ref, c_ref, u_ref, packed_ref,
):
    blocks = v_ref.shape[0]
    at = 2 * len(apart_of(blocks)) + blocks + 1
    fill_coupling(c_ref, core_ref[0], in_mine_ref, in_other_ref, at)
    local_part(v_ref, (below_ref, above_ref, left_ref, right_ref), p_ref, u_ref)
    xi = joined(xi_ref)
    y = flat_lanes(u_ref) - dot(xi, c_ref[...], (1, 0))
    v, z = stepped(joined(old_ref), flat_lanes(v_ref), y, stats_ref[...], blocks)
    both = transformed(jnp.concatenate([v, z], axis=0), x_ref[...])
    finish(
        core_ref[0], core_ref[1], both[: v.shape[0]], both[v.shape[0] :], xi, vp_ref, w_ref, packed_ref, mine_ref,
        other_ref,
    )


def ring(count, by):
    return [(i, (i + by) % count) for i in range(count)]


def turn():
    far = lax.axis_index("grid") // (lax.axis_size("grid") // 2)
    return far * (lax.axis_size(BAND) // 2)


def slab_ring(by):
    slabs, quarters = lax.axis_size("grid"), lax.axis_size(BAND)

    def pair(g, b):
        there = (g + by) % slabs
        crosses = g // (slabs // 2) != there // (slabs // 2)
        return g * quarters + b, there * quarters + (b + crosses * (quarters // 2)) % quarters

    return [pair(g, b) for g in range(slabs) for b in range(quarters)]


def neighbours(v):
    near = lax.axis_size(BAND)
    return (
        lax.ppermute(v, EVERY, slab_ring(1)),
        lax.ppermute(v, EVERY, slab_ring(-1)),
        lax.ppermute(v, BAND, ring(near, 1)),
        lax.ppermute(v, BAND, ring(near, -1)),
    )


def swapped(x):
    return lax.ppermute(x, "band_1", ring(lax.axis_size("band_1"), 1))


def exchange(pieces):
    return lax.all_to_all(pieces, CHIPS, split_axis=0, concat_axis=0, tiled=True)


def from_every_chip(x):
    count = lax.axis_size(CHIPS)
    copies = jnp.broadcast_to(x, (count, *x.shape)).reshape(count * x.shape[0], *x.shape[1:])
    return exchange(copies)


def total_everywhere(mine, other):
    rows, lanes = mine.shape
    count = lax.axis_size(CHIPS)
    pieces = (mine + swapped(other)).reshape(rows // LINES, LINES, lanes)
    arrived = exchange(pieces)
    total = arrived.reshape(count, rows // LINES // count, LINES, lanes).sum(axis=0)
    half = from_every_chip(total).reshape(rows, lanes)
    return half, swapped(half)


def to_cells(*fields):
    count = lax.axis_size(BAND)
    z, x, y, lanes = fields[0].shape
    pieces = jnp.stack([f.reshape(z, 2, count // 2, x // count, y, lanes) for f in fields])
    pieces = jnp.where(turn() == 0, pieces, pieces[:, :, ::-1])
    pieces = pieces.reshape(len(fields), z, count, x // count, y, lanes)
    pieces = lax.all_to_all(jnp.moveaxis(pieces, 2, 0), BAND, split_axis=0, concat_axis=0, tiled=True)
    return [pieces[:, at] for at in range(len(fields))]


def call(kernel, shapes, *args, scratch=(), flops=2_000_000_000, room=32):
    place = jnp.stack([lax.axis_index("band_1"), lax.axis_index(BAND), turn()]).astype(jnp.int32)
    return pl.pallas_call(
        kernel,
        out_shape=[jax.ShapeDtypeStruct(s, jnp.float32) for s in shapes],
        in_specs=[pl.BlockSpec(memory_space=pltpu.SMEM)] + [WHOLE] * len(args),
        out_specs=[WHOLE] * len(shapes),
        scratch_shapes=[pltpu.VMEM(s, jnp.float32) for s in scratch],
        compiler_params=pltpu.CompilerParams(vmem_limit_bytes=room << 20),
        cost_estimate=pl.CostEstimate(
            flops=flops, bytes_accessed=4 * sum(a.size for a in args), transcendentals=0
        ),
    )(place, *args)


def local(orbitals, projectors, potential):
    v, xi = to_cells(orbitals, projectors)
    full = v.shape
    blocks, planes, rows, columns, lanes = full
    flat = (blocks, planes * rows * columns, lanes)
    total = blocks * lanes
    square = (total, total)
    xi = xi.reshape(flat)
    band = lax.axis_index(BAND)
    own = lax.dynamic_slice_in_dim(potential, (band + turn()) % blocks * rows, rows, 1)
    own = jnp.broadcast_to(own[..., None], (planes, rows, columns, lanes))
    pairs = len(pairs_of(blocks))

    def packed(count):
        return (BLOCK * count, BLOCK), (BLOCK * count // 2, BLOCK)

    small, small_half = packed(pairs + blocks * blocks)
    large, large_half = packed(blocks * (blocks - 1) + blocks + 2 + blocks * blocks)
    sums = (3 * blocks // 2, BLOCK)
    stats_shape = (2 * blocks, BLOCK)
    stats_list = []
    around = neighbours(v)
    mine, other = total_everywhere(*call(gram_kernel, [small_half] * 2, v.reshape(flat), xi, scratch=[small]))
    (x,) = call(first_factor_kernel, [square], mine, other, flops=20_000_000_000, room=16)
    vp, w, mine, other = call(
        first_transform_kernel, [flat, full, large_half, large_half], x, mine, other, v, *around, own, xi,
        scratch=[square, full, large],
    )
    for iteration in range(1, ITERS):
        around = neighbours(w)
        mine, other = total_everywhere(mine, other)
        x, stats = call(factor_kernel, [square, stats_shape], mine, other, flops=20_000_000_000, room=16)
        stats_list.append(stats)
        given = (x, stats, mine, other, vp, w, *around, own, xi)
        if iteration < ITERS - 1:
            vp, w, mine, other = call(
                transform_kernel, [flat, full, large_half, large_half], *given,
                scratch=[square, full, large],
            )
    both = (blocks, 2, planes, rows, columns, lanes)
    parts, mine, other = call(
        last_transform_kernel, [both, sums, sums], *given, scratch=[square, full]
    )
    parts = [parts[0]] + [lax.ppermute(parts[k], BAND, ring(blocks, k)) for k in range(1, blocks)]
    lines = (mine + swapped(other)).reshape(-1, LINES, lanes)
    here = from_every_chip(lines)
    here = here.reshape(lax.axis_size(CHIPS), *sums)
    v, stats = call(
        last_kernel, [(planes, blocks * rows, columns, lanes), stats_shape], *parts, here, swapped(here)
    )
    stats_list.append(stats)
    stats = jnp.stack(stats_list).reshape(ITERS, 2, blocks, lanes)
    stats = lax.dynamic_slice_in_dim(stats, band, 1, 2)[:, :, 0]
    return (v, stats[:, 0], jnp.sqrt(stats[:, 1]))


def solution(mesh):
    finer = Mesh(mesh.devices.reshape(mesh.shape["grid"], 2, 2), ("grid", "band_0", "band_1"))
    placed = (P("grid", None, None, BAND), P("grid", None, None, BAND), P("grid", None, None))
    return jax.shard_map(
        local,
        mesh=finer,
        in_specs=placed,
        out_specs=(P("grid", None, None, BAND), P(None, BAND), P(None, BAND)),
        check_vma=False,
    )
```

```python
import jax
import jax.numpy as jnp
from jax import lax
from jax.experimental import pallas as pl
from jax.experimental.pallas import tpu as pltpu
from jax.sharding import Mesh
from jax.sharding import PartitionSpec as P

ITERS = 3
BAND = ("band_0", "band_1")
CHIPS = ("grid", "band_0")
EVERY = ("grid", "band_0", "band_1")
BLOCK = 128
TILE = 8
HALF = 64
LINES = 2

STENCIL = (-205.0 / 72.0, 8.0 / 5.0, -1.0 / 5.0, 8.0 / 315.0, -1.0 / 560.0)
STEP_LENGTH = 0.25
NORM_EPS = 1e-06
WHOLE = pl.BlockSpec(memory_space=pltpu.VMEM)


def split(x):
    high = x.astype(jnp.bfloat16)
    return high, (x - high.astype(jnp.float32)).astype(jnp.bfloat16)


def dot_parts(left, right, sides):
    (lh, ll), (rh, rl) = left, right

    def once(a, b):
        return lax.dot_general(
            a, b, ((sides[:1], sides[1:]), ((), ())), preferred_element_type=jnp.float32
        )

    return once(lh, rl) + once(ll, rh) + once(lh, rh)


def dot(left, right, sides):
    return dot_parts(split(left), split(right), sides)


def lanes_of(parts, start, stop):
    return tuple(part[:, start:stop] for part in parts)


def row_of(tile, j):
    return jnp.broadcast_to(tile[j:j + 1, :], tile.shape)


def lane_of(tile, j):
    return jnp.broadcast_to(tile[:, j:j + 1], tile.shape)


def inverse_factor(tiles):
    count = len(tiles)
    lane = lax.broadcasted_iota(jnp.int32, tiles[0].shape, 1)
    sub = lax.broadcasted_iota(jnp.int32, tiles[0].shape, 0)
    tiles = list(tiles)
    head = [lane_of(tiles[0], j) for j in range(TILE)]
    for p in range(count):
        base = TILE * p
        inside = (lane >= base) & (lane < base + TILE)
        own = jnp.where(inside, (lane == base + sub).astype(jnp.float32), tiles[p])
        ahead = p + 1 < count
        if ahead:
            coming = [lane_of(tiles[p + 1], base + TILE + j) for j in range(TILE)]
        rows, crosses = [], []
        for j in range(TILE):
            scale = lax.rsqrt(row_of(head[j], j))
            row = row_of(own, j) * scale
            column = jnp.where(sub > j, head[j] * scale, 0.0)
            own = jnp.where(sub == j, row, own - column * row)
            cross = [None] * TILE
            for k in range(j + 1, TILE):
                cross[k] = row_of(head[k], j) * scale
                head[k] = head[k] - column * cross[k]
                cross[k] = cross[k] * scale
            rows.append(row * scale)
            crosses.append(cross)
            if ahead:
                if j == 0:
                    parts = [lane_of(tiles[p + 1], base + k) for k in range(TILE)]
                    following = jnp.where(inside, 0.0, tiles[p + 1])
                following = following - parts[j] * rows[j]
                for k in range(j + 1, TILE):
                    parts[k] = parts[k] - parts[j] * crosses[j][k]
                scaled = parts[j] * (scale * scale)
                for k in range(TILE):
                    coming[k] = coming[k] - scaled * row_of(parts[j], k)
        tiles[p] = jnp.where((lane < base + TILE) | (lane >= TILE * count), own, 0.0)
        if ahead:
            tiles[p + 1] = following
            head = coming
        for t in range(p + 2, count):
            parts = [lane_of(tiles[t], base + j) for j in range(TILE)]
            tile = jnp.where(inside, 0.0, tiles[t])
            for j in range(TILE):
                tile = tile - parts[j] * rows[j]
                for k in range(j + 1, TILE):
                    parts[k] = parts[k] - parts[j] * crosses[j][k]
            tiles[t] = tile
    return tiles


def pairs_of(blocks):
    return [(i, j) for i in range(blocks) for j in range(i, blocks)]


def cut(x, b):
    return x[:, BLOCK * b : BLOCK * (b + 1)]


def rows_at(ref, at):
    return ref[BLOCK * at : BLOCK * (at + 1), :]


def block_of(core, mine_ref, other_ref, at):
    half = mine_ref.shape[0] // BLOCK
    mine, other = rows_at(mine_ref, at % half), rows_at(other_ref, at % half)
    here = jnp.full(mine.shape, core, jnp.int32) == at // half
    return jnp.where(here, mine, other)


def spread(x_ref, own, at):
    size = x_ref.shape[0]
    start, stop = BLOCK * at, BLOCK * (at + 1)
    here, below = slice(start, stop), slice(stop, size)
    around = [x_ref[here, part] for part in (slice(0, start), slice(stop, size)) if part.stop > part.start]
    sides = dot(own, jnp.concatenate(around, axis=1), (1, 0))
    row = jnp.concatenate(
        [part for part in (sides[:, :start], own, sides[:, start:]) if part.shape[1]], axis=1
    )
    x_ref[here, :] = row
    if stop < size:
        parts = split(row)
        change = dot_parts(lanes_of(parts, stop, size), parts, (0, 0))
        x_ref[below, here] = -change[:, here]
        x_ref[below, below] = x_ref[below, below] - change[:, stop:]
        if start:
            x_ref[below, :start] = x_ref[below, :start] - change[:, :start]


def factorize(x_ref):
    blocks = x_ref.shape[0] // BLOCK
    block_row = lax.broadcasted_iota(jnp.int32, (BLOCK, BLOCK), 0)
    block_lane = lax.broadcasted_iota(jnp.int32, (BLOCK, BLOCK), 1)

    def step(k, carry):
        first = pl.multiple_of(k * BLOCK, BLOCK)
        here = pl.ds(first, BLOCK)

        def part(h, carry):
            top = first + HALF * h
            rows = [pl.ds(pl.multiple_of(top + TILE * t, TILE), TILE) for t in range(HALF // TILE)]
            tiles = inverse_factor([pltpu.roll(x_ref[r, here], HALF * h, 1) for r in rows])
            for r, tile in zip(rows, tiles):
                x_ref[r, here] = pltpu.roll(tile, HALF * h, 1)

            @pl.when(h == 0)
            def _():
                upper = x_ref[pl.ds(first, HALF), here]
                below = pl.ds(pl.multiple_of(first + HALF, HALF), HALF)
                change = dot(upper, upper, (0, 0))[HALF:, :]
                lane = lax.broadcasted_iota(jnp.int32, change.shape, 1)
                x_ref[below, here] = jnp.where(lane < HALF, 0.0, x_ref[below, here]) - change

            return carry

        lax.fori_loop(0, 2, part, 0)
        own = jnp.where((block_row < HALF) & (block_lane >= HALF), 0.0, x_ref[here, here])
        for at in range(blocks):
            @pl.when(k == at)
            def _(at=at):
                spread(x_ref, own, at)

        return carry

    lax.fori_loop(0, blocks, step, 0)
    for i in range(blocks - 1):
        x_ref[BLOCK * i : BLOCK * (i + 1), BLOCK * (i + 1) :] = jnp.zeros(
            (BLOCK, BLOCK * (blocks - 1 - i)), jnp.float32
        )


def first_factor_kernel(core_ref, mine_ref, other_ref, x_ref):
    blocks = x_ref.shape[0] // BLOCK
    for at, (i, j) in enumerate(pairs_of(blocks)):
        x_ref[BLOCK * i : BLOCK * (i + 1), BLOCK * j : BLOCK * (j + 1)] = block_of(
            core_ref[0], mine_ref, other_ref, at
        )
    factorize(x_ref)


def squared_of(rayleigh, energy, weight):
    return jnp.maximum(energy - 2.0 * rayleigh * rayleigh + rayleigh * rayleigh * weight, 0.0)


def length_of(squared):
    return STEP_LENGTH / jnp.sqrt(squared + NORM_EPS)


def apart_of(blocks):
    return [(i, j) for i in range(blocks) for j in range(i + 1, blocks)]


def factor_kernel(core_ref, mine_ref, other_ref, x_ref, stats_ref):
    blocks = x_ref.shape[0] // BLOCK
    apart = apart_of(blocks)
    row = lax.broadcasted_iota(jnp.int32, (BLOCK, BLOCK), 0)
    lane = lax.broadcasted_iota(jnp.int32, (BLOCK, BLOCK), 1)

    def block(at):
        return block_of(core_ref[0], mine_ref, other_ref, at)

    def upright(line):
        return jnp.sum(jnp.where(row == lane, line, 0.0), axis=1, keepdims=True)

    lines = block(2 * len(apart) + blocks)[: 3 * blocks]
    rayleigh, energy, weight = (lines[blocks * k : blocks * (k + 1)] for k in range(3))
    squared = squared_of(rayleigh, energy, weight)
    stats_ref[:blocks, :] = rayleigh
    stats_ref[blocks:, :] = squared
    length = length_of(squared)
    gain = 1.0 + rayleigh * length
    diagonal = (length * energy - 2.0 * gain * rayleigh) * length + gain * gain * weight
    d = [length[b : b + 1] for b in range(blocks)]
    a = [gain[b : b + 1] for b in range(blocks)]
    d_up = [upright(line) for line in d]
    a_up = [upright(line) for line in a]
    for at, (i, j) in enumerate(apart):
        x_ref[BLOCK * i : BLOCK * (i + 1), BLOCK * j : BLOCK * (j + 1)] = (
            d_up[i] * d[j]
        ) * block(len(apart) + at) - (a_up[i] * d[j] + d_up[i] * a[j]) * block(at)
    for b in range(blocks):
        both = block(2 * len(apart) + b)
        energies = jnp.transpose(jnp.where(row > lane, both, 0.0))
        upper = (d_up[b] * d[b]) * energies - (a_up[b] * d[b] + d_up[b] * a[b]) * both
        upper = jnp.where(row < lane, upper, 0.0)
        x_ref[BLOCK * b : BLOCK * (b + 1), BLOCK * b : BLOCK * (b + 1)] = (
            upper + jnp.transpose(upper) + jnp.where(row == lane, diagonal[b : b + 1], 0.0)
        )
    factorize(x_ref)


def joined(ref):
    return jnp.concatenate([ref[b] for b in range(ref.shape[0])], axis=1)


def share_out(core, packed_ref, mine_ref, other_ref):
    half = mine_ref.shape[0]
    mine_ref[...] = packed_ref[pl.ds(pl.multiple_of(core * half, TILE), half), :]
    other_ref[...] = packed_ref[pl.ds(pl.multiple_of((1 - core) * half, TILE), half), :]


def write_pairs(left, right, at, packed_ref):
    blocks = left.shape[1] // BLOCK
    for i in range(blocks):
        row = dot(cut(left, i), right[:, BLOCK * i :], (0, 0))
        for j in range(blocks - i):
            packed_ref[BLOCK * at : BLOCK * (at + 1), :] = cut(row, j)
            at += 1
    return at


def write_coupling(xi, v, at, packed_ref):
    c = dot_parts(xi, v, (0, 0))
    blocks = c.shape[1] // BLOCK
    for j in range(blocks):
        packed_ref[BLOCK * at : BLOCK * (at + blocks), :] = cut(c, j)
        at += blocks
    return at


def gram_kernel(core_ref, v_ref, xi_ref, mine_ref, other_ref, packed_ref):
    v = joined(v_ref)
    at = write_pairs(v, v, 0, packed_ref)
    write_coupling(split(joined(xi_ref)), split(v), at, packed_ref)
    share_out(core_ref[0], packed_ref, mine_ref, other_ref)


def totals_of(core, mine_ref, other_ref):
    mine = jnp.sum(mine_ref[...], axis=0)
    other = jnp.sum(other_ref[...], axis=0)
    first = jnp.full(mine.shape, core, jnp.int32) == 0
    return jnp.concatenate([jnp.where(first, mine, other), jnp.where(first, other, mine)], axis=0)


def along_lanes(rows, at, blocks):
    return jnp.concatenate([rows[at + b : at + b + 1] for b in range(blocks)], axis=1)


def last_kernel(core_ref, own_ref, near_ref, across_ref, far_ref, here_ref, there_ref, v_ref, stats_ref):
    planes, rows = own_ref.shape[1:3]
    totals = totals_of(core_ref[0], here_ref, there_ref)
    blocks = totals.shape[0] // 3
    rayleigh, energy, weight = (totals[blocks * k : blocks * (k + 1)] for k in range(3))
    stats_ref[:blocks, :] = rayleigh
    stats_ref[blocks:, :] = squared_of(rayleigh, energy, weight)
    rayleigh = stats_ref[pl.ds(core_ref[1], 1), :]
    length = length_of(stats_ref[pl.ds(blocks + core_ref[1], 1), :])
    for away, ref in enumerate((own_ref, near_ref, across_ref, far_ref)):
        first_row = rows * lax.rem(core_ref[1] + core_ref[2] + blocks - away, blocks)
        for z in range(planes):
            for x in range(rows):
                vp = ref[0, z, x]
                v_ref[z, first_row + x] = vp - (ref[1, z, x] - rayleigh * vp) * length


def local_part(core_ref, v_ref, around, p_ref, u_ref):
    far_ref, close_ref, left_ref, right_ref = around

    @pl.when(core_ref[3] == 0)
    def _():
        apply_local(v_ref, far_ref, close_ref, left_ref, right_ref, p_ref, u_ref)

    @pl.when(core_ref[3] != 0)
    def _():
        apply_local(v_ref, close_ref, far_ref, left_ref, right_ref, p_ref, u_ref)


def apply_local(v_ref, below_ref, above_ref, left_ref, right_ref, p_ref, u_ref):
    blocks, planes, rows, columns, _ = v_ref.shape
    along_z = [(ref, z) for ref in (below_ref, v_ref, above_ref) for z in range(planes)]
    along_x = [(ref, x) for ref in (left_ref, v_ref, right_ref) for x in range(rows)]

    def one(b, carry):
        for z in range(planes):
            for x in range(rows):
                centre = v_ref[b, z, x]
                total = 3.0 * STENCIL[0] * centre
                for d in range(1, 5):
                    group = pltpu.roll(centre, d, 0) + pltpu.roll(centre, columns - d, 0)
                    for way in (d, -d):
                        ref, at = along_z[planes + z + way]
                        group = group + ref[b, at, x]
                        ref, at = along_x[rows + x + way]
                        group = group + ref[b, z, at]
                    total = total + STENCIL[d] * group
                u_ref[b, z, x] = p_ref[z, x] * centre - 0.5 * total
        return carry

    lax.fori_loop(0, blocks, one, 0)


def flat_lanes(ref):
    blocks, planes, rows, columns, lanes = ref.shape
    return jnp.concatenate(
        [ref[b].reshape(planes * rows * columns, lanes) for b in range(blocks)], axis=1
    )


def fill_coupling(c_ref, core, mine_ref, other_ref, at):
    blocks = c_ref.shape[1] // BLOCK
    for j in range(blocks):
        for i in range(blocks):
            c_ref[BLOCK * i : BLOCK * (i + 1), BLOCK * j : BLOCK * (j + 1)] = block_of(
                core, mine_ref, other_ref, at
            )
            at += 1


def transformed(v, x):
    middle = x.shape[0] // 2
    parts = split(v)
    return jnp.concatenate(
        [
            dot_parts(lanes_of(parts, 0, middle), split(x[:middle, :middle]), (1, 1)),
            dot_parts(parts, split(x[middle:, :]), (1, 1)),
        ],
        axis=1,
    )


def line_sums(product):
    total = jnp.sum(product, axis=0, keepdims=True)
    return [cut(total, b) for b in range(product.shape[1] // BLOCK)]


def finish(core, band, vp, w, xi, vp_ref, w_ref, packed_ref, mine_ref, other_ref):
    blocks = vp.shape[1] // BLOCK
    if packed_ref is None:
        for b in range(blocks):
            away = lax.rem(b + blocks - band, blocks)
            vp_ref[away, 0] = cut(vp, b).reshape(vp_ref.shape[2:])
            vp_ref[away, 1] = cut(w, b).reshape(vp_ref.shape[2:])
        lines = line_sums(vp * w) + line_sums(w * w) + line_sums(vp * vp)
        half = len(lines) // 2
        first, second = (jnp.concatenate(part, axis=0) for part in (lines[:half], lines[half:]))
        front = jnp.full(first.shape, core, jnp.int32) == 0
        mine_ref[...] = jnp.where(front, first, second)
        other_ref[...] = jnp.where(front, second, first)
        return
    for b in range(blocks):
        vp_ref[b] = cut(vp, b)
        w_ref[b] = cut(w, b).reshape(w_ref.shape[1:])
    row = lax.broadcasted_iota(jnp.int32, (BLOCK, BLOCK), 0)
    lane = lax.broadcasted_iota(jnp.int32, (BLOCK, BLOCK), 1)
    count = blocks * (blocks - 1) // 2
    at = 0

    def put(at, value):
        packed_ref[BLOCK * at : BLOCK * (at + 1), :] = value

    left, right = split(vp), split(w)
    total, middle = w.shape[1], w.shape[1] // 2
    for i in range(blocks):
        top = BLOCK * i // middle * middle
        if BLOCK * i == top:
            products, energies = (
                dot_parts(lanes_of(p, top, top + middle), lanes_of(right, top, total), (0, 0))
                for p in (left, right)
            )
        lines = slice(BLOCK * i - top, BLOCK * (i + 1) - top)
        for j in range(i, blocks):
            lanes = slice(BLOCK * j - top, BLOCK * (j + 1) - top)
            if i == j:
                put(2 * count + i, jnp.where(row <= lane, products[lines, lanes], energies[lines, lanes]))
            else:
                put(at, products[lines, lanes])
                put(count + at, energies[lines, lanes])
                at += 1
    at = 2 * count + blocks
    put(at, jnp.zeros((BLOCK, BLOCK), jnp.float32))
    lines = line_sums(vp * w) + line_sums(w * w) + line_sums(vp * vp)
    packed_ref[BLOCK * at : BLOCK * at + len(lines), :] = jnp.concatenate(lines, axis=0)
    at = write_coupling(split(xi), right, at + 1, packed_ref)
    put(at, jnp.zeros((BLOCK, BLOCK), jnp.float32))
    share_out(core, packed_ref, mine_ref, other_ref)


def first_transform_kernel(
    core_ref, x_ref, in_mine_ref, in_other_ref, v_ref, far_ref, close_ref, left_ref, right_ref, p_ref,
    xi_ref, vp_ref, w_ref, mine_ref, other_ref, c_ref, u_ref, packed_ref,
):
    blocks = v_ref.shape[0]
    at = len(pairs_of(blocks))
    fill_coupling(c_ref, core_ref[0], in_mine_ref, in_other_ref, at)
    local_part(core_ref, v_ref, (far_ref, close_ref, left_ref, right_ref), p_ref, u_ref)
    v = flat_lanes(v_ref)
    xi = joined(xi_ref)
    z = flat_lanes(u_ref) - dot(xi, c_ref[...], (1, 0))
    both = transformed(jnp.concatenate([v, z], axis=0), x_ref[...])
    finish(
        core_ref[0], core_ref[1], both[: v.shape[0]], both[v.shape[0] :], xi, vp_ref, w_ref, packed_ref, mine_ref,
        other_ref,
    )


def stepped(vp, w, y, stats, blocks):
    rayleigh = along_lanes(stats, 0, blocks)
    length = length_of(along_lanes(stats, blocks, blocks))
    return vp - (w - rayleigh * vp) * length, w - (y - rayleigh * w) * length


def last_transform_kernel(*refs):
    outs = 14
    transform_kernel(*refs[:outs], None, *refs[outs:], None)


def transform_kernel(
    core_ref, x_ref, stats_ref, in_mine_ref, in_other_ref, old_ref, v_ref, far_ref, close_ref, left_ref,
    right_ref, p_ref, xi_ref, vp_ref, w_ref, mine_ref, other_ref, c_ref, u_ref, packed_ref,
):
    blocks = v_ref.shape[0]
    at = 2 * len(apart_of(blocks)) + blocks + 1
    fill_coupling(c_ref, core_ref[0], in_mine_ref, in_other_ref, at)
    local_part(core_ref, v_ref, (far_ref, close_ref, left_ref, right_ref), p_ref, u_ref)
    xi = joined(xi_ref)
    y = flat_lanes(u_ref) - dot(xi, c_ref[...], (1, 0))
    v, z = stepped(joined(old_ref), flat_lanes(v_ref), y, stats_ref[...], blocks)
    both = transformed(jnp.concatenate([v, z], axis=0), x_ref[...])
    finish(
        core_ref[0], core_ref[1], both[: v.shape[0]], both[v.shape[0] :], xi, vp_ref, w_ref, packed_ref, mine_ref,
        other_ref,
    )


def ring(count, by):
    return [(i, (i + by) % count) for i in range(count)]


def turn():
    far = lax.axis_index("grid") // (lax.axis_size("grid") // 2)
    return far * (lax.axis_size(BAND) // 2)


def slab_pairs(start):
    slabs, quarters = lax.axis_size("grid"), lax.axis_size(BAND)

    def pair(g, b):
        there = (g + (1 if g % 2 == start else -1)) % slabs
        crosses = g // (slabs // 2) != there // (slabs // 2)
        return g * quarters + b, there * quarters + (b + crosses * (quarters // 2)) % quarters

    return [pair(g, b) for g in range(slabs) for b in range(quarters)]


def neighbours(v):
    near = lax.axis_size(BAND)
    far = lax.ppermute(v, EVERY, slab_pairs(1))
    close = lax.ppermute(v, EVERY, slab_pairs(0))
    return far, close, lax.ppermute(v, BAND, ring(near, 1)), lax.ppermute(v, BAND, ring(near, -1))


def swapped(x):
    return lax.ppermute(x, "band_1", ring(lax.axis_size("band_1"), 1))


def exchange(pieces):
    return lax.all_to_all(pieces, CHIPS, split_axis=0, concat_axis=0, tiled=True)


def from_every_chip(x):
    count = lax.axis_size(CHIPS)
    copies = jnp.broadcast_to(x, (count, *x.shape)).reshape(count * x.shape[0], *x.shape[1:])
    return exchange(copies)


def total_everywhere(mine, other):
    rows, lanes = mine.shape
    count = lax.axis_size(CHIPS)
    pieces = (mine + swapped(other)).reshape(rows // LINES, LINES, lanes)
    arrived = exchange(pieces)
    total = arrived.reshape(count, rows // LINES // count, LINES, lanes).sum(axis=0)
    half = from_every_chip(total).reshape(rows, lanes)
    return half, swapped(half)


def pieces_kernel(core_ref, first_ref, second_ref, out_ref):
    quarters, _, planes, rows, _, _ = out_ref.shape
    for q in range(quarters):
        first_row = rows * lax.rem(core_ref[2] + q, quarters)
        for k, ref in enumerate((first_ref, second_ref)):
            for z in range(planes):
                for x in range(rows):
                    out_ref[q, k, z, x] = ref[z, first_row + x]


def to_cells(first, second):
    quarters = lax.axis_size(BAND)
    z, x, y, lanes = first.shape
    shape = (quarters, 2, z, x // quarters, y, lanes)
    (pieces,) = call(pieces_kernel, [shape], first, second, flops=1_000_000)
    pieces = lax.all_to_all(pieces, BAND, split_axis=0, concat_axis=0, tiled=True)
    return pieces[:, 0], pieces[:, 1]


def call(kernel, shapes, *args, scratch=(), flops=2_000_000_000, room=32):
    place = [lax.axis_index("band_1"), lax.axis_index(BAND), turn(), lax.axis_index("grid") % 2]
    place = jnp.stack(place).astype(jnp.int32)
    return pl.pallas_call(
        kernel,
        out_shape=[jax.ShapeDtypeStruct(s, jnp.float32) for s in shapes],
        in_specs=[pl.BlockSpec(memory_space=pltpu.SMEM)] + [WHOLE] * len(args),
        out_specs=[WHOLE] * len(shapes),
        scratch_shapes=[pltpu.VMEM(s, jnp.float32) for s in scratch],
        compiler_params=pltpu.CompilerParams(vmem_limit_bytes=room << 20),
        cost_estimate=pl.CostEstimate(
            flops=flops, bytes_accessed=4 * sum(a.size for a in args), transcendentals=0
        ),
    )(place, *args)


def local(orbitals, projectors, potential):
    v, xi = to_cells(orbitals, projectors)
    full = v.shape
    blocks, planes, rows, columns, lanes = full
    flat = (blocks, planes * rows * columns, lanes)
    total = blocks * lanes
    square = (total, total)
    xi = xi.reshape(flat)
    band = lax.axis_index(BAND)
    own = lax.dynamic_slice_in_dim(potential, (band + turn()) % blocks * rows, rows, 1)
    own = jnp.broadcast_to(own[..., None], (planes, rows, columns, lanes))
    pairs = len(pairs_of(blocks))

    def packed(count):
        return (BLOCK * count, BLOCK), (BLOCK * count // 2, BLOCK)

    small, small_half = packed(pairs + blocks * blocks)
    large, large_half = packed(blocks * (blocks - 1) + blocks + 2 + blocks * blocks)
    sums = (3 * blocks // 2, BLOCK)
    stats_shape = (2 * blocks, BLOCK)
    stats_list = []
    around = neighbours(v)
    mine, other = total_everywhere(*call(gram_kernel, [small_half] * 2, v.reshape(flat), xi, scratch=[small]))
    (x,) = call(first_factor_kernel, [square], mine, other, flops=20_000_000_000, room=16)
    vp, w, mine, other = call(
        first_transform_kernel, [flat, full, large_half, large_half], x, mine, other, v, *around, own, xi,
        scratch=[square, full, large],
    )
    for iteration in range(1, ITERS):
        around = neighbours(w)
        mine, other = total_everywhere(mine, other)
        x, stats = call(factor_kernel, [square, stats_shape], mine, other, flops=20_000_000_000, room=16)
        stats_list.append(stats)
        given = (x, stats, mine, other, vp, w, *around, own, xi)
        if iteration < ITERS - 1:
            vp, w, mine, other = call(
                transform_kernel, [flat, full, large_half, large_half], *given,
                scratch=[square, full, large],
            )
    both = (blocks, 2, planes, rows, columns, lanes)
    parts, mine, other = call(
        last_transform_kernel, [both, sums, sums], *given, scratch=[square, full]
    )
    parts = [parts[0]] + [lax.ppermute(parts[k], BAND, ring(blocks, k)) for k in range(1, blocks)]
    lines = (mine + swapped(other)).reshape(-1, LINES, lanes)
    here = from_every_chip(lines)
    here = here.reshape(lax.axis_size(CHIPS), *sums)
    v, stats = call(
        last_kernel, [(planes, blocks * rows, columns, lanes), stats_shape], *parts, here, swapped(here)
    )
    stats_list.append(stats)
    stats = jnp.stack(stats_list).reshape(ITERS, 2, blocks, lanes)
    stats = lax.dynamic_slice_in_dim(stats, band, 1, 2)[:, :, 0]
    return (v, stats[:, 0], jnp.sqrt(stats[:, 1]))


def solution(mesh):
    finer = Mesh(mesh.devices.reshape(mesh.shape["grid"], 2, 2), ("grid", "band_0", "band_1"))
    placed = (P("grid", None, None, BAND), P("grid", None, None, BAND), P("grid", None, None))
    return jax.shard_map(
        local,
        mesh=finer,
        in_specs=placed,
        out_specs=(P("grid", None, None, BAND), P(None, BAND), P(None, BAND)),
        check_vma=False,
    )
```

```python
import jax
import jax.numpy as jnp
from jax import lax
from jax.experimental import pallas as pl
from jax.experimental.pallas import tpu as pltpu
from jax.sharding import Mesh
from jax.sharding import PartitionSpec as P

ITERS = 3
BAND = ("band_0", "band_1")
CHIPS = ("grid", "band_0")
EVERY = ("grid", "band_0", "band_1")
BLOCK = 128
TILE = 8
HALF = 64
LINES = 2

STENCIL = (-205.0 / 72.0, 8.0 / 5.0, -1.0 / 5.0, 8.0 / 315.0, -1.0 / 560.0)
STEP_LENGTH = 0.25
NORM_EPS = 1e-06
WHOLE = pl.BlockSpec(memory_space=pltpu.VMEM)


def split(x):
    high = x.astype(jnp.bfloat16)
    return high, (x - high.astype(jnp.float32)).astype(jnp.bfloat16)


def dot_parts(left, right, sides):
    (lh, ll), (rh, rl) = left, right

    def once(a, b):
        return lax.dot_general(
            a, b, ((sides[:1], sides[1:]), ((), ())), preferred_element_type=jnp.float32
        )

    return once(lh, rl) + once(ll, rh) + once(lh, rh)


def dot(left, right, sides):
    return dot_parts(split(left), split(right), sides)


def lanes_of(parts, start, stop):
    return tuple(part[:, start:stop] for part in parts)


def row_of(tile, j):
    return jnp.broadcast_to(tile[j:j + 1, :], tile.shape)


def lane_of(tile, j):
    return jnp.broadcast_to(tile[:, j:j + 1], tile.shape)


def inverse_factor(tiles):
    count = len(tiles)
    lane = lax.broadcasted_iota(jnp.int32, tiles[0].shape, 1)
    sub = lax.broadcasted_iota(jnp.int32, tiles[0].shape, 0)
    tiles = list(tiles)
    head = [lane_of(tiles[0], j) for j in range(TILE)]
    for p in range(count):
        base = TILE * p
        inside = (lane >= base) & (lane < base + TILE)
        own = jnp.where(inside, (lane == base + sub).astype(jnp.float32), tiles[p])
        ahead = p + 1 < count
        if ahead:
            coming = [lane_of(tiles[p + 1], base + TILE + j) for j in range(TILE)]
        rows, crosses = [], []
        for j in range(TILE):
            scale = lax.rsqrt(row_of(head[j], j))
            row = row_of(own, j) * scale
            column = jnp.where(sub > j, head[j] * scale, 0.0)
            own = jnp.where(sub == j, row, own - column * row)
            cross = [None] * TILE
            for k in range(j + 1, TILE):
                cross[k] = row_of(head[k], j) * scale
                head[k] = head[k] - column * cross[k]
                cross[k] = cross[k] * scale
            rows.append(row * scale)
            crosses.append(cross)
            if ahead:
                if j == 0:
                    parts = [lane_of(tiles[p + 1], base + k) for k in range(TILE)]
                    following = jnp.where(inside, 0.0, tiles[p + 1])
                following = following - parts[j] * rows[j]
                for k in range(j + 1, TILE):
                    parts[k] = parts[k] - parts[j] * crosses[j][k]
                scaled = parts[j] * (scale * scale)
                for k in range(TILE):
                    coming[k] = coming[k] - scaled * row_of(parts[j], k)
        tiles[p] = jnp.where((lane < base + TILE) | (lane >= TILE * count), own, 0.0)
        if ahead:
            tiles[p + 1] = following
            head = coming
        for t in range(p + 2, count):
            parts = [lane_of(tiles[t], base + j) for j in range(TILE)]
            tile = jnp.where(inside, 0.0, tiles[t])
            for j in range(TILE):
                tile = tile - parts[j] * rows[j]
                for k in range(j + 1, TILE):
                    parts[k] = parts[k] - parts[j] * crosses[j][k]
            tiles[t] = tile
    return tiles


def pairs_of(blocks):
    return [(i, j) for i in range(blocks) for j in range(i, blocks)]


def cut(x, b):
    return x[:, BLOCK * b : BLOCK * (b + 1)]


def rows_at(ref, at):
    return ref[BLOCK * at : BLOCK * (at + 1), :]


def block_of(core, mine_ref, other_ref, at):
    half = mine_ref.shape[0] // BLOCK
    mine, other = rows_at(mine_ref, at % half), rows_at(other_ref, at % half)
    here = jnp.full(mine.shape, core, jnp.int32) == at // half
    return jnp.where(here, mine, other)


def spread(x_ref, own, at):
    size = x_ref.shape[0]
    start, stop = BLOCK * at, BLOCK * (at + 1)
    here, below = slice(start, stop), slice(stop, size)
    around = [x_ref[here, part] for part in (slice(0, start), slice(stop, size)) if part.stop > part.start]
    sides = dot(own, jnp.concatenate(around, axis=1), (1, 0))
    row = jnp.concatenate(
        [part for part in (sides[:, :start], own, sides[:, start:]) if part.shape[1]], axis=1
    )
    x_ref[here, :] = row
    if stop < size:
        parts = split(row)
        change = dot_parts(lanes_of(parts, stop, size), parts, (0, 0))
        x_ref[below, here] = -change[:, here]
        x_ref[below, below] = x_ref[below, below] - change[:, stop:]
        if start:
            x_ref[below, :start] = x_ref[below, :start] - change[:, :start]


def factorize(x_ref):
    blocks = x_ref.shape[0] // BLOCK
    block_row = lax.broadcasted_iota(jnp.int32, (BLOCK, BLOCK), 0)
    block_lane = lax.broadcasted_iota(jnp.int32, (BLOCK, BLOCK), 1)

    def step(k, carry):
        first = pl.multiple_of(k * BLOCK, BLOCK)
        here = pl.ds(first, BLOCK)

        def part(h, carry):
            top = first + HALF * h
            rows = [pl.ds(pl.multiple_of(top + TILE * t, TILE), TILE) for t in range(HALF // TILE)]
            tiles = inverse_factor([pltpu.roll(x_ref[r, here], HALF * h, 1) for r in rows])
            for r, tile in zip(rows, tiles):
                x_ref[r, here] = pltpu.roll(tile, HALF * h, 1)

            @pl.when(h == 0)
            def _():
                upper = x_ref[pl.ds(first, HALF), here]
                below = pl.ds(pl.multiple_of(first + HALF, HALF), HALF)
                change = dot(upper, upper, (0, 0))[HALF:, :]
                lane = lax.broadcasted_iota(jnp.int32, change.shape, 1)
                x_ref[below, here] = jnp.where(lane < HALF, 0.0, x_ref[below, here]) - change

            return carry

        lax.fori_loop(0, 2, part, 0)
        own = jnp.where((block_row < HALF) & (block_lane >= HALF), 0.0, x_ref[here, here])
        for at in range(blocks):
            @pl.when(k == at)
            def _(at=at):
                spread(x_ref, own, at)

        return carry

    lax.fori_loop(0, blocks, step, 0)
    for i in range(blocks - 1):
        x_ref[BLOCK * i : BLOCK * (i + 1), BLOCK * (i + 1) :] = jnp.zeros(
            (BLOCK, BLOCK * (blocks - 1 - i)), jnp.float32
        )


def first_factor_kernel(core_ref, mine_ref, other_ref, x_ref):
    blocks = x_ref.shape[0] // BLOCK
    for at, (i, j) in enumerate(pairs_of(blocks)):
        x_ref[BLOCK * i : BLOCK * (i + 1), BLOCK * j : BLOCK * (j + 1)] = block_of(
            core_ref[0], mine_ref, other_ref, at
        )
    factorize(x_ref)


def squared_of(rayleigh, energy, weight):
    return jnp.maximum(energy - 2.0 * rayleigh * rayleigh + rayleigh * rayleigh * weight, 0.0)


def length_of(squared):
    return STEP_LENGTH / jnp.sqrt(squared + NORM_EPS)


def apart_of(blocks):
    return [(i, j) for i in range(blocks) for j in range(i + 1, blocks)]


def factor_kernel(core_ref, mine_ref, other_ref, x_ref, stats_ref):
    blocks = x_ref.shape[0] // BLOCK
    apart = apart_of(blocks)
    row = lax.broadcasted_iota(jnp.int32, (BLOCK, BLOCK), 0)
    lane = lax.broadcasted_iota(jnp.int32, (BLOCK, BLOCK), 1)

    def block(at):
        return block_of(core_ref[0], mine_ref, other_ref, at)

    def upright(line):
        return jnp.sum(jnp.where(row == lane, line, 0.0), axis=1, keepdims=True)

    lines = block(2 * len(apart) + blocks)[: 3 * blocks]
    rayleigh, energy, weight = (lines[blocks * k : blocks * (k + 1)] for k in range(3))
    squared = squared_of(rayleigh, energy, weight)
    stats_ref[:blocks, :] = rayleigh
    stats_ref[blocks:, :] = squared
    length = length_of(squared)
    gain = 1.0 + rayleigh * length
    diagonal = (length * energy - 2.0 * gain * rayleigh) * length + gain * gain * weight
    d = [length[b : b + 1] for b in range(blocks)]
    a = [gain[b : b + 1] for b in range(blocks)]
    d_up = [upright(line) for line in d]
    a_up = [upright(line) for line in a]
    for at, (i, j) in enumerate(apart):
        x_ref[BLOCK * i : BLOCK * (i + 1), BLOCK * j : BLOCK * (j + 1)] = (
            d_up[i] * d[j]
        ) * block(len(apart) + at) - (a_up[i] * d[j] + d_up[i] * a[j]) * block(at)
    for b in range(blocks):
        both = block(2 * len(apart) + b)
        energies = jnp.transpose(jnp.where(row > lane, both, 0.0))
        upper = (d_up[b] * d[b]) * energies - (a_up[b] * d[b] + d_up[b] * a[b]) * both
        upper = jnp.where(row < lane, upper, 0.0)
        x_ref[BLOCK * b : BLOCK * (b + 1), BLOCK * b : BLOCK * (b + 1)] = (
            upper + jnp.transpose(upper) + jnp.where(row == lane, diagonal[b : b + 1], 0.0)
        )
    factorize(x_ref)


def joined(ref):
    return jnp.concatenate([ref[b] for b in range(ref.shape[0])], axis=1)


def share_out(core, packed_ref, mine_ref, other_ref):
    half = mine_ref.shape[0]
    mine_ref[...] = packed_ref[pl.ds(pl.multiple_of(core * half, TILE), half), :]
    other_ref[...] = packed_ref[pl.ds(pl.multiple_of((1 - core) * half, TILE), half), :]


def write_pairs(left, right, at, packed_ref):
    blocks = left.shape[1] // BLOCK
    for i in range(blocks):
        row = dot(cut(left, i), right[:, BLOCK * i :], (0, 0))
        for j in range(blocks - i):
            packed_ref[BLOCK * at : BLOCK * (at + 1), :] = cut(row, j)
            at += 1
    return at


def write_coupling(xi, v, at, packed_ref):
    c = dot_parts(xi, v, (0, 0))
    blocks = c.shape[1] // BLOCK
    for j in range(blocks):
        packed_ref[BLOCK * at : BLOCK * (at + blocks), :] = cut(c, j)
        at += blocks
    return at


def gram_kernel(core_ref, v_ref, xi_ref, mine_ref, other_ref, packed_ref):
    v = joined(v_ref)
    at = write_pairs(v, v, 0, packed_ref)
    write_coupling(split(joined(xi_ref)), split(v), at, packed_ref)
    share_out(core_ref[0], packed_ref, mine_ref, other_ref)


def totals_of(core, mine_ref, other_ref):
    mine = jnp.sum(mine_ref[...], axis=0)
    other = jnp.sum(other_ref[...], axis=0)
    first = jnp.full(mine.shape, core, jnp.int32) == 0
    return jnp.concatenate([jnp.where(first, mine, other), jnp.where(first, other, mine)], axis=0)


def along_lanes(rows, at, blocks):
    return jnp.concatenate([rows[at + b : at + b + 1] for b in range(blocks)], axis=1)


def last_kernel(
    core_ref, own_ref, near_ref, across_ref, far_ref, here_ref, there_ref, *refs,
):
    planes, rows = own_ref.shape[1:3]
    totals = totals_of(core_ref[0], here_ref, there_ref)
    blocks = totals.shape[0] // 3
    rayleigh, energy, weight = (totals[blocks * k : blocks * (k + 1)] for k in range(3))
    *earlier, v_ref, quotients_ref, norms_ref, stats_ref = refs
    stats_ref[:blocks, :] = rayleigh
    stats_ref[blocks:, :] = squared_of(rayleigh, energy, weight)
    for at, ref in enumerate((*earlier, stats_ref)):
        rayleigh, squared = (ref[pl.ds(blocks * k + core_ref[1], 1), :] for k in range(2))
        quotients_ref[at : at + 1, :] = rayleigh
        norms_ref[at : at + 1, :] = jnp.sqrt(squared)
    length = length_of(squared)
    for away, ref in enumerate((own_ref, near_ref, across_ref, far_ref)):
        first_row = rows * lax.rem(core_ref[1] + core_ref[2] + blocks - away, blocks)
        for z in range(planes):
            for x in range(rows):
                vp = ref[0, z, x]
                v_ref[z, first_row + x] = vp - (ref[1, z, x] - rayleigh * vp) * length


def local_part(core_ref, v_ref, around, p_ref, u_ref):
    far_ref, close_ref, left_ref, right_ref = around

    @pl.when(core_ref[3] == 0)
    def _():
        apply_local(v_ref, far_ref, close_ref, left_ref, right_ref, p_ref, u_ref)

    @pl.when(core_ref[3] != 0)
    def _():
        apply_local(v_ref, close_ref, far_ref, left_ref, right_ref, p_ref, u_ref)


def apply_local(v_ref, below_ref, above_ref, left_ref, right_ref, p_ref, u_ref):
    blocks, planes, rows, columns, _ = v_ref.shape
    along_z = [(ref, z) for ref in (below_ref, v_ref, above_ref) for z in range(planes)]
    along_x = [(ref, x) for ref in (left_ref, v_ref, right_ref) for x in range(rows)]

    def one(b, carry):
        for z in range(planes):
            for x in range(rows):
                centre = v_ref[b, z, x]
                total = 3.0 * STENCIL[0] * centre
                for d in range(1, 5):
                    group = pltpu.roll(centre, d, 0) + pltpu.roll(centre, columns - d, 0)
                    for way in (d, -d):
                        ref, at = along_z[planes + z + way]
                        group = group + ref[b, at, x]
                        ref, at = along_x[rows + x + way]
                        group = group + ref[b, z, at]
                    total = total + STENCIL[d] * group
                u_ref[b, z, x] = p_ref[z, x] * centre - 0.5 * total
        return carry

    lax.fori_loop(0, blocks, one, 0)


def flat_lanes(ref):
    blocks, planes, rows, columns, lanes = ref.shape
    return jnp.concatenate(
        [ref[b].reshape(planes * rows * columns, lanes) for b in range(blocks)], axis=1
    )


def fill_coupling(c_ref, core, mine_ref, other_ref, at):
    blocks = c_ref.shape[1] // BLOCK
    for j in range(blocks):
        for i in range(blocks):
            c_ref[BLOCK * i : BLOCK * (i + 1), BLOCK * j : BLOCK * (j + 1)] = block_of(
                core, mine_ref, other_ref, at
            )
            at += 1


def transformed(v, x):
    middle = x.shape[0] // 2
    parts = split(v)
    return jnp.concatenate(
        [
            dot_parts(lanes_of(parts, 0, middle), split(x[:middle, :middle]), (1, 1)),
            dot_parts(parts, split(x[middle:, :]), (1, 1)),
        ],
        axis=1,
    )


def line_sums(product):
    total = jnp.sum(product, axis=0, keepdims=True)
    return [cut(total, b) for b in range(product.shape[1] // BLOCK)]


def finish(core, band, vp, w, xi, vp_ref, w_ref, packed_ref, mine_ref, other_ref):
    blocks = vp.shape[1] // BLOCK
    if packed_ref is None:
        for b in range(blocks):
            away = lax.rem(b + blocks - band, blocks)
            vp_ref[away, 0] = cut(vp, b).reshape(vp_ref.shape[2:])
            vp_ref[away, 1] = cut(w, b).reshape(vp_ref.shape[2:])
        lines = line_sums(vp * w) + line_sums(w * w) + line_sums(vp * vp)
        half = len(lines) // 2
        first, second = (jnp.concatenate(part, axis=0) for part in (lines[:half], lines[half:]))
        front = jnp.full(first.shape, core, jnp.int32) == 0
        mine_ref[...] = jnp.where(front, first, second)
        other_ref[...] = jnp.where(front, second, first)
        return
    for b in range(blocks):
        vp_ref[b] = cut(vp, b)
        w_ref[b] = cut(w, b).reshape(w_ref.shape[1:])
    row = lax.broadcasted_iota(jnp.int32, (BLOCK, BLOCK), 0)
    lane = lax.broadcasted_iota(jnp.int32, (BLOCK, BLOCK), 1)
    count = blocks * (blocks - 1) // 2
    at = 0

    def put(at, value):
        packed_ref[BLOCK * at : BLOCK * (at + 1), :] = value

    left, right = split(vp), split(w)
    total, middle = w.shape[1], w.shape[1] // 2
    for i in range(blocks):
        top = BLOCK * i // middle * middle
        if BLOCK * i == top:
            products, energies = (
                dot_parts(lanes_of(p, top, top + middle), lanes_of(right, top, total), (0, 0))
                for p in (left, right)
            )
        lines = slice(BLOCK * i - top, BLOCK * (i + 1) - top)
        for j in range(i, blocks):
            lanes = slice(BLOCK * j - top, BLOCK * (j + 1) - top)
            if i == j:
                put(2 * count + i, jnp.where(row <= lane, products[lines, lanes], energies[lines, lanes]))
            else:
                put(at, products[lines, lanes])
                put(count + at, energies[lines, lanes])
                at += 1
    at = 2 * count + blocks
    put(at, jnp.zeros((BLOCK, BLOCK), jnp.float32))
    lines = line_sums(vp * w) + line_sums(w * w) + line_sums(vp * vp)
    packed_ref[BLOCK * at : BLOCK * at + len(lines), :] = jnp.concatenate(lines, axis=0)
    at = write_coupling(split(xi), right, at + 1, packed_ref)
    put(at, jnp.zeros((BLOCK, BLOCK), jnp.float32))
    share_out(core, packed_ref, mine_ref, other_ref)


def first_transform_kernel(
    core_ref, x_ref, in_mine_ref, in_other_ref, v_ref, far_ref, close_ref, left_ref, right_ref, p_ref,
    xi_ref, vp_ref, w_ref, mine_ref, other_ref, c_ref, u_ref, packed_ref,
):
    blocks = v_ref.shape[0]
    at = len(pairs_of(blocks))
    fill_coupling(c_ref, core_ref[0], in_mine_ref, in_other_ref, at)
    local_part(core_ref, v_ref, (far_ref, close_ref, left_ref, right_ref), p_ref, u_ref)
    v = flat_lanes(v_ref)
    xi = joined(xi_ref)
    z = flat_lanes(u_ref) - dot(xi, c_ref[...], (1, 0))
    both = transformed(jnp.concatenate([v, z], axis=0), x_ref[...])
    finish(
        core_ref[0], core_ref[1], both[: v.shape[0]], both[v.shape[0] :], xi, vp_ref, w_ref, packed_ref, mine_ref,
        other_ref,
    )


def stepped(vp, w, y, stats, blocks):
    rayleigh = along_lanes(stats, 0, blocks)
    length = length_of(along_lanes(stats, blocks, blocks))
    return vp - (w - rayleigh * vp) * length, w - (y - rayleigh * w) * length


def last_transform_kernel(*refs):
    outs = 14
    transform_kernel(*refs[:outs], None, *refs[outs:], None)


def transform_kernel(
    core_ref, x_ref, stats_ref, in_mine_ref, in_other_ref, old_ref, v_ref, far_ref, close_ref, left_ref,
    right_ref, p_ref, xi_ref, vp_ref, w_ref, mine_ref, other_ref, c_ref, u_ref, packed_ref,
):
    blocks = v_ref.shape[0]
    at = 2 * len(apart_of(blocks)) + blocks + 1
    fill_coupling(c_ref, core_ref[0], in_mine_ref, in_other_ref, at)
    local_part(core_ref, v_ref, (far_ref, close_ref, left_ref, right_ref), p_ref, u_ref)
    xi = joined(xi_ref)
    y = flat_lanes(u_ref) - dot(xi, c_ref[...], (1, 0))
    v, z = stepped(joined(old_ref), flat_lanes(v_ref), y, stats_ref[...], blocks)
    both = transformed(jnp.concatenate([v, z], axis=0), x_ref[...])
    finish(
        core_ref[0], core_ref[1], both[: v.shape[0]], both[v.shape[0] :], xi, vp_ref, w_ref, packed_ref, mine_ref,
        other_ref,
    )


def ring(count, by):
    return [(i, (i + by) % count) for i in range(count)]


def turn():
    far = lax.axis_index("grid") // (lax.axis_size("grid") // 2)
    return far * (lax.axis_size(BAND) // 2)


def slab_pairs(start):
    slabs, quarters = lax.axis_size("grid"), lax.axis_size(BAND)

    def pair(g, b):
        there = (g + (1 if g % 2 == start else -1)) % slabs
        crosses = g // (slabs // 2) != there // (slabs // 2)
        return g * quarters + b, there * quarters + (b + crosses * (quarters // 2)) % quarters

    return [pair(g, b) for g in range(slabs) for b in range(quarters)]


def neighbours(v):
    near = lax.axis_size(BAND)
    far = lax.ppermute(v, EVERY, slab_pairs(1))
    close = lax.ppermute(v, EVERY, slab_pairs(0))
    return far, close, lax.ppermute(v, BAND, ring(near, 1)), lax.ppermute(v, BAND, ring(near, -1))


def swapped(x):
    return lax.ppermute(x, "band_1", ring(lax.axis_size("band_1"), 1))


def exchange(pieces):
    return lax.all_to_all(pieces, CHIPS, split_axis=0, concat_axis=0, tiled=True)


def from_every_chip(x):
    count = lax.axis_size(CHIPS)
    copies = jnp.broadcast_to(x, (count, *x.shape)).reshape(count * x.shape[0], *x.shape[1:])
    return exchange(copies)


def total_everywhere(mine, other):
    rows, lanes = mine.shape
    count = lax.axis_size(CHIPS)
    pieces = (mine + swapped(other)).reshape(rows // LINES, LINES, lanes)
    arrived = exchange(pieces)
    total = arrived.reshape(count, rows // LINES // count, LINES, lanes).sum(axis=0)
    half = from_every_chip(total).reshape(rows, lanes)
    return half, swapped(half)


def pieces_kernel(core_ref, first_ref, second_ref, out_ref):
    quarters, _, planes, rows, _, _ = out_ref.shape
    for q in range(quarters):
        first_row = rows * lax.rem(core_ref[2] + q, quarters)
        for k, ref in enumerate((first_ref, second_ref)):
            for z in range(planes):
                for x in range(rows):
                    out_ref[q, k, z, x] = ref[z, first_row + x]


def to_cells(first, second):
    quarters = lax.axis_size(BAND)
    z, x, y, lanes = first.shape
    shape = (quarters, 2, z, x // quarters, y, lanes)
    (pieces,) = call(pieces_kernel, [shape], first, second, flops=1_000_000)
    pieces = lax.all_to_all(pieces, BAND, split_axis=0, concat_axis=0, tiled=True)
    return pieces[:, 0], pieces[:, 1]


def call(kernel, shapes, *args, scratch=(), flops=2_000_000_000, room=32):
    place = [lax.axis_index("band_1"), lax.axis_index(BAND), turn(), lax.axis_index("grid") % 2]
    place = jnp.stack(place).astype(jnp.int32)
    return pl.pallas_call(
        kernel,
        out_shape=[jax.ShapeDtypeStruct(s, jnp.float32) for s in shapes],
        in_specs=[pl.BlockSpec(memory_space=pltpu.SMEM)] + [WHOLE] * len(args),
        out_specs=[WHOLE] * len(shapes),
        scratch_shapes=[pltpu.VMEM(s, jnp.float32) for s in scratch],
        compiler_params=pltpu.CompilerParams(vmem_limit_bytes=room << 20),
        cost_estimate=pl.CostEstimate(
            flops=flops, bytes_accessed=4 * sum(a.size for a in args), transcendentals=0
        ),
    )(place, *args)


def local(orbitals, projectors, potential):
    v, xi = to_cells(orbitals, projectors)
    full = v.shape
    blocks, planes, rows, columns, lanes = full
    flat = (blocks, planes * rows * columns, lanes)
    total = blocks * lanes
    square = (total, total)
    xi = xi.reshape(flat)
    band = lax.axis_index(BAND)
    own = lax.dynamic_slice_in_dim(potential, (band + turn()) % blocks * rows, rows, 1)
    own = jnp.broadcast_to(own[..., None], (planes, rows, columns, lanes))
    pairs = len(pairs_of(blocks))

    def packed(count):
        return (BLOCK * count, BLOCK), (BLOCK * count // 2, BLOCK)

    small, small_half = packed(pairs + blocks * blocks)
    large, large_half = packed(blocks * (blocks - 1) + blocks + 2 + blocks * blocks)
    sums = (3 * blocks // 2, BLOCK)
    stats_shape = (2 * blocks, BLOCK)
    stats_list = []
    around = neighbours(v)
    mine, other = total_everywhere(*call(gram_kernel, [small_half] * 2, v.reshape(flat), xi, scratch=[small]))
    (x,) = call(first_factor_kernel, [square], mine, other, flops=20_000_000_000, room=16)
    vp, w, mine, other = call(
        first_transform_kernel, [flat, full, large_half, large_half], x, mine, other, v, *around, own, xi,
        scratch=[square, full, large],
    )
    for iteration in range(1, ITERS):
        around = neighbours(w)
        mine, other = total_everywhere(mine, other)
        x, stats = call(factor_kernel, [square, stats_shape], mine, other, flops=20_000_000_000, room=16)
        stats_list.append(stats)
        given = (x, stats, mine, other, vp, w, *around, own, xi)
        if iteration < ITERS - 1:
            vp, w, mine, other = call(
                transform_kernel, [flat, full, large_half, large_half], *given,
                scratch=[square, full, large],
            )
    both = (blocks, 2, planes, rows, columns, lanes)
    parts, mine, other = call(
        last_transform_kernel, [both, sums, sums], *given, scratch=[square, full]
    )
    parts = [parts[0]] + [lax.ppermute(parts[k], BAND, ring(blocks, k)) for k in range(1, blocks)]
    lines = (mine + swapped(other)).reshape(-1, LINES, lanes)
    here = from_every_chip(lines)
    here = here.reshape(lax.axis_size(CHIPS), *sums)
    lines = (ITERS, lanes)
    return tuple(
        call(
            last_kernel, [(planes, blocks * rows, columns, lanes), lines, lines], *parts, here,
            swapped(here), *stats_list, scratch=[stats_shape],
        )
    )


def solution(mesh):
    finer = Mesh(mesh.devices.reshape(mesh.shape["grid"], 2, 2), ("grid", "band_0", "band_1"))
    placed = (P("grid", None, None, BAND), P("grid", None, None, BAND), P("grid", None, None))
    return jax.shard_map(
        local,
        mesh=finer,
        in_specs=placed,
        out_specs=(P("grid", None, None, BAND), P(None, BAND), P(None, BAND)),
        check_vma=False,
    )
```

```python
import jax
import jax.numpy as jnp
from jax import lax
from jax.experimental import pallas as pl
from jax.experimental.pallas import tpu as pltpu
from jax.sharding import Mesh
from jax.sharding import PartitionSpec as P

ITERS = 3
BAND = ("band_0", "band_1")
CHIPS = ("grid", "band_0")
EVERY = ("grid", "band_0", "band_1")
BLOCK = 128
TILE = 8
HALF = 64
LINES = 2

STENCIL = (-205.0 / 72.0, 8.0 / 5.0, -1.0 / 5.0, 8.0 / 315.0, -1.0 / 560.0)
STEP_LENGTH = 0.25
NORM_EPS = 1e-06
WHOLE = pl.BlockSpec(memory_space=pltpu.VMEM)


def split(x):
    high = x.astype(jnp.bfloat16)
    return high, (x - high.astype(jnp.float32)).astype(jnp.bfloat16)


def dot_parts(left, right, sides):
    (lh, ll), (rh, rl) = left, right

    def once(a, b):
        return lax.dot_general(
            a, b, ((sides[:1], sides[1:]), ((), ())), preferred_element_type=jnp.float32
        )

    return once(lh, rl) + once(ll, rh) + once(lh, rh)


def dot(left, right, sides):
    return dot_parts(split(left), split(right), sides)


def lanes_of(parts, start, stop):
    return tuple(part[:, start:stop] for part in parts)


def row_of(tile, j):
    return jnp.broadcast_to(tile[j:j + 1, :], tile.shape)


def lane_of(tile, j):
    return jnp.broadcast_to(tile[:, j:j + 1], tile.shape)


def inverse_factor(tiles):
    count = len(tiles)
    lane = lax.broadcasted_iota(jnp.int32, tiles[0].shape, 1)
    sub = lax.broadcasted_iota(jnp.int32, tiles[0].shape, 0)
    tiles = list(tiles)
    head = [lane_of(tiles[0], j) for j in range(TILE)]
    for p in range(count):
        base = TILE * p
        inside = (lane >= base) & (lane < base + TILE)
        own = jnp.where(inside, (lane == base + sub).astype(jnp.float32), tiles[p])
        ahead = p + 1 < count
        if ahead:
            coming = [lane_of(tiles[p + 1], base + TILE + j) for j in range(TILE)]
        rows, crosses = [], []
        for j in range(TILE):
            scale = lax.rsqrt(row_of(head[j], j))
            row = row_of(own, j) * scale
            column = jnp.where(sub > j, head[j] * scale, 0.0)
            own = jnp.where(sub == j, row, own - column * row)
            cross = [None] * TILE
            for k in range(j + 1, TILE):
                cross[k] = row_of(head[k], j) * scale
                head[k] = head[k] - column * cross[k]
                cross[k] = cross[k] * scale
            rows.append(row * scale)
            crosses.append(cross)
            if ahead:
                if j == 0:
                    parts = [lane_of(tiles[p + 1], base + k) for k in range(TILE)]
                    following = jnp.where(inside, 0.0, tiles[p + 1])
                following = following - parts[j] * rows[j]
                for k in range(j + 1, TILE):
                    parts[k] = parts[k] - parts[j] * crosses[j][k]
                scaled = parts[j] * (scale * scale)
                for k in range(TILE):
                    coming[k] = coming[k] - scaled * row_of(parts[j], k)
        tiles[p] = jnp.where((lane < base + TILE) | (lane >= TILE * count), own, 0.0)
        if ahead:
            tiles[p + 1] = following
            head = coming
        for t in range(p + 2, count):
            parts = [lane_of(tiles[t], base + j) for j in range(TILE)]
            tile = jnp.where(inside, 0.0, tiles[t])
            for j in range(TILE):
                tile = tile - parts[j] * rows[j]
                for k in range(j + 1, TILE):
                    parts[k] = parts[k] - parts[j] * crosses[j][k]
            tiles[t] = tile
    return tiles


def pairs_of(blocks):
    return [(i, j) for i in range(blocks) for j in range(i, blocks)]


def cut(x, b):
    return x[:, BLOCK * b : BLOCK * (b + 1)]


def rows_at(ref, at):
    return ref[BLOCK * at : BLOCK * (at + 1), :]


def block_of(core, mine_ref, other_ref, at):
    half = mine_ref.shape[0] // BLOCK
    mine, other = rows_at(mine_ref, at % half), rows_at(other_ref, at % half)
    here = jnp.full(mine.shape, core, jnp.int32) == at // half
    return jnp.where(here, mine, other)


def spread(x_ref, own, at):
    size = x_ref.shape[0]
    start, stop = BLOCK * at, BLOCK * (at + 1)
    here, below = slice(start, stop), slice(stop, size)
    around = [x_ref[here, part] for part in (slice(0, start), slice(stop, size)) if part.stop > part.start]
    sides = dot(own, jnp.concatenate(around, axis=1), (1, 0))
    row = jnp.concatenate(
        [part for part in (sides[:, :start], own, sides[:, start:]) if part.shape[1]], axis=1
    )
    x_ref[here, :] = row
    if stop < size:
        parts = split(row)
        change = dot_parts(lanes_of(parts, stop, size), parts, (0, 0))
        x_ref[below, here] = -change[:, here]
        x_ref[below, below] = x_ref[below, below] - change[:, stop:]
        if start:
            x_ref[below, :start] = x_ref[below, :start] - change[:, :start]


def factorize(x_ref):
    blocks = x_ref.shape[0] // BLOCK
    block_row = lax.broadcasted_iota(jnp.int32, (BLOCK, BLOCK), 0)
    block_lane = lax.broadcasted_iota(jnp.int32, (BLOCK, BLOCK), 1)

    def step(k, carry):
        first = pl.multiple_of(k * BLOCK, BLOCK)
        here = pl.ds(first, BLOCK)

        def part(h, carry):
            top = first + HALF * h
            rows = [pl.ds(pl.multiple_of(top + TILE * t, TILE), TILE) for t in range(HALF // TILE)]
            tiles = inverse_factor([pltpu.roll(x_ref[r, here], HALF * h, 1) for r in rows])
            for r, tile in zip(rows, tiles):
                x_ref[r, here] = pltpu.roll(tile, HALF * h, 1)

            @pl.when(h == 0)
            def _():
                upper = x_ref[pl.ds(first, HALF), here]
                below = pl.ds(pl.multiple_of(first + HALF, HALF), HALF)
                change = dot(upper, upper, (0, 0))[HALF:, :]
                lane = lax.broadcasted_iota(jnp.int32, change.shape, 1)
                x_ref[below, here] = jnp.where(lane < HALF, 0.0, x_ref[below, here]) - change

            return carry

        lax.fori_loop(0, 2, part, 0)
        own = jnp.where((block_row < HALF) & (block_lane >= HALF), 0.0, x_ref[here, here])
        for at in range(blocks):
            @pl.when(k == at)
            def _(at=at):
                spread(x_ref, own, at)

        return carry

    lax.fori_loop(0, blocks, step, 0)
    for i in range(blocks - 1):
        x_ref[BLOCK * i : BLOCK * (i + 1), BLOCK * (i + 1) :] = jnp.zeros(
            (BLOCK, BLOCK * (blocks - 1 - i)), jnp.float32
        )


def first_factor_kernel(core_ref, mine_ref, other_ref, x_ref):
    blocks = x_ref.shape[0] // BLOCK
    for at, (i, j) in enumerate(pairs_of(blocks)):
        x_ref[BLOCK * i : BLOCK * (i + 1), BLOCK * j : BLOCK * (j + 1)] = block_of(
            core_ref[0], mine_ref, other_ref, at
        )
    factorize(x_ref)


def squared_of(rayleigh, energy, weight):
    return jnp.maximum(energy - 2.0 * rayleigh * rayleigh + rayleigh * rayleigh * weight, 0.0)


def length_of(squared):
    return STEP_LENGTH / jnp.sqrt(squared + NORM_EPS)


def apart_of(blocks):
    return [(i, j) for i in range(blocks) for j in range(i + 1, blocks)]


def factor_kernel(core_ref, mine_ref, other_ref, x_ref, stats_ref):
    blocks = x_ref.shape[0] // BLOCK
    apart = apart_of(blocks)
    row = lax.broadcasted_iota(jnp.int32, (BLOCK, BLOCK), 0)
    lane = lax.broadcasted_iota(jnp.int32, (BLOCK, BLOCK), 1)

    def block(at):
        return block_of(core_ref[0], mine_ref, other_ref, at)

    def upright(line):
        return jnp.sum(jnp.where(row == lane, line, 0.0), axis=1, keepdims=True)

    lines = block(2 * len(apart) + blocks)[: 3 * blocks]
    rayleigh, energy, weight = (lines[blocks * k : blocks * (k + 1)] for k in range(3))
    squared = squared_of(rayleigh, energy, weight)
    stats_ref[:blocks, :] = rayleigh
    stats_ref[blocks:, :] = squared
    length = length_of(squared)
    gain = 1.0 + rayleigh * length
    diagonal = (length * energy - 2.0 * gain * rayleigh) * length + gain * gain * weight
    d = [length[b : b + 1] for b in range(blocks)]
    a = [gain[b : b + 1] for b in range(blocks)]
    d_up = [upright(line) for line in d]
    a_up = [upright(line) for line in a]
    for at, (i, j) in enumerate(apart):
        x_ref[BLOCK * i : BLOCK * (i + 1), BLOCK * j : BLOCK * (j + 1)] = (
            d_up[i] * d[j]
        ) * block(len(apart) + at) - (a_up[i] * d[j] + d_up[i] * a[j]) * block(at)
    for b in range(blocks):
        both = block(2 * len(apart) + b)
        energies = jnp.transpose(jnp.where(row > lane, both, 0.0))
        upper = (d_up[b] * d[b]) * energies - (a_up[b] * d[b] + d_up[b] * a[b]) * both
        upper = jnp.where(row < lane, upper, 0.0)
        x_ref[BLOCK * b : BLOCK * (b + 1), BLOCK * b : BLOCK * (b + 1)] = (
            upper + jnp.transpose(upper) + jnp.where(row == lane, diagonal[b : b + 1], 0.0)
        )
    factorize(x_ref)


def joined(ref):
    return jnp.concatenate([ref[b] for b in range(ref.shape[0])], axis=1)


def share_out(core, packed_ref, mine_ref, other_ref):
    half = mine_ref.shape[0]
    mine_ref[...] = packed_ref[pl.ds(pl.multiple_of(core * half, TILE), half), :]
    other_ref[...] = packed_ref[pl.ds(pl.multiple_of((1 - core) * half, TILE), half), :]


def write_pairs(left, right, at, packed_ref):
    blocks = left.shape[1] // BLOCK
    for i in range(blocks):
        row = dot(cut(left, i), right[:, BLOCK * i :], (0, 0))
        for j in range(blocks - i):
            packed_ref[BLOCK * at : BLOCK * (at + 1), :] = cut(row, j)
            at += 1
    return at


def write_coupling(xi, v, at, packed_ref):
    c = dot_parts(xi, v, (0, 0))
    blocks = c.shape[1] // BLOCK
    for j in range(blocks):
        packed_ref[BLOCK * at : BLOCK * (at + blocks), :] = cut(c, j)
        at += blocks
    return at


def gram_kernel(core_ref, v_ref, xi_ref, mine_ref, other_ref, packed_ref):
    v = joined(v_ref)
    at = write_pairs(v, v, 0, packed_ref)
    write_coupling(split(joined(xi_ref)), split(v), at, packed_ref)
    share_out(core_ref[0], packed_ref, mine_ref, other_ref)


def totals_of(core, mine_ref, other_ref):
    mine = jnp.sum(mine_ref[...], axis=0)
    other = jnp.sum(other_ref[...], axis=0)
    first = jnp.full(mine.shape, core, jnp.int32) == 0
    return jnp.concatenate([jnp.where(first, mine, other), jnp.where(first, other, mine)], axis=0)


def along_lanes(rows, at, blocks):
    return jnp.concatenate([rows[at + b : at + b + 1] for b in range(blocks)], axis=1)


def last_kernel(
    core_ref, own_ref, near_ref, across_ref, far_ref, here_ref, there_ref, *refs,
):
    planes, rows = own_ref.shape[1:3]
    totals = totals_of(core_ref[0], here_ref, there_ref)
    blocks = totals.shape[0] // 3
    rayleigh, energy, weight = (totals[blocks * k : blocks * (k + 1)] for k in range(3))
    *earlier, v_ref, quotients_ref, norms_ref, stats_ref = refs
    stats_ref[:blocks, :] = rayleigh
    stats_ref[blocks:, :] = squared_of(rayleigh, energy, weight)
    for at, ref in enumerate((*earlier, stats_ref)):
        rayleigh, squared = (ref[pl.ds(blocks * k + core_ref[1], 1), :] for k in range(2))
        quotients_ref[at : at + 1, :] = rayleigh
        norms_ref[at : at + 1, :] = jnp.sqrt(squared)
    length = length_of(squared)
    for away, ref in enumerate((own_ref, near_ref, across_ref, far_ref)):
        first_row = rows * lax.rem(core_ref[1] + core_ref[2] + blocks - away, blocks)
        for z in range(planes):
            for x in range(rows):
                vp = ref[0, z, x]
                v_ref[z, first_row + x] = vp - (ref[1, z, x] - rayleigh * vp) * length


def local_part(core_ref, v_ref, around, p_ref, u_ref):
    far_ref, close_ref, left_ref, right_ref = around

    @pl.when(core_ref[3] == 0)
    def _():
        apply_local(v_ref, far_ref, close_ref, left_ref, right_ref, p_ref, u_ref)

    @pl.when(core_ref[3] != 0)
    def _():
        apply_local(v_ref, close_ref, far_ref, left_ref, right_ref, p_ref, u_ref)


def apply_local(v_ref, below_ref, above_ref, left_ref, right_ref, p_ref, u_ref):
    blocks, planes, rows, columns, _ = v_ref.shape
    along_z = [(ref, z) for ref in (below_ref, v_ref, above_ref) for z in range(planes)]
    along_x = [(ref, x) for ref in (left_ref, v_ref, right_ref) for x in range(rows)]

    def one(b, carry):
        for z in range(planes):
            for x in range(rows):
                centre = v_ref[b, z, x]
                total = 3.0 * STENCIL[0] * centre
                for d in range(1, 5):
                    group = pltpu.roll(centre, d, 0) + pltpu.roll(centre, columns - d, 0)
                    for way in (d, -d):
                        ref, at = along_z[planes + z + way]
                        group = group + ref[b, at, x]
                        ref, at = along_x[rows + x + way]
                        group = group + ref[b, z, at]
                    total = total + STENCIL[d] * group
                u_ref[b, z, x] = p_ref[z, x] * centre - 0.5 * total
        return carry

    lax.fori_loop(0, blocks, one, 0)


def flat_lanes(ref):
    blocks, planes, rows, columns, lanes = ref.shape
    return jnp.concatenate(
        [ref[b].reshape(planes * rows * columns, lanes) for b in range(blocks)], axis=1
    )


def fill_coupling(c_ref, core, mine_ref, other_ref, at):
    blocks = c_ref.shape[1] // BLOCK
    for j in range(blocks):
        for i in range(blocks):
            c_ref[BLOCK * i : BLOCK * (i + 1), BLOCK * j : BLOCK * (j + 1)] = block_of(
                core, mine_ref, other_ref, at
            )
            at += 1


def transformed(v, x):
    middle = x.shape[0] // 2
    parts = split(v)
    return jnp.concatenate(
        [
            dot_parts(lanes_of(parts, 0, middle), split(x[:middle, :middle]), (1, 1)),
            dot_parts(parts, split(x[middle:, :]), (1, 1)),
        ],
        axis=1,
    )


def line_sums(product):
    total = jnp.sum(product, axis=0, keepdims=True)
    return [cut(total, b) for b in range(product.shape[1] // BLOCK)]


def finish(core, band, vp, w, xi, vp_ref, w_ref, packed_ref, mine_ref, other_ref):
    blocks = vp.shape[1] // BLOCK
    if packed_ref is None:
        for b in range(blocks):
            away = lax.rem(b + blocks - band, blocks)
            vp_ref[away, 0] = cut(vp, b).reshape(vp_ref.shape[2:])
            vp_ref[away, 1] = cut(w, b).reshape(vp_ref.shape[2:])
        lines = line_sums(vp * w) + line_sums(w * w) + line_sums(vp * vp)
        half = len(lines) // 2
        first, second = (jnp.concatenate(part, axis=0) for part in (lines[:half], lines[half:]))
        front = jnp.full(first.shape, core, jnp.int32) == 0
        mine_ref[...] = jnp.where(front, first, second)
        other_ref[...] = jnp.where(front, second, first)
        return
    for b in range(blocks):
        vp_ref[b] = cut(vp, b)
        w_ref[b] = cut(w, b).reshape(w_ref.shape[1:])
    row = lax.broadcasted_iota(jnp.int32, (BLOCK, BLOCK), 0)
    lane = lax.broadcasted_iota(jnp.int32, (BLOCK, BLOCK), 1)
    count = blocks * (blocks - 1) // 2
    at = 0

    def put(at, value):
        packed_ref[BLOCK * at : BLOCK * (at + 1), :] = value

    left, right = split(vp), split(w)
    total, middle = w.shape[1], w.shape[1] // 2
    for i in range(blocks):
        top = BLOCK * i // middle * middle
        if BLOCK * i == top:
            products, energies = (
                dot_parts(lanes_of(p, top, top + middle), lanes_of(right, top, total), (0, 0))
                for p in (left, right)
            )
        lines = slice(BLOCK * i - top, BLOCK * (i + 1) - top)
        for j in range(i, blocks):
            lanes = slice(BLOCK * j - top, BLOCK * (j + 1) - top)
            if i == j:
                put(2 * count + i, jnp.where(row <= lane, products[lines, lanes], energies[lines, lanes]))
            else:
                put(at, products[lines, lanes])
                put(count + at, energies[lines, lanes])
                at += 1
    at = 2 * count + blocks
    put(at, jnp.zeros((BLOCK, BLOCK), jnp.float32))
    lines = line_sums(vp * w) + line_sums(w * w) + line_sums(vp * vp)
    packed_ref[BLOCK * at : BLOCK * at + len(lines), :] = jnp.concatenate(lines, axis=0)
    at = write_coupling(split(xi), right, at + 1, packed_ref)
    put(at, jnp.zeros((BLOCK, BLOCK), jnp.float32))
    share_out(core, packed_ref, mine_ref, other_ref)


def first_transform_kernel(
    core_ref, x_ref, in_mine_ref, in_other_ref, v_ref, far_ref, close_ref, left_ref, right_ref, p_ref,
    xi_ref, vp_ref, w_ref, mine_ref, other_ref, c_ref, u_ref, packed_ref,
):
    blocks = v_ref.shape[0]
    at = len(pairs_of(blocks))
    fill_coupling(c_ref, core_ref[0], in_mine_ref, in_other_ref, at)
    local_part(core_ref, v_ref, (far_ref, close_ref, left_ref, right_ref), p_ref, u_ref)
    v = flat_lanes(v_ref)
    xi = joined(xi_ref)
    z = flat_lanes(u_ref) - dot(xi, c_ref[...], (1, 0))
    both = transformed(jnp.concatenate([v, z], axis=0), x_ref[...])
    finish(
        core_ref[0], core_ref[1], both[: v.shape[0]], both[v.shape[0] :], xi, vp_ref, w_ref, packed_ref, mine_ref,
        other_ref,
    )


def stepped(vp, w, y, stats, blocks):
    rayleigh = along_lanes(stats, 0, blocks)
    length = length_of(along_lanes(stats, blocks, blocks))
    return vp - (w - rayleigh * vp) * length, w - (y - rayleigh * w) * length


def last_transform_kernel(*refs):
    outs = 14
    transform_kernel(*refs[:outs], None, *refs[outs:], None)


def transform_kernel(
    core_ref, x_ref, stats_ref, in_mine_ref, in_other_ref, old_ref, v_ref, far_ref, close_ref, left_ref,
    right_ref, p_ref, xi_ref, vp_ref, w_ref, mine_ref, other_ref, c_ref, u_ref, packed_ref,
):
    blocks = v_ref.shape[0]
    at = 2 * len(apart_of(blocks)) + blocks + 1
    fill_coupling(c_ref, core_ref[0], in_mine_ref, in_other_ref, at)
    local_part(core_ref, v_ref, (far_ref, close_ref, left_ref, right_ref), p_ref, u_ref)
    xi = joined(xi_ref)
    y = flat_lanes(u_ref) - dot(xi, c_ref[...], (1, 0))
    v, z = stepped(joined(old_ref), flat_lanes(v_ref), y, stats_ref[...], blocks)
    both = transformed(jnp.concatenate([v, z], axis=0), x_ref[...])
    finish(
        core_ref[0], core_ref[1], both[: v.shape[0]], both[v.shape[0] :], xi, vp_ref, w_ref, packed_ref, mine_ref,
        other_ref,
    )


def ring(count, by):
    return [(i, (i + by) % count) for i in range(count)]


def turn():
    far = lax.axis_index("grid") // (lax.axis_size("grid") // 2)
    return far * (lax.axis_size(BAND) // 2)


def slab_pairs(start):
    slabs, quarters = lax.axis_size("grid"), lax.axis_size(BAND)

    def pair(g, b):
        there = (g + (1 if g % 2 == start else -1)) % slabs
        crosses = g // (slabs // 2) != there // (slabs // 2)
        return g * quarters + b, there * quarters + (b + crosses * (quarters // 2)) % quarters

    return [pair(g, b) for g in range(slabs) for b in range(quarters)]


def neighbours(v):
    near = lax.axis_size(BAND)
    far = lax.ppermute(v, EVERY, slab_pairs(1))
    close = lax.ppermute(v, EVERY, slab_pairs(0))
    return far, close, lax.ppermute(v, BAND, ring(near, 1)), lax.ppermute(v, BAND, ring(near, -1))


def swapped(x):
    return lax.ppermute(x, "band_1", ring(lax.axis_size("band_1"), 1))


def exchange(pieces):
    return lax.all_to_all(pieces, CHIPS, split_axis=0, concat_axis=0, tiled=True)


def from_every_chip(x):
    count = lax.axis_size(CHIPS)
    copies = jnp.broadcast_to(x, (count, *x.shape)).reshape(count * x.shape[0], *x.shape[1:])
    return exchange(copies)


def total_everywhere(mine, other):
    rows, lanes = mine.shape
    count = lax.axis_size(CHIPS)
    pieces = (mine + swapped(other)).reshape(rows // LINES, LINES, lanes)
    arrived = exchange(pieces)
    total = arrived.reshape(count, rows // LINES // count, LINES, lanes).sum(axis=0)
    half = from_every_chip(total).reshape(rows, lanes)
    return half, swapped(half)


def pieces_kernel(core_ref, first_ref, second_ref, out_ref):
    quarters, _, _, rows, _, _ = out_ref.shape
    for q in range(quarters):
        first_row = rows * lax.rem(core_ref[0] + q, quarters)
        for k, ref in enumerate((first_ref, second_ref)):
            for x in range(rows):
                out_ref[q, k, 0, x] = ref[0, first_row + x]


def to_cells(first, second):
    quarters = lax.axis_size(BAND)
    z, x, y, lanes = first.shape
    rows = x // quarters
    plane = pl.BlockSpec((1, x, y, lanes), lambda at: (at, 0, 0, 0))
    pieces = pl.pallas_call(
        pieces_kernel,
        grid=(z,),
        out_shape=jax.ShapeDtypeStruct((quarters, 2, z, rows, y, lanes), jnp.float32),
        in_specs=[pl.BlockSpec(memory_space=pltpu.SMEM), plane, plane],
        out_specs=pl.BlockSpec((quarters, 2, 1, rows, y, lanes), lambda at: (0, 0, at, 0, 0, 0)),
        compiler_params=pltpu.CompilerParams(vmem_limit_bytes=60 << 20),
        name="pieces_kernel",
    )(turn().astype(jnp.int32).reshape(1), first, second)
    pieces = lax.all_to_all(pieces, BAND, split_axis=0, concat_axis=0, tiled=True)
    return pieces[:, 0], pieces[:, 1]


def call(kernel, shapes, *args, scratch=(), flops=2_000_000_000, room=32):
    place = [lax.axis_index("band_1"), lax.axis_index(BAND), turn(), lax.axis_index("grid") % 2]
    place = jnp.stack(place).astype(jnp.int32)
    return pl.pallas_call(
        kernel,
        out_shape=[jax.ShapeDtypeStruct(s, jnp.float32) for s in shapes],
        in_specs=[pl.BlockSpec(memory_space=pltpu.SMEM)] + [WHOLE] * len(args),
        out_specs=[WHOLE] * len(shapes),
        scratch_shapes=[pltpu.VMEM(s, jnp.float32) for s in scratch],
        compiler_params=pltpu.CompilerParams(vmem_limit_bytes=room << 20),
        cost_estimate=pl.CostEstimate(
            flops=flops, bytes_accessed=4 * sum(a.size for a in args), transcendentals=0
        ),
    )(place, *args)


def local(orbitals, projectors, potential):
    v, xi = to_cells(orbitals, projectors)
    full = v.shape
    blocks, planes, rows, columns, lanes = full
    flat = (blocks, planes * rows * columns, lanes)
    total = blocks * lanes
    square = (total, total)
    xi = xi.reshape(flat)
    band = lax.axis_index(BAND)
    own = lax.dynamic_slice_in_dim(potential, (band + turn()) % blocks * rows, rows, 1)
    own = jnp.broadcast_to(own[..., None], (planes, rows, columns, lanes))
    pairs = len(pairs_of(blocks))

    def packed(count):
        return (BLOCK * count, BLOCK), (BLOCK * count // 2, BLOCK)

    small, small_half = packed(pairs + blocks * blocks)
    large, large_half = packed(blocks * (blocks - 1) + blocks + 2 + blocks * blocks)
    sums = (3 * blocks // 2, BLOCK)
    stats_shape = (2 * blocks, BLOCK)
    stats_list = []
    around = neighbours(v)
    mine, other = total_everywhere(*call(gram_kernel, [small_half] * 2, v.reshape(flat), xi, scratch=[small]))
    (x,) = call(first_factor_kernel, [square], mine, other, flops=20_000_000_000, room=16)
    vp, w, mine, other = call(
        first_transform_kernel, [flat, full, large_half, large_half], x, mine, other, v, *around, own, xi,
        scratch=[square, full, large],
    )
    for iteration in range(1, ITERS):
        around = neighbours(w)
        mine, other = total_everywhere(mine, other)
        x, stats = call(factor_kernel, [square, stats_shape], mine, other, flops=20_000_000_000, room=16)
        stats_list.append(stats)
        given = (x, stats, mine, other, vp, w, *around, own, xi)
        if iteration < ITERS - 1:
            vp, w, mine, other = call(
                transform_kernel, [flat, full, large_half, large_half], *given,
                scratch=[square, full, large],
            )
    both = (blocks, 2, planes, rows, columns, lanes)
    parts, mine, other = call(
        last_transform_kernel, [both, sums, sums], *given, scratch=[square, full]
    )
    parts = [parts[0]] + [lax.ppermute(parts[k], BAND, ring(blocks, k)) for k in range(1, blocks)]
    lines = (mine + swapped(other)).reshape(-1, LINES, lanes)
    here = from_every_chip(lines)
    here = here.reshape(lax.axis_size(CHIPS), *sums)
    lines = (ITERS, lanes)
    return tuple(
        call(
            last_kernel, [(planes, blocks * rows, columns, lanes), lines, lines], *parts, here,
            swapped(here), *stats_list, scratch=[stats_shape],
        )
    )


def solution(mesh):
    finer = Mesh(mesh.devices.reshape(mesh.shape["grid"], 2, 2), ("grid", "band_0", "band_1"))
    placed = (P("grid", None, None, BAND), P("grid", None, None, BAND), P("grid", None, None))
    return jax.shard_map(
        local,
        mesh=finer,
        in_specs=placed,
        out_specs=(P("grid", None, None, BAND), P(None, BAND), P(None, BAND)),
        check_vma=False,
    )
```
